256 devices in a mesh: seq: 64 (over x, z, core), head: 4 (over y).
Axes of the slice: x: 4, y: 4, z: 8, core: 2. Of those that a mesh axis runs over, the one named last changes fastest.
Arguments:
- queries: bfloat16 [32768, 1024], P('seq', 'head'), may hold values from -6 to 6
- key_vectors: bfloat16 [32768, 1024], P('seq', 'head'), may hold values from -6 to 6
- values: bfloat16 [32768, 2048], P('seq', 'head'), may hold values from -6 to 6
- log_gate: bfloat16 [32768, 1024], P('seq', 'head'), may hold values from -1.6 to 0, as said below
- out_gate: bfloat16 [32768, 2048], P('seq', 'head'), may hold values from -6 to 6
- norm_gain: float32 [2048], P('head'), may hold values from 0.5 to 1.5
- out_weight: bfloat16 [2048, 2048], P('head'), may hold values from -0.1875 to 0.1875
Outputs:
- mixed: bfloat16 [32768, 2048], P('seq', 'head')
The draws below stay inside these ranges and needn't reach their ends.
Inputs may be any that keep to these rules, and one draw needn't show every extreme that they name: `log_gate`: every entry is below zero.
All inputs are finite; a program needn't handle non-finite values.
Results may differ from the reference program's by a relative error of at most 0.017.
Values may be sent and summed in bfloat16 or wider, within the bound.
No kernel may reach another device: no remote copies, remote signals or barrier semaphores. Data moves between devices by JAX's collectives and lax.ppermute only.
A program may use at most 128 MiB of HBM per device.

```python
import jax
import jax.numpy as jnp
from jax import lax

D = 2048
H = 4
DK = 256
DV = 512
SPAN = 64
TOK_DEV = 512
SEQUENCE_TOKENS = 32768
N_HEAD = 4


def draw_log_gate(key, part):
    parallel_lanes = jax.random.split(key, 7)
    blocks_all = SEQUENCE_TOKENS // TOK_DEV
    quick_count = H // 2
    order = jax.random.permutation(parallel_lanes[0], H)
    quick_head = order < quick_count
    quick_rate = jnp.exp(jax.random.uniform(parallel_lanes[1], (H, DK), minval=jnp.log(0.02), maxval=jnp.log(0.06)))
    slow_rate = jnp.exp(jax.random.uniform(parallel_lanes[2], (H, DK), minval=jnp.log(0.05), maxval=jnp.log(0.25))) / SEQUENCE_TOKENS
    base_rate = jnp.where(quick_head[:, None], quick_rate, slow_rate).reshape(1, 1, H * DK)
    device_factor = jnp.exp(jax.random.uniform(parallel_lanes[3], (blocks_all, 1, H * DK), minval=jnp.log(0.5), maxval=jnp.log(2.0)))
    roughness = jax.random.uniform(parallel_lanes[4], (blocks_all, TOK_DEV, H * DK), minval=0.5, maxval=1.5)
    decay_factor = (base_rate * device_factor * roughness).reshape(SEQUENCE_TOKENS, H * DK)
    block_offset = jax.random.randint(parallel_lanes[5], (2,), 0, SEQUENCE_TOKENS)
    block_length = jnp.log(jax.random.uniform(parallel_lanes[6], (2,), minval=0.5, maxval=0.8))
    token_position = lax.iota(jnp.int32, SEQUENCE_TOKENS)
    token_block = jnp.sum(jnp.where(token_position[:, None] == block_offset[None, :], block_length[None, :], 0.0), axis=1)
    return (token_block[:, None] - decay_factor).astype(jnp.bfloat16)


def raised(entries, rng, source, target, parts, factor):
    def block_of(dim):
        return (jnp.arange(entries.shape[dim]) // (entries.shape[dim] // parts)).reshape((-1,) + (1,) * (entries.ndim - 1 - dim))

    near = jax.random.permutation(rng, parts)[block_of(target)]
    other_side = (block_of(target) + parts // 2) % parts
    return jnp.where((block_of(source) == near) | (block_of(source) == other_side), factor * entries, entries)


def steps_of(stream_key, dims, pieces, least, largest):
    def one(axis_at, shards_of):
        heights = jax.random.uniform(jax.random.fold_in(jax.random.fold_in(stream_key, 6), axis_at), (shards_of,), jnp.float32, least / len(pieces), largest / len(pieces))
        return jnp.repeat(jnp.exp(heights), dims[axis_at] // shards_of).reshape((-1,) + (1,) * (len(dims) - axis_at - 1))

    factor_of = one(*pieces[0])
    for cut in pieces[1:]:
        factor_of = factor_of * one(*cut)
    return factor_of


def normal_values(stream_key, shape, scale, most, cuts=(), kind=jnp.bfloat16):
    factor_of = steps_of(stream_key, shape, cuts, -0.22, 0.18) if cuts else 1.0
    result = jax.random.normal(stream_key, shape, jnp.float32) * scale * factor_of
    return jnp.minimum(jnp.maximum(result, -most), most).astype(kind)


def noise_with(own_key, dims, scale, reach, cuts, heavy, dtype=jnp.bfloat16):
    array = scale * jax.random.normal(own_key, dims, jnp.float32)
    if cuts:
        array = array * steps_of(own_key, dims, cuts, -0.22, 0.18)
    return jnp.clip(raised(array, jax.random.fold_in(own_key, 3), *heavy), -reach, reach).astype(dtype)


def setup_inputs(seed: int = 0) -> dict:
    streams_of = jax.random.split(jax.random.key(seed), 8)
    queries = normal_values(streams_of[0], (SEQUENCE_TOKENS, H * DK), 1.0, 6.0, ((0, 64), (1, 4)))
    key_vectors = normal_values(streams_of[1], (SEQUENCE_TOKENS, H * DK), 1.0, 6.0, ((0, 64), (1, 4)))
    values = normal_values(streams_of[2], (SEQUENCE_TOKENS, H * DV), 1.0, 6.0, ((0, 64), (1, 4)))
    log_gate = draw_log_gate(jax.random.fold_in(streams_of[7], 71), 0)
    out_gate = normal_values(streams_of[4], (SEQUENCE_TOKENS, H * DV), 1.0, 6.0, ((0, 64), (1, 4)))
    norm_gain = jnp.clip(1.0 + 0.1 * jax.random.normal(streams_of[5], (H * DV,), jnp.float32), 0.5, 1.5)
    out_weight = noise_with(streams_of[6], (H * DV, D), (H * DV) ** -0.5, 0.1875, ((0, 4),), (0, 1, 4, 2.0))
    return {"queries": queries, "key_vectors": key_vectors, "values": values, "log_gate": log_gate, "out_gate": out_gate, "norm_gain": norm_gain, "out_weight": out_weight}


def lowered(array_in):
    return lax.optimization_barrier(array_in.astype(jnp.bfloat16)).astype(jnp.float32)

def reference(queries, key_vectors, values, log_gate, out_gate, norm_gain, out_weight):
    blocks = SEQUENCE_TOKENS // SPAN
    middle_pos = SPAN // 2
    causal = lax.iota(jnp.int32, SPAN)[:, None] >= lax.iota(jnp.int32, SPAN)[None, :]
    gain_table = norm_gain.reshape(H, DV)

    def advance(carried, block_in):
        query_b, key_b, value_b, gate_b, outer_b = block_in
        running = jnp.cumsum(gate_b.astype(jnp.float32), axis=0)
        middle = running[middle_pos:middle_pos + 1]
        ending = running[SPAN - 1:SPAN]
        query_f = query_b.astype(jnp.float32)
        key_f = key_b.astype(jnp.float32)
        value_f = value_b.astype(jnp.float32)
        q_inter = lowered(query_f * jnp.exp(running))
        q_intra = lowered(query_f * jnp.exp(running - middle))
        k_intra = lowered(key_f * jnp.exp(middle - running))
        k_state = lowered(key_f * jnp.exp(ending - running))
        scores = jnp.einsum('thd,shd->hts', q_intra, k_intra)
        weights = lowered(jnp.where(causal[None], scores, 0.0))
        local_part = jnp.einsum('hts,she->the', weights, value_f)
        carried_low = lowered(carried)
        carried_part = jnp.einsum('thd,hed->the', q_inter, carried_low)
        attention = local_part + carried_part
        spread = lax.optimization_barrier(jnp.mean(attention * attention, axis=-1, keepdims=True))
        normed = attention / jnp.sqrt(spread + 1e-05) * gain_table
        gated_out = (normed * jax.nn.silu(outer_b.astype(jnp.float32))).astype(jnp.bfloat16)
        block_state = jnp.einsum('the,thd->hed', value_f, k_state)
        carried = carried * jnp.exp(ending[0])[:, None, :] + block_state
        return (carried, gated_out.reshape(SPAN, H * DV))
    start_state = jnp.zeros((H, DV, DK), jnp.float32)
    inputs = (queries.reshape(blocks, SPAN, H, DK), key_vectors.reshape(blocks, SPAN, H, DK), values.reshape(blocks, SPAN, H, DV), log_gate.reshape(blocks, SPAN, H, DK), out_gate.reshape(blocks, SPAN, H, DV))
    unused_state, gated_all = lax.scan(advance, start_state, inputs)
    gated_all = gated_all.reshape(SEQUENCE_TOKENS, H * DV)
    group_width = H // N_HEAD * DV
    summed = jnp.zeros((SEQUENCE_TOKENS, D), jnp.float32)
    for group_index in range(N_HEAD):
        start_row = group_index * group_width
        end_row = start_row + group_width
        partial_value = jnp.dot(gated_all[:, start_row:end_row], out_weight[start_row:end_row], preferred_element_type=jnp.float32)
        summed = summed + lowered(partial_value)
    return summed.astype(jnp.bfloat16)
```

```python
import functools

import jax
import jax.numpy as jnp
from jax import lax
from jax.experimental import pallas as pl
from jax.experimental.pallas import tpu as pltpu
from jax.sharding import Mesh
from jax.sharding import PartitionSpec as P

DK = 256
DV = 512
SPAN = 64
LANE = 128
SEQ = ("seq_0", "seq_1", "seq_2")
F32 = jnp.float32
BF16 = jnp.bfloat16
VMEM = pl.BlockSpec(memory_space=pltpu.VMEM)


def call(body, outs, *args, flops=10**9):
    moved = sum(a.size * a.dtype.itemsize for a in args)
    return pl.pallas_call(
        body,
        out_shape=outs,
        in_specs=[VMEM] * len(args),
        out_specs=jax.tree.map(lambda _: VMEM, outs),
        cost_estimate=pl.CostEstimate(flops=flops, transcendentals=0, bytes_accessed=moved),
    )(*args)


def dot(a, b, dims=((1,), (0,))):
    return lax.dot_general(a, b, (dims, ((), ())), preferred_element_type=F32)


def triangle(length, keep):
    row = lax.broadcasted_iota(jnp.int32, (length, length), 0)
    col = lax.broadcasted_iota(jnp.int32, (length, length), 1)
    return jnp.where(keep(row, col), 1.0, 0.0).astype(BF16)


def state_body(k_ref, v_ref, g_ref, out_ref):
    length = k_ref.shape[0]
    pieces = out_ref.shape[0]
    gate = g_ref[...]
    after = dot(triangle(length, lambda r, c: c > r), gate)
    k_state = (k_ref[...].astype(F32) * jnp.exp(after)).astype(BF16)
    state = dot(v_ref[...], k_state, ((0,), (0,)))
    total = after[0:1] + gate[0:1].astype(F32)
    high = total.astype(BF16).astype(F32)
    low = total - high
    rows = state.shape[0] // pieces
    row = lax.broadcasted_iota(jnp.int32, (8, LANE), 0)
    tail = jnp.zeros((8, LANE), F32)
    for at, part in enumerate((high[:, :LANE], high[:, LANE:], low[:, :LANE], low[:, LANE:])):
        tail = jnp.where(row == at, part, tail)
    out_ref[:, 0:rows, :] = state[:, :LANE].reshape(pieces, rows, LANE).astype(BF16)
    out_ref[:, rows : 2 * rows, :] = state[:, LANE:].reshape(pieces, rows, LANE).astype(BF16)
    out_ref[:, 2 * rows :, :] = jnp.broadcast_to(tail[None], (pieces, 8, LANE)).astype(BF16)


def scan_body(in_ref, out_ref):
    pieces, rows = (in_ref.shape[0], out_ref.shape[1] // 2)
    left = right = jnp.zeros((rows, LANE), F32)
    for j in range(pieces):
        out_ref[j, 0:rows, :] = left.astype(BF16)
        out_ref[j, rows : 2 * rows, :] = right.astype(BF16)
        tail = in_ref[j, 2 * rows :, :].astype(F32)
        left = left * jnp.exp(tail[0:1] + tail[2:3]) + in_ref[j, 0:rows, :].astype(F32)
        right = right * jnp.exp(tail[1:2] + tail[3:4]) + in_ref[j, rows : 2 * rows, :].astype(F32)


def local_body(q_ref, k_ref, v_ref, g_ref, att_ref, q_out_ref):
    length = q_ref.shape[0]
    lower = triangle(SPAN, lambda r, c: c <= r)
    row = lax.broadcasted_iota(jnp.int32, (SPAN, SPAN), 0)
    col = lax.broadcasted_iota(jnp.int32, (SPAN, SPAN), 1)
    carried = None
    before = jnp.zeros((1, DK), F32)
    for i in range(length // SPAN):
        at = slice(i * SPAN, (i + 1) * SPAN)
        running = dot(lower, g_ref[at, :])
        middle = running[SPAN // 2 : SPAN // 2 + 1]
        ending = running[SPAN - 1 : SPAN]
        query_f = q_ref[at, :].astype(F32)
        key_f = k_ref[at, :].astype(F32)
        value = v_ref[at, :]
        q_inter = query_f * jnp.exp(running)
        q_intra = (query_f * jnp.exp(running - middle)).astype(BF16)
        k_intra = (key_f * jnp.exp(middle - running)).astype(BF16)
        scores = dot(q_intra, k_intra, ((1,), (1,)))
        weights = jnp.where(col <= row, scores, 0.0).astype(BF16)
        attention = dot(weights, value)
        if i:
            attention = attention + dot(q_inter.astype(BF16), carried.astype(BF16))
        att_ref[at, :] = attention
        q_out_ref[at, :] = (query_f * jnp.exp(running + before)).astype(BF16)
        before = before + ending
        if (i + 1) * SPAN < length:
            k_state = (key_f * jnp.exp(ending - running)).T.astype(BF16)
            block = dot(k_state, value)
            carried = block if i == 0 else carried * jnp.exp(ending).reshape(DK, 1) + block


def finish_body(s_ref, q_ref, att_ref, outer_ref, gain_ref, w_ref, gated_ref, far_ref):
    pieces, rows = (s_ref.shape[0], s_ref.shape[1] // 2)
    count = lax.axis_size("head")
    far = lax.rem(lax.axis_index("head") + count // 2, count)
    s_left = s_ref[:, 0:rows, :].reshape(pieces * rows, LANE)
    s_right = s_ref[:, rows : 2 * rows, :].reshape(pieces * rows, LANE)
    attention = att_ref[...]
    attention = attention + dot(q_ref[:, :LANE], s_left, ((1,), (1,)))
    attention = attention + dot(q_ref[:, LANE:], s_right, ((1,), (1,)))
    spread = jnp.mean(attention * attention, axis=-1, keepdims=True)
    normed = attention * lax.rsqrt(spread + 1e-05) * gain_ref[...]
    outer_f = outer_ref[...].astype(F32)
    gated = (normed * (outer_f / (1.0 + jnp.exp(-outer_f)))).astype(BF16)
    gated_ref[...] = gated
    width = far_ref.shape[1]
    start = pl.multiple_of(far * width, width)
    far_ref[...] = dot(gated, w_ref[:, pl.ds(start, width)]).astype(BF16)


def near_body(gated_ref, w_ref, up_ref, down_ref, own_ref):
    count = lax.axis_size("head")
    me = lax.axis_index("head")
    width = own_ref.shape[1]
    gated = gated_ref[...]
    for ref, shift in ((up_ref, 1), (down_ref, count - 1), (own_ref, 0)):
        start = pl.multiple_of(lax.rem(me + shift, count) * width, width)
        ref[...] = dot(gated, w_ref[:, pl.ds(start, width)]).astype(BF16)


def ring(axis, shift):
    length = lax.axis_size(axis)
    return [(i, (i + shift) % length) for i in range(length)]


def shards(queries, key_vectors, values, log_gate, out_gate, norm_gain, out_weight):
    length = queries.shape[0]
    pieces = lax.axis_size(SEQ)
    rows = DV // pieces
    shape = jax.ShapeDtypeStruct
    sent = call(
        state_body,
        shape((pieces, 2 * rows + 8, LANE), BF16),
        key_vectors,
        values,
        log_gate,
    )
    slices = lax.all_to_all(sent, SEQ, 0, 0, tiled=True)
    att_local, q_start = call(
        local_body,
        (shape((length, DV), F32), shape((length, DK), BF16)),
        queries,
        key_vectors,
        values,
        log_gate,
    )
    prefixes = call(scan_body, shape((pieces, 2 * rows, LANE), BF16), slices)
    incoming = lax.all_to_all(prefixes, SEQ, 0, 0, tiled=True)
    width = out_weight.shape[1] // lax.axis_size("head")
    block = shape((length, width), BF16)
    gated, far = call(
        finish_body,
        (shape((length, DV), BF16), block),
        incoming,
        q_start,
        att_local,
        out_gate,
        norm_gain.reshape(1, DV),
        out_weight,
    )
    half = length // 2
    far_up = lax.ppermute(far[:half], "head", ring("head", 1))
    far_down = lax.ppermute(far[half:], "head", ring("head", -1))
    up, down, own = call(near_body, (block, block, block), gated, out_weight)
    up_a = (up[:half].astype(F32) + far_up.astype(F32)).astype(BF16)
    down_b = (down[half:].astype(F32) + far_down.astype(F32)).astype(BF16)
    from_down_b = lax.ppermute(up[half:], "head", ring("head", 1))
    from_up_a = lax.ppermute(down[:half], "head", ring("head", -1))
    from_down_a = lax.ppermute(up_a, "head", ring("head", 1))
    from_up_b = lax.ppermute(down_b, "head", ring("head", -1))
    out_a = own[:half].astype(F32) + from_up_a.astype(F32) + from_down_a.astype(F32)
    out_b = own[half:].astype(F32) + from_up_b.astype(F32) + from_down_b.astype(F32)
    return jnp.concatenate([out_a, out_b], axis=0).astype(BF16)


def solution(mesh):
    split = Mesh(
        mesh.devices.reshape(4, 8, 2, mesh.shape["head"]), ("seq_0", "seq_1", "seq_2", "head")
    )
    in_specs = (
        P(SEQ, "head"),
        P(SEQ, "head"),
        P(SEQ, "head"),
        P(SEQ, "head"),
        P(SEQ, "head"),
        P("head"),
        P("head", None),
    )
    out_specs = P(SEQ, "head")
    return jax.shard_map(
        shards, mesh=split, in_specs=in_specs, out_specs=out_specs, check_vma=False
    )
```

```python
import functools

import jax
import jax.numpy as jnp
from jax import lax
from jax.experimental import pallas as pl
from jax.experimental.pallas import tpu as pltpu
from jax.sharding import Mesh
from jax.sharding import PartitionSpec as P

DK = 256
DV = 512
SPAN = 64
LANE = 128
SEQ = ("seq_0", "seq_1", "seq_2")
F32 = jnp.float32
BF16 = jnp.bfloat16
VMEM = pl.BlockSpec(memory_space=pltpu.VMEM)


def call(body, outs, *args, flops=10**9):
    moved = sum(a.size * a.dtype.itemsize for a in args)
    return pl.pallas_call(
        body,
        out_shape=outs,
        in_specs=[VMEM] * len(args),
        out_specs=jax.tree.map(lambda _: VMEM, outs),
        cost_estimate=pl.CostEstimate(flops=flops, transcendentals=0, bytes_accessed=moved),
        compiler_params=pltpu.CompilerParams(vmem_limit_bytes=16 * 2**20),
    )(*args)


def dot(a, b, dims=((1,), (0,))):
    return lax.dot_general(a, b, (dims, ((), ())), preferred_element_type=F32)


def triangle(length, keep):
    row = lax.broadcasted_iota(jnp.int32, (length, length), 0)
    col = lax.broadcasted_iota(jnp.int32, (length, length), 1)
    return jnp.where(keep(row, col), 1.0, 0.0).astype(BF16)


def state_body(k_ref, v_ref, g_ref, out_ref):
    length = k_ref.shape[0]
    pieces = out_ref.shape[0]
    gate = g_ref[...]
    after = dot(triangle(length, lambda r, c: c > r), gate)
    k_state = (k_ref[...].astype(F32) * jnp.exp(after)).astype(BF16)
    state = dot(v_ref[...], k_state, ((0,), (0,)))
    total = after[0:1] + gate[0:1].astype(F32)
    high = total.astype(BF16).astype(F32)
    low = total - high
    rows = state.shape[0] // pieces
    row = lax.broadcasted_iota(jnp.int32, (8, LANE), 0)
    tail = jnp.zeros((8, LANE), F32)
    for at, part in enumerate((high[:, :LANE], high[:, LANE:], low[:, :LANE], low[:, LANE:])):
        tail = jnp.where(row == at, part, tail)
    out_ref[:, 0:rows, :] = state[:, :LANE].reshape(pieces, rows, LANE).astype(BF16)
    out_ref[:, rows : 2 * rows, :] = state[:, LANE:].reshape(pieces, rows, LANE).astype(BF16)
    out_ref[:, 2 * rows :, :] = jnp.broadcast_to(tail[None], (pieces, 8, LANE)).astype(BF16)


def scan_body(in_ref, out_ref):
    pieces, rows = (in_ref.shape[0], out_ref.shape[1] // 2)
    left = right = jnp.zeros((rows, LANE), F32)
    for j in range(pieces):
        out_ref[j, 0:rows, :] = left.astype(BF16)
        out_ref[j, rows : 2 * rows, :] = right.astype(BF16)
        tail = in_ref[j, 2 * rows :, :].astype(F32)
        left = left * jnp.exp(tail[0:1] + tail[2:3]) + in_ref[j, 0:rows, :].astype(F32)
        right = right * jnp.exp(tail[1:2] + tail[3:4]) + in_ref[j, rows : 2 * rows, :].astype(F32)


def local_body(q_ref, k_ref, v_ref, g_ref, att_ref, q_out_ref):
    length = q_ref.shape[0]
    lower = triangle(SPAN, lambda r, c: c <= r)
    row = lax.broadcasted_iota(jnp.int32, (SPAN, SPAN), 0)
    col = lax.broadcasted_iota(jnp.int32, (SPAN, SPAN), 1)
    carried = None
    before = jnp.zeros((1, DK), F32)
    for i in range(length // SPAN):
        at = slice(i * SPAN, (i + 1) * SPAN)
        running = dot(lower, g_ref[at, :])
        middle = running[SPAN // 2 : SPAN // 2 + 1]
        ending = running[SPAN - 1 : SPAN]
        query_f = q_ref[at, :].astype(F32)
        key_f = k_ref[at, :].astype(F32)
        value = v_ref[at, :]
        q_inter = query_f * jnp.exp(running)
        q_intra = (query_f * jnp.exp(running - middle)).astype(BF16)
        k_intra = (key_f * jnp.exp(middle - running)).astype(BF16)
        scores = dot(q_intra, k_intra, ((1,), (1,)))
        weights = jnp.where(col <= row, scores, 0.0).astype(BF16)
        attention = dot(weights, value)
        if i:
            attention = attention + dot(q_inter.astype(BF16), carried.astype(BF16))
        att_ref[at, :] = attention
        q_out_ref[at, :] = (query_f * jnp.exp(running + before)).astype(BF16)
        before = before + ending
        if (i + 1) * SPAN < length:
            k_state = (key_f * jnp.exp(ending - running)).T.astype(BF16)
            block = dot(k_state, value)
            carried = block if i == 0 else carried * jnp.exp(ending).reshape(DK, 1) + block


def finish_body(s_ref, q_ref, att_ref, outer_ref, gain_ref, w_ref, gated_ref, far_ref):
    pieces, rows = (s_ref.shape[0], s_ref.shape[1] // 2)
    count = lax.axis_size("head")
    far = lax.rem(lax.axis_index("head") + count // 2, count)
    s_left = s_ref[:, 0:rows, :].reshape(pieces * rows, LANE)
    s_right = s_ref[:, rows : 2 * rows, :].reshape(pieces * rows, LANE)
    attention = att_ref[...]
    attention = attention + dot(q_ref[:, :LANE], s_left, ((1,), (1,)))
    attention = attention + dot(q_ref[:, LANE:], s_right, ((1,), (1,)))
    spread = jnp.mean(attention * attention, axis=-1, keepdims=True)
    normed = attention * lax.rsqrt(spread + 1e-05) * gain_ref[...]
    outer_f = outer_ref[...].astype(F32)
    gated = (normed * (outer_f / (1.0 + jnp.exp(-outer_f)))).astype(BF16)
    gated_ref[...] = gated
    width = far_ref.shape[1]
    start = pl.multiple_of(far * width, width)
    far_ref[...] = dot(gated, w_ref[:, pl.ds(start, width)]).astype(BF16)


def near_body(gated_ref, w_ref, up_ref, down_ref, own_ref):
    count = lax.axis_size("head")
    me = lax.axis_index("head")
    width = own_ref.shape[1]
    gated = gated_ref[...]
    for ref, shift in ((up_ref, 1), (down_ref, count - 1), (own_ref, 0)):
        start = pl.multiple_of(lax.rem(me + shift, count) * width, width)
        ref[...] = dot(gated, w_ref[:, pl.ds(start, width)]).astype(BF16)


def ring(axis, shift):
    length = lax.axis_size(axis)
    return [(i, (i + shift) % length) for i in range(length)]


def shards(queries, key_vectors, values, log_gate, out_gate, norm_gain, out_weight):
    length = queries.shape[0]
    pieces = lax.axis_size(SEQ)
    rows = DV // pieces
    shape = jax.ShapeDtypeStruct
    sent = call(
        state_body,
        shape((pieces, 2 * rows + 8, LANE), BF16),
        key_vectors,
        values,
        log_gate,
    )
    slices = lax.all_to_all(sent, SEQ, 0, 0, tiled=True)
    att_local, q_start = call(
        local_body,
        (shape((length, DV), F32), shape((length, DK), BF16)),
        queries,
        key_vectors,
        values,
        log_gate,
    )
    prefixes = call(scan_body, shape((pieces, 2 * rows, LANE), BF16), slices)
    incoming = lax.all_to_all(prefixes, SEQ, 0, 0, tiled=True)
    width = out_weight.shape[1] // lax.axis_size("head")
    block = shape((length, width), BF16)
    gated, far = call(
        finish_body,
        (shape((length, DV), BF16), block),
        incoming,
        q_start,
        att_local,
        out_gate,
        norm_gain.reshape(1, DV),
        out_weight,
    )
    half = length // 2
    far_up = lax.ppermute(far[:half], "head", ring("head", 1))
    far_down = lax.ppermute(far[half:], "head", ring("head", -1))
    up, down, own = call(near_body, (block, block, block), gated, out_weight)
    up_a = (up[:half].astype(F32) + far_up.astype(F32)).astype(BF16)
    down_b = (down[half:].astype(F32) + far_down.astype(F32)).astype(BF16)
    from_down_b = lax.ppermute(up[half:], "head", ring("head", 1))
    from_up_a = lax.ppermute(down[:half], "head", ring("head", -1))
    from_down_a = lax.ppermute(up_a, "head", ring("head", 1))
    from_up_b = lax.ppermute(down_b, "head", ring("head", -1))
    out_a = own[:half].astype(F32) + from_up_a.astype(F32) + from_down_a.astype(F32)
    out_b = own[half:].astype(F32) + from_up_b.astype(F32) + from_down_b.astype(F32)
    return jnp.concatenate([out_a, out_b], axis=0).astype(BF16)


def solution(mesh):
    split = Mesh(
        mesh.devices.reshape(4, 8, 2, mesh.shape["head"]), ("seq_0", "seq_1", "seq_2", "head")
    )
    in_specs = (
        P(SEQ, "head"),
        P(SEQ, "head"),
        P(SEQ, "head"),
        P(SEQ, "head"),
        P(SEQ, "head"),
        P("head"),
        P("head", None),
    )
    out_specs = P(SEQ, "head")
    return jax.shard_map(
        shards, mesh=split, in_specs=in_specs, out_specs=out_specs, check_vma=False
    )
```

```python
import jax
import jax.numpy as jnp
from jax import lax
from jax.experimental import pallas as pl
from jax.experimental.pallas import tpu as pltpu
from jax.sharding import Mesh
from jax.sharding import PartitionSpec as P

DK = 256
DV = 512
SPAN = 64
LANE = 128
SEQ = ("chip_x", "chip_z", "core")
CHIPS = ("chip_x", "chip_z")
F32 = jnp.float32
BF16 = jnp.bfloat16
VMEM = pl.BlockSpec(memory_space=pltpu.VMEM)
HBM = pl.BlockSpec(memory_space=pltpu.HBM)


def call(body, outs, *args, fetched=(), flops=10**9):
    moved = sum(a.size * a.dtype.itemsize for a in args)
    scratch = [pltpu.VMEM(args[i].shape, args[i].dtype) for i in fetched]
    if fetched:
        scratch.append(pltpu.SemaphoreType.DMA((len(fetched),)))
    return pl.pallas_call(
        body,
        out_shape=outs,
        in_specs=[HBM if i in fetched else VMEM for i in range(len(args))],
        out_specs=jax.tree.map(lambda _: VMEM, outs),
        scratch_shapes=scratch,
        cost_estimate=pl.CostEstimate(flops=flops, transcendentals=0, bytes_accessed=moved),
        compiler_params=pltpu.CompilerParams(vmem_limit_bytes=16 * 2**20),
    )(*args)


def dot(a, b, dims=((1,), (0,))):
    return lax.dot_general(a, b, (dims, ((), ())), preferred_element_type=F32)


def triangle(length, keep):
    row = lax.broadcasted_iota(jnp.int32, (length, length), 0)
    col = lax.broadcasted_iota(jnp.int32, (length, length), 1)
    return jnp.where(keep(row, col), 1.0, 0.0).astype(BF16)


def stacked(*parts):
    row = lax.broadcasted_iota(jnp.int32, (8, LANE), 0)
    block = jnp.zeros((8, LANE), F32)
    for at, part in enumerate(parts):
        block = jnp.where(row == at, part, block)
    return block


def split_bf16(values):
    high = values.astype(BF16).astype(F32)
    return high, values - high


def state_body(k_hbm, v_hbm, g_hbm, own_ref, log_ref, swap_ref, k_ref, v_ref, g_ref, sems):
    copies = [
        pltpu.make_async_copy(src, dst, sems.at[i])
        for i, (src, dst) in enumerate(((g_hbm, g_ref), (k_hbm, k_ref), (v_hbm, v_ref)))
    ]
    for copy in copies:
        copy.start()
    length = k_ref.shape[0]
    half = DV // 2
    mask = triangle(length, lambda r, c: c > r)
    copies[0].wait()
    gate = g_ref[...]
    after = dot(mask, gate)
    total = after[0:1] + gate[0:1].astype(F32)
    copies[1].wait()
    k_state = (k_ref[...].astype(F32) * jnp.exp(after)).astype(BF16)
    copies[2].wait()
    core = lax.axis_index("core")
    theirs = pl.ds(pl.multiple_of((1 - core) * half, half), half)
    state = dot(v_ref[:, theirs], k_state, ((0,), (0,))).astype(BF16)
    swap_ref[0:half, :] = state[:, :LANE]
    swap_ref[half : 2 * half, :] = state[:, LANE:]
    left_high, left_low = split_bf16(total[:, :LANE])
    right_high, right_low = split_bf16(total[:, LANE:])
    tail = stacked(left_high, right_high, left_low, right_low)
    swap_ref[2 * half :, :] = jnp.concatenate([tail, tail], axis=0).astype(BF16)
    mine = pl.ds(pl.multiple_of(core * half, half), half)
    state = dot(v_ref[:, mine], k_state, ((0,), (0,)))
    own_ref[0:half, :] = state[:, :LANE]
    own_ref[half:, :] = state[:, LANE:]
    log_ref[...] = stacked(total[:, :LANE], total[:, LANE:])


def join_body(own_ref, log_ref, swap_ref, out_ref, first_ref, decay_ref):
    pieces, rows = (out_ref.shape[0], (out_ref.shape[1] - 8) // 2)
    half = pieces * rows
    early = lax.axis_index("core") == 0
    tail = swap_ref[2 * half : 2 * half + 8, :].astype(F32)
    sums = []
    decays = []
    for side in range(2):
        at = slice(side * half, (side + 1) * half)
        own_log = log_ref[side : side + 1, :]
        other_log = tail[side : side + 1] + tail[side + 2 : side + 3]
        own = own_ref[at, :]
        other = swap_ref[at, :].astype(F32)
        first = jnp.where(early, own, other)
        second = jnp.where(early, other, own)
        state = first * jnp.exp(jnp.where(early, other_log, own_log)) + second
        first_ref[at, :] = first
        decays.append(jnp.exp(jnp.where(early, own_log, other_log)))
        sums.append(own_log + other_log)
        piece = slice(side * rows, (side + 1) * rows)
        out_ref[:, piece, :] = state.reshape(pieces, rows, LANE).astype(BF16)
    decay_ref[...] = stacked(*decays)
    left_high, left_low = split_bf16(sums[0])
    right_high, right_low = split_bf16(sums[1])
    tail = stacked(left_high, right_high, left_low, right_low)
    out_ref[:, 2 * rows :, :] = jnp.broadcast_to(tail[None], (pieces, 8, LANE)).astype(BF16)


def scan_body(in_ref, out_ref):
    pieces, rows = (in_ref.shape[0], out_ref.shape[1] // 2)
    left = right = jnp.zeros((rows, LANE), F32)
    for j in range(pieces):
        out_ref[j, 0:rows, :] = left.astype(BF16)
        out_ref[j, rows : 2 * rows, :] = right.astype(BF16)
        tail = in_ref[j, 2 * rows :, :].astype(F32)
        left = left * jnp.exp(tail[0:1] + tail[2:3]) + in_ref[j, 0:rows, :].astype(F32)
        right = right * jnp.exp(tail[1:2] + tail[3:4]) + in_ref[j, rows : 2 * rows, :].astype(F32)


def part_body(in_ref, first_ref, decay_ref, keep_ref, send_ref):
    pieces, rows = (in_ref.shape[0], in_ref.shape[1] // 2)
    half = pieces * rows
    early = lax.axis_index("core") == 0
    for side in range(2):
        at = slice(side * half, (side + 1) * half)
        piece = slice(side * rows, (side + 1) * rows)
        entering = in_ref[:, piece, :].astype(F32).reshape(half, LANE)
        between = entering * decay_ref[side : side + 1, :] + first_ref[at, :]
        keep_ref[at, :] = jnp.where(early, entering, between).astype(BF16)
        send_ref[at, :] = jnp.where(early, between, entering).astype(BF16)


def local_body(
    q_hbm, k_hbm, v_hbm, g_hbm, outer_hbm, gain_ref, att_ref, start_ref, scale_ref,
    q_ref, k_ref, v_ref, g_ref, outer_ref, sems,
):
    pairs = ((g_hbm, g_ref), (q_hbm, q_ref), (k_hbm, k_ref), (v_hbm, v_ref), (outer_hbm, outer_ref))
    copies = [pltpu.make_async_copy(src, dst, sems.at[i]) for i, (src, dst) in enumerate(pairs)]
    for copy in copies:
        copy.start()
    length = q_ref.shape[0]
    lower = triangle(SPAN, lambda r, c: c <= r)
    row = lax.broadcasted_iota(jnp.int32, (SPAN, SPAN), 0)
    col = lax.broadcasted_iota(jnp.int32, (SPAN, SPAN), 1)
    for copy in copies:
        copy.wait()
    carried = None
    before = jnp.zeros((1, DK), F32)
    for i in range(length // SPAN):
        at = slice(i * SPAN, (i + 1) * SPAN)
        running = dot(lower, g_ref[at, :])
        middle = running[SPAN // 2 : SPAN // 2 + 1]
        ending = running[SPAN - 1 : SPAN]
        query_f = q_ref[at, :].astype(F32)
        key_f = k_ref[at, :].astype(F32)
        value = v_ref[at, :]
        q_inter = query_f * jnp.exp(running)
        q_intra = (query_f * jnp.exp(running - middle)).astype(BF16)
        k_intra = (key_f * jnp.exp(middle - running)).astype(BF16)
        scores = dot(q_intra, k_intra, ((1,), (1,)))
        weights = jnp.where(col <= row, scores, 0.0).astype(BF16)
        attention = dot(weights, value)
        if i:
            attention = attention + dot(q_inter.astype(BF16), carried.astype(BF16))
        att_ref[at, :] = attention
        start_ref[at, :] = (query_f * jnp.exp(running + before)).astype(BF16)
        before = before + ending
        if (i + 1) * SPAN < length:
            k_state = (key_f * jnp.exp(ending - running)).T.astype(BF16)
            block = dot(k_state, value)
            carried = block if i == 0 else carried * jnp.exp(ending).reshape(DK, 1) + block
        outer_f = outer_ref[at, :].astype(F32)
        scale_ref[at, :] = outer_f / (1.0 + jnp.exp(-outer_f)) * gain_ref[...]


def columns(index, width):
    return pl.ds(pl.multiple_of(index * width, width), width)


def finish_body(
    keep_ref, other_ref, q_ref, att_ref, scale_ref, w_hbm, gated_ref, far_a_ref, far_b_ref,
    w_ref, sems,
):
    count = lax.axis_size("head")
    width = far_a_ref.shape[1]
    far = lax.rem(lax.axis_index("head") + count // 2, count)
    copy = pltpu.make_async_copy(
        w_hbm.at[:, columns(far, width)], w_ref.at[:, columns(0, width)], sems.at[0]
    )
    copy.start()
    half = DV // 2
    core = lax.axis_index("core")
    total = 0.0
    parts = []
    for ref, place in ((keep_ref, core), (other_ref, 1 - core)):
        attention = att_ref[:, columns(place, half)]
        attention = attention + dot(q_ref[:, :LANE], ref[:half, :], ((1,), (1,)))
        attention = attention + dot(q_ref[:, LANE:], ref[half:, :], ((1,), (1,)))
        total = total + jnp.sum(attention * attention, axis=-1, keepdims=True)
        parts.append((attention, place))
    inverse = lax.rsqrt(total * (1.0 / DV) + 1e-05)
    for attention, place in parts:
        at = columns(place, half)
        gated_ref[:, at] = (attention * inverse * scale_ref[:, at]).astype(BF16)
    copy.wait()
    rows = far_a_ref.shape[0]
    weight = w_ref[:, 0:width]
    far_a_ref[...] = dot(gated_ref[:rows, :], weight).astype(BF16)
    far_b_ref[...] = dot(gated_ref[rows:, :], weight).astype(BF16)


def near_body(gated_ref, w_hbm, up_ref, down_ref, own_ref, w_ref, sems):
    count = lax.axis_size("head")
    width = own_ref.shape[1]
    me = lax.axis_index("head")
    copy = pltpu.make_async_copy(w_hbm, w_ref, sems.at[0])
    copy.start()
    copy.wait()
    for ref, shift in ((up_ref, 1), (down_ref, count - 1), (own_ref, 0)):
        ref[...] = dot(gated_ref[...], w_ref[:, columns(lax.rem(me + shift, count), width)])


def pass_body(up_ref, down_ref, far_up_ref, far_down_ref, up_out_ref, down_out_ref):
    rows = far_up_ref.shape[0]
    up_out_ref[:rows, :] = (up_ref[:rows, :] + far_up_ref[...].astype(F32)).astype(BF16)
    up_out_ref[rows:, :] = up_ref[rows:, :].astype(BF16)
    down_out_ref[:rows, :] = down_ref[:rows, :].astype(BF16)
    down_out_ref[rows:, :] = (down_ref[rows:, :] + far_down_ref[...].astype(F32)).astype(BF16)


def sum_body(own_ref, below_ref, above_ref, out_ref):
    total = own_ref[...] + below_ref[...].astype(F32) + above_ref[...].astype(F32)
    out_ref[...] = total.astype(BF16)


def ring(axis, shift):
    length = lax.axis_size(axis)
    return [(i, (i + shift) % length) for i in range(length)]


def shards(queries, key_vectors, values, log_gate, out_gate, norm_gain, out_weight):
    length = queries.shape[0]
    pieces = lax.axis_size(CHIPS)
    half = DV // 2
    rows = half // pieces
    shape = jax.ShapeDtypeStruct
    small = shape((8, LANE), F32)
    own, own_log, swap = call(
        state_body,
        (shape((DV, LANE), F32), small, shape((DV + 16, LANE), BF16)),
        key_vectors,
        values,
        log_gate,
        fetched=(0, 1, 2),
    )
    swapped = lax.ppermute(swap, "core", ring("core", 1))
    sent, first, decay = call(
        join_body,
        (shape((pieces, 2 * rows + 8, LANE), BF16), shape((DV, LANE), F32), small),
        own,
        own_log,
        swapped,
    )
    slices = lax.all_to_all(sent, CHIPS, 0, 0, tiled=True)
    att_local, q_start, scale = call(
        local_body,
        (shape((length, DV), F32), shape((length, DK), BF16), shape((length, DV), F32)),
        queries,
        key_vectors,
        values,
        log_gate,
        out_gate,
        norm_gain.reshape(1, DV),
        fetched=(0, 1, 2, 3, 4),
    )
    prefixes = call(scan_body, shape((pieces, 2 * rows, LANE), BF16), slices)
    entering = lax.all_to_all(prefixes, CHIPS, 0, 0, tiled=True)
    state_half = shape((DV, LANE), BF16)
    keep, send = call(part_body, (state_half, state_half), entering, first, decay)
    other = lax.ppermute(send, "core", ring("core", 1))
    width = out_weight.shape[1] // lax.axis_size("head")
    near = shape((length // 2, width), BF16)
    gated, far_a, far_b = call(
        finish_body,
        (shape((length, DV), BF16), near, near),
        keep,
        other,
        q_start,
        att_local,
        scale,
        out_weight,
        fetched=(5,),
    )
    far_up = lax.ppermute(far_a, "head", ring("head", 1))
    far_down = lax.ppermute(far_b, "head", ring("head", -1))
    block = shape((length, width), F32)
    up, down, own_part = call(near_body, (block, block, block), gated, out_weight, fetched=(1,))
    block = shape((length, width), BF16)
    to_up, to_down = call(pass_body, (block, block), up, down, far_up, far_down)
    below = lax.ppermute(to_up, "head", ring("head", 1))
    above = lax.ppermute(to_down, "head", ring("head", -1))
    return call(sum_body, block, own_part, below, above)


def solution(mesh):
    split = Mesh(mesh.devices.reshape(4, 8, 2, mesh.shape["head"]), (*SEQ, "head"))
    in_specs = (
        P(SEQ, "head"),
        P(SEQ, "head"),
        P(SEQ, "head"),
        P(SEQ, "head"),
        P(SEQ, "head"),
        P("head"),
        P("head", None),
    )
    out_specs = P(SEQ, "head")
    return jax.shard_map(
        shards, mesh=split, in_specs=in_specs, out_specs=out_specs, check_vma=False
    )
```

```python
import jax
import jax.numpy as jnp
from jax import lax
from jax.experimental import pallas as pl
from jax.experimental.pallas import tpu as pltpu
from jax.sharding import Mesh
from jax.sharding import PartitionSpec as P

DK = 256
DV = 512
SPAN = 64
LANE = 128
SEQ = ("chip_x", "chip_z", "core")
CHIPS = ("chip_x", "chip_z")
F32 = jnp.float32
BF16 = jnp.bfloat16
VMEM = pl.BlockSpec(memory_space=pltpu.VMEM)
HBM = pl.BlockSpec(memory_space=pltpu.HBM)


def call(body, outs, *args, fetched=(), pieces=0, flops=10**9):
    moved = sum(a.size * a.dtype.itemsize for a in args)
    args = [
        pltpu.with_memory_space_constraint(a, pltpu.HBM) if i in fetched else a
        for i, a in enumerate(args)
    ]
    scratch = [pltpu.VMEM(args[i].shape, args[i].dtype) for i in fetched]
    if pieces:
        scratch = [pltpu.VMEM((pieces, DV, DV), BF16)]
    if fetched:
        scratch.append(pltpu.SemaphoreType.DMA((max(pieces, len(fetched)),)))
    return pl.pallas_call(
        body,
        out_shape=outs,
        in_specs=[HBM if i in fetched else VMEM for i in range(len(args))],
        out_specs=jax.tree.map(lambda _: VMEM, outs),
        scratch_shapes=scratch,
        cost_estimate=pl.CostEstimate(flops=flops, transcendentals=0, bytes_accessed=moved),
        compiler_params=pltpu.CompilerParams(vmem_limit_bytes=16 * 2**20),
    )(*args)


def dot(a, b, dims=((1,), (0,))):
    return lax.dot_general(a, b, (dims, ((), ())), preferred_element_type=F32)


def triangle(length, keep):
    row = lax.broadcasted_iota(jnp.int32, (length, length), 0)
    col = lax.broadcasted_iota(jnp.int32, (length, length), 1)
    return jnp.where(keep(row, col), 1.0, 0.0).astype(BF16)


def stacked(*parts):
    row = lax.broadcasted_iota(jnp.int32, (8, LANE), 0)
    block = jnp.zeros((8, LANE), F32)
    for at, part in enumerate(parts):
        block = jnp.where(row == at, part, block)
    return block


def split_bf16(values):
    high = values.astype(BF16).astype(F32)
    return high, values - high


def state_body(k_hbm, v_hbm, g_hbm, own_ref, log_ref, swap_ref, k_ref, v_ref, g_ref, sems):
    copies = [
        pltpu.make_async_copy(src, dst, sems.at[i])
        for i, (src, dst) in enumerate(((g_hbm, g_ref), (k_hbm, k_ref), (v_hbm, v_ref)))
    ]
    for copy in copies:
        copy.start()
    length = k_ref.shape[0]
    half = DV // 2
    mask = triangle(length, lambda r, c: c > r)
    copies[0].wait()
    gate = g_ref[...]
    after = dot(mask, gate)
    total = after[0:1] + gate[0:1].astype(F32)
    copies[1].wait()
    k_state = (k_ref[...].astype(F32) * jnp.exp(after)).astype(BF16)
    copies[2].wait()
    core = lax.axis_index("core")
    theirs = pl.ds(pl.multiple_of((1 - core) * half, half), half)
    state = dot(v_ref[:, theirs], k_state, ((0,), (0,))).astype(BF16)
    swap_ref[0:half, :] = state[:, :LANE]
    swap_ref[half : 2 * half, :] = state[:, LANE:]
    left_high, left_low = split_bf16(total[:, :LANE])
    right_high, right_low = split_bf16(total[:, LANE:])
    tail = stacked(left_high, right_high, left_low, right_low)
    swap_ref[2 * half :, :] = jnp.concatenate([tail, tail], axis=0).astype(BF16)
    mine = pl.ds(pl.multiple_of(core * half, half), half)
    state = dot(v_ref[:, mine], k_state, ((0,), (0,)))
    own_ref[0:half, :] = state[:, :LANE]
    own_ref[half:, :] = state[:, LANE:]
    log_ref[...] = stacked(total[:, :LANE], total[:, LANE:])


def join_body(own_ref, log_ref, swap_ref, out_ref, first_ref, decay_ref):
    pieces, rows = (out_ref.shape[0], (out_ref.shape[1] - 8) // 2)
    half = pieces * rows
    early = lax.axis_index("core") == 0
    tail = swap_ref[2 * half : 2 * half + 8, :].astype(F32)
    sums = []
    decays = []
    for side in range(2):
        at = slice(side * half, (side + 1) * half)
        own_log = log_ref[side : side + 1, :]
        other_log = tail[side : side + 1] + tail[side + 2 : side + 3]
        own = own_ref[at, :]
        other = swap_ref[at, :].astype(F32)
        first = jnp.where(early, own, other)
        second = jnp.where(early, other, own)
        state = first * jnp.exp(jnp.where(early, other_log, own_log)) + second
        first_ref[at, :] = first.astype(BF16)
        decays.append(jnp.exp(jnp.where(early, own_log, other_log)))
        sums.append(own_log + other_log)
        piece = slice(side * rows, (side + 1) * rows)
        out_ref[:, piece, :] = state.reshape(pieces, rows, LANE).astype(BF16)
    decay_ref[...] = stacked(*decays)
    left_high, left_low = split_bf16(sums[0])
    right_high, right_low = split_bf16(sums[1])
    tail = stacked(left_high, right_high, left_low, right_low)
    out_ref[:, 2 * rows :, :] = jnp.broadcast_to(tail[None], (pieces, 8, LANE)).astype(BF16)


def scan_body(in_ref, out_ref):
    pieces, rows = (in_ref.shape[0], out_ref.shape[1] // 2)
    left = right = jnp.zeros((rows, LANE), F32)
    for j in range(pieces):
        out_ref[j, 0:rows, :] = left.astype(BF16)
        out_ref[j, rows : 2 * rows, :] = right.astype(BF16)
        tail = in_ref[j, 2 * rows :, :].astype(F32)
        left = left * jnp.exp(tail[0:1] + tail[2:3]) + in_ref[j, 0:rows, :].astype(F32)
        right = right * jnp.exp(tail[1:2] + tail[3:4]) + in_ref[j, rows : 2 * rows, :].astype(F32)


def part_body(in_ref, first_ref, decay_ref, keep_ref, send_ref):
    pieces, rows = (in_ref.shape[0], in_ref.shape[1] // 2)
    half = pieces * rows
    early = lax.axis_index("core") == 0
    for side in range(2):
        at = slice(side * half, (side + 1) * half)
        piece = slice(side * rows, (side + 1) * rows)
        entering = in_ref[:, piece, :].astype(F32).reshape(half, LANE)
        between = entering * decay_ref[side : side + 1, :] + first_ref[at, :].astype(F32)
        keep_ref[at, :] = jnp.where(early, entering, between).astype(BF16)
        send_ref[at, :] = jnp.where(early, between, entering).astype(BF16)


def local_body(
    q_hbm, k_hbm, v_hbm, g_hbm, outer_hbm, gain_ref, att_ref, start_ref, scale_ref,
    q_ref, k_ref, v_ref, g_ref, outer_ref, sems,
):
    pairs = ((g_hbm, g_ref), (q_hbm, q_ref), (k_hbm, k_ref), (v_hbm, v_ref), (outer_hbm, outer_ref))
    copies = [pltpu.make_async_copy(src, dst, sems.at[i]) for i, (src, dst) in enumerate(pairs)]
    for copy in copies:
        copy.start()
    length = q_ref.shape[0]
    lower = triangle(SPAN, lambda r, c: c <= r)
    row = lax.broadcasted_iota(jnp.int32, (SPAN, SPAN), 0)
    col = lax.broadcasted_iota(jnp.int32, (SPAN, SPAN), 1)
    for copy in copies:
        copy.wait()
    carried = None
    before = jnp.zeros((1, DK), F32)
    for i in range(length // SPAN):
        at = slice(i * SPAN, (i + 1) * SPAN)
        running = dot(lower, g_ref[at, :])
        middle = running[SPAN // 2 : SPAN // 2 + 1]
        ending = running[SPAN - 1 : SPAN]
        query_f = q_ref[at, :].astype(F32)
        key_f = k_ref[at, :].astype(F32)
        value = v_ref[at, :]
        q_inter = query_f * jnp.exp(running)
        q_intra = (query_f * jnp.exp(running - middle)).astype(BF16)
        k_intra = (key_f * jnp.exp(middle - running)).astype(BF16)
        scores = dot(q_intra, k_intra, ((1,), (1,)))
        weights = jnp.where(col <= row, scores, 0.0).astype(BF16)
        attention = dot(weights, value)
        if i:
            attention = attention + dot(q_inter.astype(BF16), carried.astype(BF16))
        att_ref[at, :] = attention
        start_ref[at, :] = (query_f * jnp.exp(running + before)).astype(BF16)
        before = before + ending
        if (i + 1) * SPAN < length:
            k_state = (key_f * jnp.exp(ending - running)).T.astype(BF16)
            block = dot(k_state, value)
            carried = block if i == 0 else carried * jnp.exp(ending).reshape(DK, 1) + block
        outer_f = outer_ref[at, :].astype(F32)
        scale = outer_f / (1.0 + jnp.exp(-outer_f)) * gain_ref[...]
        scale_ref[at, :] = scale.astype(BF16)


def columns(index, width):
    return pl.ds(pl.multiple_of(index * width, width), width)


def head_columns(shift, width):
    count = lax.axis_size("head")
    return columns(lax.rem(lax.axis_index("head") + shift, count), width)


def fetch_columns(w_hbm, w_ref, sems, *shifts):
    width = w_ref.shape[-1]
    copies = [
        pltpu.make_async_copy(w_hbm.at[:, head_columns(shift, width)], w_ref.at[i], sems.at[i])
        for i, shift in enumerate(shifts)
    ]
    for copy in copies:
        copy.start()
    return copies


def finish_body(
    keep_ref, other_ref, q_ref, att_ref, scale_ref, w_hbm, gated_ref, far_up_ref, far_down_ref,
    w_ref, sems,
):
    (copy,) = fetch_columns(w_hbm, w_ref, sems, 2)
    half = DV // 2
    core = lax.axis_index("core")
    total = 0.0
    parts = []
    for ref, place in ((keep_ref, core), (other_ref, 1 - core)):
        attention = att_ref[:, columns(place, half)]
        attention = attention + dot(q_ref[:, :LANE], ref[:half, :], ((1,), (1,)))
        attention = attention + dot(q_ref[:, LANE:], ref[half:, :], ((1,), (1,)))
        total = total + jnp.sum(attention * attention, axis=-1, keepdims=True)
        parts.append((attention, place))
    inverse = lax.rsqrt(total * (1.0 / DV) + 1e-05)
    for attention, place in parts:
        at = columns(place, half)
        scale = scale_ref[:, at].astype(F32)
        gated_ref[:, at] = (attention * inverse * scale).astype(BF16)
    rows = far_up_ref.shape[0]
    copy.wait()
    far_up_ref[...] = dot(gated_ref[:rows, :], w_ref[0]).astype(BF16)
    far_down_ref[...] = dot(gated_ref[rows:, :], w_ref[0]).astype(BF16)


def direct_body(gated_ref, w_hbm, up_ref, down_ref, w_ref, sems):
    copies = fetch_columns(w_hbm, w_ref, sems, 1, 3)
    rows = up_ref.shape[0]
    copies[0].wait()
    up_ref[...] = dot(gated_ref[rows:, :], w_ref[0]).astype(BF16)
    copies[1].wait()
    down_ref[...] = dot(gated_ref[:rows, :], w_ref[1]).astype(BF16)


def near_body(gated_ref, w_hbm, up_ref, down_ref, own_ref, w_ref, sems):
    copies = fetch_columns(w_hbm, w_ref, sems, 1, 3, 0)
    rows = up_ref.shape[0]
    copies[0].wait()
    up_ref[...] = dot(gated_ref[:rows, :], w_ref[0])
    copies[1].wait()
    down_ref[...] = dot(gated_ref[rows:, :], w_ref[1])
    copies[2].wait()
    own_ref[...] = dot(gated_ref[...], w_ref[2])


def pass_body(up_ref, down_ref, far_up_ref, far_down_ref, up_out_ref, down_out_ref):
    up_out_ref[...] = (up_ref[...] + far_up_ref[...].astype(F32)).astype(BF16)
    down_out_ref[...] = (down_ref[...] + far_down_ref[...].astype(F32)).astype(BF16)


def sum_body(own_ref, below_a_ref, below_b_ref, above_a_ref, above_b_ref, out_ref):
    rows = below_a_ref.shape[0]
    for at, below, above in (
        (slice(0, rows), below_a_ref, above_a_ref),
        (slice(rows, 2 * rows), below_b_ref, above_b_ref),
    ):
        total = own_ref[at, :] + below[...].astype(F32) + above[...].astype(F32)
        out_ref[at, :] = total.astype(BF16)


def ring(axis, shift):
    length = lax.axis_size(axis)
    return [(i, (i + shift) % length) for i in range(length)]


def shards(queries, key_vectors, values, log_gate, out_gate, norm_gain, out_weight):
    length = queries.shape[0]
    pieces = lax.axis_size(CHIPS)
    half = DV // 2
    rows = half // pieces
    shape = jax.ShapeDtypeStruct
    small = shape((8, LANE), F32)
    own, own_log, swap = call(
        state_body,
        (shape((DV, LANE), F32), small, shape((DV + 16, LANE), BF16)),
        key_vectors,
        values,
        log_gate,
        fetched=(0, 1, 2),
    )
    swapped = lax.ppermute(swap, "core", ring("core", 1))
    sent, first, decay = call(
        join_body,
        (shape((pieces, 2 * rows + 8, LANE), BF16), shape((DV, LANE), BF16), small),
        own,
        own_log,
        swapped,
    )
    slices = lax.all_to_all(sent, CHIPS, 0, 0, tiled=True)
    att_local, q_start, scale = call(
        local_body,
        (shape((length, DV), F32), shape((length, DK), BF16), shape((length, DV), BF16)),
        queries,
        key_vectors,
        values,
        log_gate,
        out_gate,
        norm_gain.reshape(1, DV),
        fetched=(0, 1, 2, 3, 4),
    )
    prefixes = call(scan_body, shape((pieces, 2 * rows, LANE), BF16), slices)
    entering = lax.all_to_all(prefixes, CHIPS, 0, 0, tiled=True)
    state_half = shape((DV, LANE), BF16)
    entering, att_local, q_start, scale = lax.optimization_barrier(
        (entering, att_local, q_start, scale)
    )
    keep, send = call(part_body, (state_half, state_half), entering, first, decay)
    other = lax.ppermute(send, "core", ring("core", 1))
    width = out_weight.shape[1] // lax.axis_size("head")
    near = shape((length // 2, width), BF16)
    near_f = shape((length // 2, width), F32)
    gated, far_up, far_down = call(
        finish_body,
        (shape((length, DV), BF16), near, near),
        keep,
        other,
        q_start,
        att_local,
        scale,
        out_weight,
        fetched=(5,),
        pieces=1,
    )
    up, down = ring("head", 1), ring("head", -1)
    far_up = lax.ppermute(far_up, "head", up)
    far_down = lax.ppermute(far_down, "head", down)
    up_b, down_a = call(
        direct_body, (near, near), gated, out_weight, fetched=(1,), pieces=2
    )
    below_b = lax.ppermute(up_b, "head", up)
    above_a = lax.ppermute(down_a, "head", down)
    up_a, down_b, own_part = call(
        near_body,
        (near_f, near_f, shape((length, width), F32)),
        gated,
        out_weight,
        fetched=(1,),
        pieces=3,
    )
    up_a, down_b = call(pass_body, (near, near), up_a, down_b, far_up, far_down)
    below_a = lax.ppermute(up_a, "head", up)
    above_b = lax.ppermute(down_b, "head", down)
    return call(
        sum_body, shape((length, width), BF16), own_part, below_a, below_b, above_a, above_b
    )


def solution(mesh):
    split = Mesh(mesh.devices.reshape(4, 8, 2, mesh.shape["head"]), (*SEQ, "head"))
    in_specs = (
        P(SEQ, "head"),
        P(SEQ, "head"),
        P(SEQ, "head"),
        P(SEQ, "head"),
        P(SEQ, "head"),
        P("head"),
        P("head", None),
    )
    out_specs = P(SEQ, "head")
    return jax.shard_map(
        shards, mesh=split, in_specs=in_specs, out_specs=out_specs, check_vma=False
    )
```

```python
import jax
import jax.numpy as jnp
from jax import lax
from jax.experimental import pallas as pl
from jax.experimental.pallas import tpu as pltpu
from jax.sharding import Mesh
from jax.sharding import PartitionSpec as P


DK = 256
DV = 512
SPAN = 64
LANE = 128
SEQ = ("chip_x", "chip_z", "core")
CHIPS = ("chip_x", "chip_z")
F32 = jnp.float32
BF16 = jnp.bfloat16
VMEM = pl.BlockSpec(memory_space=pltpu.VMEM)
HBM = pl.BlockSpec(memory_space=pltpu.HBM)


def call(body, outs, *args, fetched=(), scratch=(), copies=0, outs_in=VMEM):
    moved = sum(a.size * a.dtype.itemsize for a in args)
    args = [
        pltpu.with_memory_space_constraint(a, pltpu.HBM) if i in fetched else a
        for i, a in enumerate(args)
    ]
    if fetched and not copies:
        scratch = [pltpu.VMEM(args[i].shape, args[i].dtype) for i in fetched]
        copies = len(fetched)
    if copies:
        scratch = [*scratch, pltpu.SemaphoreType.DMA((copies,))]
    return pl.pallas_call(
        body,
        out_shape=outs,
        in_specs=[HBM if i in fetched else VMEM for i in range(len(args))],
        out_specs=jax.tree.map(lambda _: outs_in, outs),
        scratch_shapes=scratch,
        cost_estimate=pl.CostEstimate(flops=10**9, transcendentals=0, bytes_accessed=moved),
        compiler_params=pltpu.CompilerParams(vmem_limit_bytes=16 * 2**20),
    )(*args)


def dot(a, b, dims=((1,), (0,))):
    return lax.dot_general(a, b, (dims, ((), ())), preferred_element_type=F32)


def triangle(length, keep):
    row = lax.broadcasted_iota(jnp.int32, (length, length), 0)
    col = lax.broadcasted_iota(jnp.int32, (length, length), 1)
    return jnp.where(keep(row, col), 1.0, 0.0).astype(BF16)


def stacked(*parts):
    row = lax.broadcasted_iota(jnp.int32, (8, LANE), 0)
    block = jnp.zeros((8, LANE), F32)
    for at, part in enumerate(parts):
        block = jnp.where(row == at, part, block)
    return block


def split_bf16(values):
    high = values.astype(BF16).astype(F32)
    return high, values - high


def fetch(sems, *pairs):
    copies = [pltpu.make_async_copy(src, dst, sems.at[i]) for i, (src, dst) in enumerate(pairs)]
    for copy in copies:
        copy.start()
    return copies


def columns(index, width):
    return pl.ds(pl.multiple_of(index * width, width), width)


def head_columns(shift, width):
    count = lax.axis_size("head")
    return columns(lax.rem(lax.axis_index("head") + shift, count), width)


def swap_body(k_hbm, v_hbm, g_hbm, swap_ref, log_ref, state_ref, k_ref, v_ref, g_ref, sems):
    gate_copy, k_copy, v_copy = fetch(sems, (g_hbm, g_ref), (k_hbm, k_ref), (v_hbm, v_ref))
    length = k_ref.shape[0]
    half = DV // 2
    mask = triangle(length, lambda r, c: c > r)
    gate_copy.wait()
    gate = g_ref[...]
    after = dot(mask, gate)
    total = after[0:1] + gate[0:1].astype(F32)
    k_copy.wait()
    k_state = (k_ref[...].astype(F32) * jnp.exp(after)).astype(BF16)
    state_ref[...] = k_state
    v_copy.wait()
    theirs = columns(1 - lax.axis_index("core"), half)
    state = dot(v_ref[:, theirs], k_state, ((0,), (0,))).astype(BF16)
    swap_ref[0:half, :] = state[:, :LANE]
    swap_ref[half : 2 * half, :] = state[:, LANE:]
    left_high, left_low = split_bf16(total[:, :LANE])
    right_high, right_low = split_bf16(total[:, LANE:])
    tail = stacked(left_high, right_high, left_low, right_low)
    swap_ref[2 * half :, :] = jnp.concatenate([tail, tail], axis=0).astype(BF16)
    log_ref[...] = stacked(total[:, :LANE], total[:, LANE:])


def own_body(v_hbm, state_ref, own_ref, v_ref, sems):
    (copy,) = fetch(sems, (v_hbm, v_ref))
    copy.wait()
    half = DV // 2
    mine = columns(lax.axis_index("core"), half)
    state = dot(v_ref[:, mine], state_ref[...], ((0,), (0,)))
    own_ref[0:half, :] = state[:, :LANE]
    own_ref[half:, :] = state[:, LANE:]


def join_body(own_ref, log_ref, swap_ref, out_ref, first_ref, decay_ref):
    pieces, rows = (out_ref.shape[0], (out_ref.shape[1] - 8) // 2)
    half = pieces * rows
    early = lax.axis_index("core") == 0
    tail = swap_ref[2 * half : 2 * half + 8, :].astype(F32)
    sums = []
    decays = []
    for side in range(2):
        at = slice(side * half, (side + 1) * half)
        own_log = log_ref[side : side + 1, :]
        other_log = tail[side : side + 1] + tail[side + 2 : side + 3]
        own = own_ref[at, :]
        other = swap_ref[at, :].astype(F32)
        first = jnp.where(early, own, other)
        second = jnp.where(early, other, own)
        state = first * jnp.exp(jnp.where(early, other_log, own_log)) + second
        first_ref[at, :] = first.astype(BF16)
        decays.append(jnp.exp(jnp.where(early, own_log, other_log)))
        sums.append(own_log + other_log)
        piece = slice(side * rows, (side + 1) * rows)
        out_ref[:, piece, :] = state.reshape(pieces, rows, LANE).astype(BF16)
    decay_ref[...] = stacked(*decays)
    left_high, left_low = split_bf16(sums[0])
    right_high, right_low = split_bf16(sums[1])
    tail = stacked(left_high, right_high, left_low, right_low)
    out_ref[:, 2 * rows :, :] = jnp.broadcast_to(tail[None], (pieces, 8, LANE)).astype(BF16)


def scan_body(in_ref, out_ref):
    pieces, rows = (in_ref.shape[0], out_ref.shape[1] // 2)
    left = right = jnp.zeros((rows, LANE), F32)
    for j in range(pieces):
        out_ref[j, 0:rows, :] = left.astype(BF16)
        out_ref[j, rows : 2 * rows, :] = right.astype(BF16)
        tail = in_ref[j, 2 * rows :, :].astype(F32)
        left = left * jnp.exp(tail[0:1] + tail[2:3]) + in_ref[j, 0:rows, :].astype(F32)
        right = right * jnp.exp(tail[1:2] + tail[3:4]) + in_ref[j, rows : 2 * rows, :].astype(F32)


def part_body(in_ref, first_ref, decay_ref, keep_ref, send_ref):
    pieces, rows = (in_ref.shape[0], in_ref.shape[1] // 2)
    half = pieces * rows
    early = lax.axis_index("core") == 0
    for side in range(2):
        at = slice(side * half, (side + 1) * half)
        piece = slice(side * rows, (side + 1) * rows)
        entering = in_ref[:, piece, :].astype(F32).reshape(half, LANE)
        between = entering * decay_ref[side : side + 1, :] + first_ref[at, :].astype(F32)
        keep_ref[at, :] = jnp.where(early, entering, between).astype(BF16)
        send_ref[at, :] = jnp.where(early, between, entering).astype(BF16)


def local_body(
    q_hbm, k_hbm, v_hbm, g_hbm, outer_hbm, gain_ref, att_ref, start_ref, scale_ref,
    q_ref, k_ref, v_ref, g_ref, outer_ref, sems,
):
    copies = fetch(
        sems, (g_hbm, g_ref), (q_hbm, q_ref), (k_hbm, k_ref), (v_hbm, v_ref), (outer_hbm, outer_ref)
    )
    length = q_ref.shape[0]
    lower = triangle(SPAN, lambda r, c: c <= r)
    row = lax.broadcasted_iota(jnp.int32, (SPAN, SPAN), 0)
    col = lax.broadcasted_iota(jnp.int32, (SPAN, SPAN), 1)
    for copy in copies:
        copy.wait()
    carried = None
    before = jnp.zeros((1, DK), F32)
    for i in range(length // SPAN):
        at = slice(i * SPAN, (i + 1) * SPAN)
        running = dot(lower, g_ref[at, :])
        middle = running[SPAN // 2 : SPAN // 2 + 1]
        ending = running[SPAN - 1 : SPAN]
        query_f = q_ref[at, :].astype(F32)
        key_f = k_ref[at, :].astype(F32)
        value = v_ref[at, :]
        q_inter = query_f * jnp.exp(running)
        q_intra = (query_f * jnp.exp(running - middle)).astype(BF16)
        k_intra = (key_f * jnp.exp(middle - running)).astype(BF16)
        scores = dot(q_intra, k_intra, ((1,), (1,)))
        weights = jnp.where(col <= row, scores, 0.0).astype(BF16)
        attention = dot(weights, value)
        if i:
            attention = attention + dot(q_inter.astype(BF16), carried.astype(BF16))
        att_ref[at, :] = attention
        start_ref[at, :] = (query_f * jnp.exp(running + before)).astype(BF16)
        before = before + ending
        if (i + 1) * SPAN < length:
            k_state = (key_f * jnp.exp(ending - running)).T.astype(BF16)
            block = dot(k_state, value)
            carried = block if i == 0 else carried * jnp.exp(ending).reshape(DK, 1) + block
        outer_f = outer_ref[at, :].astype(F32)
        scale = outer_f / (1.0 + jnp.exp(-outer_f)) * gain_ref[...]
        scale_ref[at, :] = scale.astype(BF16)


def finish_body(keep_ref, other_ref, q_ref, att_ref, scale_ref, top_ref, low_ref):
    half = DV // 2
    core = lax.axis_index("core")
    total = 0.0
    parts = []
    for ref, place in ((keep_ref, core), (other_ref, 1 - core)):
        attention = att_ref[:, columns(place, half)]
        attention = attention + dot(q_ref[:, :LANE], ref[:half, :], ((1,), (1,)))
        attention = attention + dot(q_ref[:, LANE:], ref[half:, :], ((1,), (1,)))
        total = total + jnp.sum(attention * attention, axis=-1, keepdims=True)
        parts.append((attention, place))
    inverse = lax.rsqrt(total * (1.0 / DV) + 1e-05)
    rows = top_ref.shape[0]
    for attention, place in parts:
        at = columns(place, half)
        gated = (attention * inverse * scale_ref[:, at].astype(F32)).astype(BF16)
        top_ref[:, at] = gated[:rows]
        low_ref[:, at] = gated[rows:]


def weights_body(w_hbm, *refs):
    out_refs, sems = (refs[:-1], refs[-1])
    width = out_refs[0].shape[1]
    for copy in fetch(
        sems,
        *((w_hbm.at[:, head_columns(i + 1, width)], ref) for i, ref in enumerate(out_refs)),
    ):
        copy.wait()


def own_part_body(top_ref, low_ref, w_hbm, out_ref, w_ref, sems):
    (copy,) = fetch(sems, (w_hbm.at[:, head_columns(0, w_ref.shape[1])], w_ref))
    copy.wait()
    rows = top_ref.shape[0]
    out_ref[:rows, :] = dot(top_ref[...], w_ref[...])
    out_ref[rows:, :] = dot(low_ref[...], w_ref[...])


def near_part_body(
    part_ref, below_top_ref, below_low_ref, above_top_ref, above_low_ref,
    w_below_hbm, w_above_hbm, out_ref, w_below_ref, w_above_ref, sems,
):
    below_copy, above_copy = fetch(sems, (w_below_hbm, w_below_ref), (w_above_hbm, w_above_ref))
    below_copy.wait()
    above_copy.wait()
    rows = below_top_ref.shape[0]
    for at, below, above in (
        (slice(0, rows), below_top_ref, above_top_ref),
        (slice(rows, 2 * rows), below_low_ref, above_low_ref),
    ):
        total = part_ref[at, :] + dot(below[...], w_below_ref[...])
        out_ref[at, :] = total + dot(above[...], w_above_ref[...])


def sum_body(part_ref, far_top_ref, far_low_ref, w_ref, out_ref):
    rows = far_top_ref.shape[0]
    out_ref[:rows, :] = (part_ref[:rows, :] + dot(far_top_ref[...], w_ref[...])).astype(BF16)
    out_ref[rows:, :] = (part_ref[rows:, :] + dot(far_low_ref[...], w_ref[...])).astype(BF16)


def ring(axis, shift):
    length = lax.axis_size(axis)
    return [(i, (i + shift) % length) for i in range(length)]


def shards(queries, key_vectors, values, log_gate, out_gate, norm_gain, out_weight):
    length = queries.shape[0]
    pieces = lax.axis_size(CHIPS)
    half = DV // 2
    rows = half // pieces
    width = out_weight.shape[1] // lax.axis_size("head")
    shape = jax.ShapeDtypeStruct
    small = shape((8, LANE), F32)
    swap, own_log, k_state = call(
        swap_body,
        (shape((DV + 16, LANE), BF16), small, shape((length, DK), BF16)),
        key_vectors,
        values,
        log_gate,
        fetched=(0, 1, 2),
    )
    swapped = lax.ppermute(swap, "core", ring("core", 1))
    own = call(own_body, shape((DV, LANE), F32), values, k_state, fetched=(0,))
    sent, first, decay = call(
        join_body,
        (shape((pieces, 2 * rows + 8, LANE), BF16), shape((DV, LANE), BF16), small),
        own,
        own_log,
        swapped,
    )
    sent, later_weight = lax.optimization_barrier((sent, out_weight))
    slices = lax.all_to_all(sent, CHIPS, 0, 0, tiled=True)
    blocks = call(
        weights_body,
        tuple(pltpu.HBM((DV, width), BF16) for _ in range(3)),
        later_weight,
        fetched=(0,),
        copies=3,
        outs_in=HBM,
    )
    up, down = ring("head", 1), ring("head", -1)
    w_below = lax.ppermute(blocks[0], "head", up)
    w_far = lax.ppermute(blocks[1], "head", ring("head", 2))
    w_above = lax.ppermute(blocks[2], "head", down)
    prefixes = call(scan_body, shape((pieces, 2 * rows, LANE), BF16), slices)
    prefixes, queries = lax.optimization_barrier((prefixes, queries))
    att_local, q_start, scale = call(
        local_body,
        (shape((length, DV), F32), shape((length, DK), BF16), shape((length, DV), BF16)),
        queries,
        key_vectors,
        values,
        log_gate,
        out_gate,
        norm_gain.reshape(1, DV),
        fetched=(0, 1, 2, 3, 4),
    )
    entering = lax.all_to_all(prefixes, CHIPS, 0, 0, tiled=True)
    state_half = shape((DV, LANE), BF16)
    entering, att_local, q_start, scale = lax.optimization_barrier(
        (entering, att_local, q_start, scale)
    )
    keep, send = call(part_body, (state_half, state_half), entering, first, decay)
    other = lax.ppermute(send, "core", ring("core", 1))
    near = shape((length // 2, DV), BF16)
    top, low = call(finish_body, (near, near), keep, other, q_start, att_local, scale)
    below_top = lax.ppermute(top, "head", up)
    above_low = lax.ppermute(low, "head", down)
    below_low = lax.ppermute(low, "head", up)
    above_top = lax.ppermute(top, "head", down)
    whole = shape((length, width), F32)
    part = call(
        own_part_body,
        whole,
        top,
        low,
        out_weight,
        fetched=(2,),
        scratch=[pltpu.VMEM((DV, width), BF16)],
        copies=1,
    )
    far_top = lax.ppermute(below_top, "head", up)
    far_low = lax.ppermute(above_low, "head", down)
    part = call(
        near_part_body,
        whole,
        part,
        below_top,
        below_low,
        above_top,
        above_low,
        w_below,
        w_above,
        fetched=(5, 6),
    )
    return call(sum_body, shape((length, width), BF16), part, far_top, far_low, w_far)


def solution(mesh):
    split = Mesh(mesh.devices.reshape(4, 8, 2, mesh.shape["head"]), (*SEQ, "head"))
    in_specs = (
        P(SEQ, "head"),
        P(SEQ, "head"),
        P(SEQ, "head"),
        P(SEQ, "head"),
        P(SEQ, "head"),
        P("head"),
        P("head", None),
    )
    out_specs = P(SEQ, "head")


    return jax.shard_map(
        shards, mesh=split, in_specs=in_specs, out_specs=out_specs, check_vma=False
    )
```

```python
import jax
import jax.numpy as jnp
from jax import lax
from jax.experimental import pallas as pl
from jax.experimental.pallas import tpu as pltpu
from jax.sharding import Mesh
from jax.sharding import PartitionSpec as P


DK = 256
DV = 512
SPAN = 64
LANE = 128
SEQ = ("chip_x", "chip_z", "core")
CHIPS = ("chip_x", "chip_z")
F32 = jnp.float32
BF16 = jnp.bfloat16
VMEM = pl.BlockSpec(memory_space=pltpu.VMEM)
HBM = pl.BlockSpec(memory_space=pltpu.HBM)


def call(body, outs, *args, fetched=(), scratch=(), copies=0, outs_in=VMEM):
    moved = sum(a.size * a.dtype.itemsize for a in args)
    args = [
        pltpu.with_memory_space_constraint(a, pltpu.HBM) if i in fetched else a
        for i, a in enumerate(args)
    ]
    if fetched and not copies:
        scratch = [pltpu.VMEM(args[i].shape, args[i].dtype) for i in fetched]
        copies = len(fetched)
    if copies:
        scratch = [*scratch, pltpu.SemaphoreType.DMA((copies,))]
    return pl.pallas_call(
        body,
        out_shape=outs,
        in_specs=[HBM if i in fetched else VMEM for i in range(len(args))],
        out_specs=jax.tree.map(lambda _: outs_in, outs),
        scratch_shapes=scratch,
        cost_estimate=pl.CostEstimate(flops=10**9, transcendentals=0, bytes_accessed=moved),
        compiler_params=pltpu.CompilerParams(vmem_limit_bytes=16 * 2**20),
    )(*args)


def dot(a, b, dims=((1,), (0,))):
    return lax.dot_general(a, b, (dims, ((), ())), preferred_element_type=F32)


def triangle(length, keep):
    row = lax.broadcasted_iota(jnp.int32, (length, length), 0)
    col = lax.broadcasted_iota(jnp.int32, (length, length), 1)
    return jnp.where(keep(row, col), 1.0, 0.0).astype(BF16)


def stacked(*parts):
    row = lax.broadcasted_iota(jnp.int32, (8, LANE), 0)
    block = jnp.zeros((8, LANE), F32)
    for at, part in enumerate(parts):
        block = jnp.where(row == at, part, block)
    return block


def split_bf16(values):
    high = values.astype(BF16).astype(F32)
    return high, values - high


def fetch(sems, *pairs):
    copies = [pltpu.make_async_copy(src, dst, sems.at[i]) for i, (src, dst) in enumerate(pairs)]
    for copy in copies:
        copy.start()
    return copies


def columns(index, width):
    return pl.ds(pl.multiple_of(index * width, width), width)


def head_columns(shift, width):
    count = lax.axis_size("head")
    return columns(lax.rem(lax.axis_index("head") + shift, count), width)


def swap_body(k_hbm, v_hbm, g_hbm, swap_ref, log_ref, state_ref, k_ref, v_ref, g_ref, sems):
    gate_copy, k_copy, v_copy = fetch(sems, (g_hbm, g_ref), (k_hbm, k_ref), (v_hbm, v_ref))
    length = k_ref.shape[0]
    half = DV // 2
    mask = triangle(length, lambda r, c: c > r)
    gate_copy.wait()
    gate = g_ref[...]
    after = dot(mask, gate)
    total = after[0:1] + gate[0:1].astype(F32)
    k_copy.wait()
    k_state = (k_ref[...].astype(F32) * jnp.exp(after)).astype(BF16)
    state_ref[...] = k_state
    v_copy.wait()
    theirs = columns(1 - lax.axis_index("core"), half)
    state = dot(v_ref[:, theirs], k_state, ((0,), (0,))).astype(BF16)
    swap_ref[0:half, :] = state[:, :LANE]
    swap_ref[half : 2 * half, :] = state[:, LANE:]
    left_high, left_low = split_bf16(total[:, :LANE])
    right_high, right_low = split_bf16(total[:, LANE:])
    tail = stacked(left_high, right_high, left_low, right_low)
    swap_ref[2 * half :, :] = jnp.concatenate([tail, tail], axis=0).astype(BF16)
    log_ref[...] = stacked(total[:, :LANE], total[:, LANE:])


def own_body(v_hbm, state_ref, own_ref, v_ref, sems):
    (copy,) = fetch(sems, (v_hbm, v_ref))
    copy.wait()
    half = DV // 2
    mine = columns(lax.axis_index("core"), half)
    state = dot(v_ref[:, mine], state_ref[...], ((0,), (0,)))
    own_ref[0:half, :] = state[:, :LANE]
    own_ref[half:, :] = state[:, LANE:]


def join_body(own_ref, log_ref, swap_ref, out_ref, first_ref, decay_ref):
    pieces, rows = (out_ref.shape[0], (out_ref.shape[1] - 8) // 2)
    half = pieces * rows
    early = lax.axis_index("core") == 0
    tail = swap_ref[2 * half : 2 * half + 8, :].astype(F32)
    sums = []
    decays = []
    for side in range(2):
        at = slice(side * half, (side + 1) * half)
        own_log = log_ref[side : side + 1, :]
        other_log = tail[side : side + 1] + tail[side + 2 : side + 3]
        own = own_ref[at, :]
        other = swap_ref[at, :].astype(F32)
        first = jnp.where(early, own, other)
        second = jnp.where(early, other, own)
        state = first * jnp.exp(jnp.where(early, other_log, own_log)) + second
        first_ref[at, :] = first.astype(BF16)
        decays.append(jnp.exp(jnp.where(early, own_log, other_log)))
        sums.append(own_log + other_log)
        piece = slice(side * rows, (side + 1) * rows)
        out_ref[:, piece, :] = state.reshape(pieces, rows, LANE).astype(BF16)
    decay_ref[...] = stacked(*decays)
    left_high, left_low = split_bf16(sums[0])
    right_high, right_low = split_bf16(sums[1])
    tail = stacked(left_high, right_high, left_low, right_low)
    out_ref[:, 2 * rows :, :] = jnp.broadcast_to(tail[None], (pieces, 8, LANE)).astype(BF16)


def scan_body(in_ref, out_ref):
    pieces, rows = (in_ref.shape[0], out_ref.shape[1] // 2)
    left = right = jnp.zeros((rows, LANE), F32)
    for j in range(pieces):
        out_ref[j, 0:rows, :] = left.astype(BF16)
        out_ref[j, rows : 2 * rows, :] = right.astype(BF16)
        tail = in_ref[j, 2 * rows :, :].astype(F32)
        left = left * jnp.exp(tail[0:1] + tail[2:3]) + in_ref[j, 0:rows, :].astype(F32)
        right = right * jnp.exp(tail[1:2] + tail[3:4]) + in_ref[j, rows : 2 * rows, :].astype(F32)


def part_body(in_ref, first_ref, decay_ref, keep_ref, send_ref):
    pieces, rows = (in_ref.shape[0], in_ref.shape[1] // 2)
    half = pieces * rows
    early = lax.axis_index("core") == 0
    for side in range(2):
        at = slice(side * half, (side + 1) * half)
        piece = slice(side * rows, (side + 1) * rows)
        entering = in_ref[:, piece, :].astype(F32).reshape(half, LANE)
        between = entering * decay_ref[side : side + 1, :] + first_ref[at, :].astype(F32)
        keep_ref[at, :] = jnp.where(early, entering, between).astype(BF16)
        send_ref[at, :] = jnp.where(early, between, entering).astype(BF16)


def local_body(
    q_hbm, k_hbm, v_hbm, g_hbm, outer_hbm, w_hbm, gain_ref,
    att_ref, start_ref, scale_ref, w_ref, q_ref, k_ref, v_ref, g_ref, outer_ref, sems,
):
    far_columns = w_hbm.at[:, head_columns(2, w_ref.shape[1])]
    *copies, far_copy = fetch(
        sems,
        (g_hbm, g_ref),
        (q_hbm, q_ref),
        (k_hbm, k_ref),
        (v_hbm, v_ref),
        (outer_hbm, outer_ref),
        (far_columns, w_ref),
    )
    length = q_ref.shape[0]
    lower = triangle(SPAN, lambda r, c: c <= r)
    row = lax.broadcasted_iota(jnp.int32, (SPAN, SPAN), 0)
    col = lax.broadcasted_iota(jnp.int32, (SPAN, SPAN), 1)
    for copy in copies:
        copy.wait()
    carried = None
    before = jnp.zeros((1, DK), F32)
    for i in range(length // SPAN):
        at = slice(i * SPAN, (i + 1) * SPAN)
        running = dot(lower, g_ref[at, :])
        middle = running[SPAN // 2 : SPAN // 2 + 1]
        ending = running[SPAN - 1 : SPAN]
        query_f = q_ref[at, :].astype(F32)
        key_f = k_ref[at, :].astype(F32)
        value = v_ref[at, :]
        q_inter = query_f * jnp.exp(running)
        q_intra = (query_f * jnp.exp(running - middle)).astype(BF16)
        k_intra = (key_f * jnp.exp(middle - running)).astype(BF16)
        scores = dot(q_intra, k_intra, ((1,), (1,)))
        weights = jnp.where(col <= row, scores, 0.0).astype(BF16)
        attention = dot(weights, value)
        if i:
            attention = attention + dot(q_inter.astype(BF16), carried.astype(BF16))
        att_ref[at, :] = attention
        start_ref[at, :] = (query_f * jnp.exp(running + before)).astype(BF16)
        before = before + ending
        if (i + 1) * SPAN < length:
            k_state = (key_f * jnp.exp(ending - running)).T.astype(BF16)
            block = dot(k_state, value)
            carried = block if i == 0 else carried * jnp.exp(ending).reshape(DK, 1) + block
        outer_f = outer_ref[at, :].astype(F32)
        scale = outer_f / (1.0 + jnp.exp(-outer_f)) * gain_ref[...]
        scale_ref[at, :] = scale.astype(BF16)
    far_copy.wait()


def keep_body(keep_ref, q_ref, att_ref, out_ref, square_ref):
    half = keep_ref.shape[0] // 2
    attention = att_ref[:, columns(lax.axis_index("core"), half)]
    attention = attention + dot(q_ref[:, :LANE], keep_ref[:half, :], ((1,), (1,)))
    attention = attention + dot(q_ref[:, LANE:], keep_ref[half:, :], ((1,), (1,)))
    out_ref[...] = attention
    square_ref[...] = jnp.sum(attention * attention, axis=-1, keepdims=True)


def finish_body(
    other_ref, q_ref, att_ref, kept_ref, square_ref, scale_ref, w_ref,
    gated_ref, far_up_ref, far_down_ref,
):
    half = other_ref.shape[0] // 2
    core = lax.axis_index("core")
    here, there = columns(core, half), columns(1 - core, half)
    attention = att_ref[:, there]
    attention = attention + dot(q_ref[:, :LANE], other_ref[:half, :], ((1,), (1,)))
    attention = attention + dot(q_ref[:, LANE:], other_ref[half:, :], ((1,), (1,)))
    total = square_ref[...] + jnp.sum(attention * attention, axis=-1, keepdims=True)
    inverse = lax.rsqrt(total * (1.0 / DV) + 1e-05)
    gated_ref[:, there] = (attention * inverse * scale_ref[:, there].astype(F32)).astype(BF16)
    gated_ref[:, here] = (kept_ref[...] * inverse * scale_ref[:, here].astype(F32)).astype(BF16)
    split = far_up_ref.shape[0]
    far_up_ref[...] = dot(gated_ref[:split, :], w_ref[...]).astype(BF16)
    far_down_ref[...] = dot(gated_ref[split:, :], w_ref[...]).astype(BF16)


def fetch_columns(w_hbm, w_ref, sems, *shifts):
    width = w_ref.shape[-1]
    pairs = [(w_hbm.at[:, head_columns(s, width)], w_ref.at[i]) for i, s in enumerate(shifts)]
    return fetch(sems, *pairs)


def direct_body(gated_ref, w_hbm, up_ref, down_ref, w_ref, sems):
    copies = fetch_columns(w_hbm, w_ref, sems, 1, 3)
    length, split = (gated_ref.shape[0], down_ref.shape[0])
    copies[0].wait()
    up_ref[...] = dot(gated_ref[length - up_ref.shape[0] :, :], w_ref[0]).astype(BF16)
    copies[1].wait()
    down_ref[...] = dot(gated_ref[:split, :], w_ref[1]).astype(BF16)


def near_body(gated_ref, w_hbm, up_ref, down_ref, own_ref, w_ref, sems):
    copies = fetch_columns(w_hbm, w_ref, sems, 1, 3, 0)
    split = up_ref.shape[0]
    copies[0].wait()
    up_ref[...] = dot(gated_ref[:split, :], w_ref[0])
    copies[1].wait()
    down_ref[...] = dot(gated_ref[split:, :], w_ref[1])
    copies[2].wait()
    own_ref[...] = dot(gated_ref[...], w_ref[2])


def pass_body(up_ref, down_ref, far_up_ref, far_down_ref, up_out_ref, down_out_ref):
    up_out_ref[...] = (up_ref[...] + far_up_ref[...].astype(F32)).astype(BF16)
    down_out_ref[...] = (down_ref[...] + far_down_ref[...].astype(F32)).astype(BF16)


def sum_body(own_ref, below_a_ref, below_b_ref, above_a_ref, above_b_ref, out_ref):
    split = below_a_ref.shape[0]
    for at, below, above in (
        (slice(0, split), below_a_ref, above_a_ref),
        (slice(split, own_ref.shape[0]), below_b_ref, above_b_ref),
    ):
        total = own_ref[at, :] + below[...].astype(F32) + above[...].astype(F32)
        out_ref[at, :] = total.astype(BF16)


def ring(axis, shift):
    length = lax.axis_size(axis)
    return [(i, (i + shift) % length) for i in range(length)]


def shards(queries, key_vectors, values, log_gate, out_gate, norm_gain, out_weight):
    length = queries.shape[0]
    pieces = lax.axis_size(CHIPS)
    half = DV // 2
    rows = half // pieces
    width = out_weight.shape[1] // lax.axis_size("head")
    shape = jax.ShapeDtypeStruct
    small = shape((8, LANE), F32)
    swap, own_log, k_state = call(
        swap_body,
        (shape((DV + 16, LANE), BF16), small, shape((length, DK), BF16)),
        key_vectors,
        values,
        log_gate,
        fetched=(0, 1, 2),
    )
    swapped = lax.ppermute(swap, "core", ring("core", 1))
    own = call(own_body, shape((DV, LANE), F32), values, k_state, fetched=(0,))
    sent, early, decay = call(
        join_body,
        (shape((pieces, 2 * rows + 8, LANE), BF16), shape((DV, LANE), BF16), small),
        own,
        own_log,
        swapped,
    )
    slices = lax.all_to_all(sent, CHIPS, 0, 0, tiled=True)
    prefixes = call(scan_body, shape((pieces, 2 * rows, LANE), BF16), slices)
    prefixes, queries = lax.optimization_barrier((prefixes, queries))
    inputs = (queries, key_vectors, values, log_gate, out_gate)
    att_local, q_start, scale, w_far = call(
        local_body,
        (
            shape((length, DV), F32),
            shape((length, DK), BF16),
            shape((length, DV), BF16),
            shape((DV, width), BF16),
        ),
        *inputs,
        out_weight,
        norm_gain.reshape(1, DV),
        fetched=(0, 1, 2, 3, 4, 5),
        scratch=[pltpu.VMEM(part.shape, BF16) for part in inputs],
        copies=6,
    )
    entering = lax.all_to_all(prefixes, CHIPS, 0, 0, tiled=True)
    state_half = shape((DV, LANE), BF16)
    entering, att_local, q_start, scale, w_far = lax.optimization_barrier(
        (entering, att_local, q_start, scale, w_far)
    )
    keep, send = call(part_body, (state_half, state_half), entering, early, decay)
    other = lax.ppermute(send, "core", ring("core", 1))
    kept, square = call(
        keep_body, (shape((length, half), F32), shape((length, 1), F32)), keep, q_start, att_local
    )
    split = length // 2
    first, last = shape((split, width), BF16), shape((length - split, width), BF16)
    gated, far_up, far_down = call(
        finish_body,
        (shape((length, DV), BF16), first, last),
        other,
        q_start,
        att_local,
        kept,
        square,
        scale,
        w_far,
    )
    up, down = ring("head", 1), ring("head", -1)
    far_up = lax.ppermute(far_up, "head", up)
    far_down = lax.ppermute(far_down, "head", down)
    up_b, down_a = call(
        direct_body,
        (last, first),
        gated,
        out_weight,
        fetched=(1,),
        scratch=[pltpu.VMEM((2, DV, width), BF16)],
        copies=2,
    )
    below_b = lax.ppermute(up_b, "head", up)
    above_a = lax.ppermute(down_a, "head", down)
    up_a, down_b, own_part = call(
        near_body,
        (shape(first.shape, F32), shape(last.shape, F32), shape((length, width), F32)),
        gated,
        out_weight,
        fetched=(1,),
        scratch=[pltpu.VMEM((3, DV, width), BF16)],
        copies=3,
    )
    up_a, down_b = call(pass_body, (first, last), up_a, down_b, far_up, far_down)
    below_a = lax.ppermute(up_a, "head", up)
    above_b = lax.ppermute(down_b, "head", down)
    return call(
        sum_body, shape((length, width), BF16), own_part, below_a, below_b, above_a, above_b
    )


def solution(mesh):
    split = Mesh(mesh.devices.reshape(4, 8, 2, mesh.shape["head"]), (*SEQ, "head"))
    in_specs = (
        P(SEQ, "head"),
        P(SEQ, "head"),
        P(SEQ, "head"),
        P(SEQ, "head"),
        P(SEQ, "head"),
        P("head"),
        P("head", None),
    )
    out_specs = P(SEQ, "head")

    return jax.shard_map(
        shards, mesh=split, in_specs=in_specs, out_specs=out_specs, check_vma=False
    )
```

```python
import jax
import jax.numpy as jnp
from jax import lax
from jax.experimental import pallas as pl
from jax.experimental.pallas import tpu as pltpu
from jax.sharding import Mesh
from jax.sharding import PartitionSpec as P


DK = 256
DV = 512
SPAN = 64
LANE = 128
SEQ = ("chip_x", "chip_z", "core")
CHIPS = ("chip_x", "chip_z")
F32 = jnp.float32
BF16 = jnp.bfloat16
VMEM = pl.BlockSpec(memory_space=pltpu.VMEM)
HBM = pl.BlockSpec(memory_space=pltpu.HBM)


def call(body, outs, *args, fetched=(), scratch=(), copies=0, outs_in=VMEM):
    moved = sum(a.size * a.dtype.itemsize for a in args)
    args = [
        pltpu.with_memory_space_constraint(a, pltpu.HBM) if i in fetched else a
        for i, a in enumerate(args)
    ]
    if fetched and not copies:
        scratch = [pltpu.VMEM(args[i].shape, args[i].dtype) for i in fetched]
        copies = len(fetched)
    if copies:
        scratch = [*scratch, pltpu.SemaphoreType.DMA((copies,))]
    return pl.pallas_call(
        body,
        out_shape=outs,
        in_specs=[HBM if i in fetched else VMEM for i in range(len(args))],
        out_specs=jax.tree.map(lambda _: outs_in, outs),
        scratch_shapes=scratch,
        cost_estimate=pl.CostEstimate(flops=10**9, transcendentals=0, bytes_accessed=moved),
        compiler_params=pltpu.CompilerParams(vmem_limit_bytes=16 * 2**20),
    )(*args)


def dot(a, b, dims=((1,), (0,))):
    return lax.dot_general(a, b, (dims, ((), ())), preferred_element_type=F32)


def triangle(length, keep):
    row = lax.broadcasted_iota(jnp.int32, (length, length), 0)
    col = lax.broadcasted_iota(jnp.int32, (length, length), 1)
    return jnp.where(keep(row, col), 1.0, 0.0).astype(BF16)


def stacked(*parts):
    row = lax.broadcasted_iota(jnp.int32, (8, LANE), 0)
    block = jnp.zeros((8, LANE), F32)
    for at, part in enumerate(parts):
        block = jnp.where(row == at, part, block)
    return block


def split_bf16(values):
    high = values.astype(BF16).astype(F32)
    return high, values - high


def fetch(sems, *pairs):
    copies = [pltpu.make_async_copy(src, dst, sems.at[i]) for i, (src, dst) in enumerate(pairs)]
    for copy in copies:
        copy.start()
    return copies


def columns(index, width):
    return pl.ds(pl.multiple_of(index * width, width), width)


def head_columns(shift, width):
    count = lax.axis_size("head")
    return columns(lax.rem(lax.axis_index("head") + shift, count), width)


def swap_body(k_hbm, v_hbm, g_hbm, swap_ref, log_ref, state_ref, k_ref, v_ref, g_ref, sems):
    gate_copy, k_copy, v_copy = fetch(sems, (g_hbm, g_ref), (k_hbm, k_ref), (v_hbm, v_ref))
    length = k_ref.shape[0]
    half = DV // 2
    mask = triangle(length, lambda r, c: c > r)
    gate_copy.wait()
    gate = g_ref[...]
    after = dot(mask, gate)
    total = after[0:1] + gate[0:1].astype(F32)
    k_copy.wait()
    k_state = (k_ref[...].astype(F32) * jnp.exp(after)).astype(BF16)
    state_ref[...] = k_state
    v_copy.wait()
    theirs = columns(1 - lax.axis_index("core"), half)
    state = dot(v_ref[:, theirs], k_state, ((0,), (0,))).astype(BF16)
    swap_ref[0:half, :] = state[:, :LANE]
    swap_ref[half : 2 * half, :] = state[:, LANE:]
    left_high, left_low = split_bf16(total[:, :LANE])
    right_high, right_low = split_bf16(total[:, LANE:])
    tail = stacked(left_high, right_high, left_low, right_low)
    swap_ref[2 * half :, :] = jnp.concatenate([tail, tail], axis=0).astype(BF16)
    log_ref[...] = stacked(total[:, :LANE], total[:, LANE:])


def own_body(v_hbm, state_ref, own_ref, v_ref, sems):
    (copy,) = fetch(sems, (v_hbm, v_ref))
    copy.wait()
    half = DV // 2
    mine = columns(lax.axis_index("core"), half)
    state = dot(v_ref[:, mine], state_ref[...], ((0,), (0,)))
    own_ref[0:half, :] = state[:, :LANE]
    own_ref[half:, :] = state[:, LANE:]


def join_body(own_ref, log_ref, swap_ref, out_ref, first_ref, decay_ref):
    pieces, rows = (out_ref.shape[0], (out_ref.shape[1] - 8) // 2)
    half = pieces * rows
    early = lax.axis_index("core") == 0
    tail = swap_ref[2 * half : 2 * half + 8, :].astype(F32)
    sums = []
    decays = []
    for side in range(2):
        at = slice(side * half, (side + 1) * half)
        own_log = log_ref[side : side + 1, :]
        other_log = tail[side : side + 1] + tail[side + 2 : side + 3]
        own = own_ref[at, :]
        other = swap_ref[at, :].astype(F32)
        first = jnp.where(early, own, other)
        second = jnp.where(early, other, own)
        state = first * jnp.exp(jnp.where(early, other_log, own_log)) + second
        first_ref[at, :] = first.astype(BF16)
        decays.append(jnp.exp(jnp.where(early, own_log, other_log)))
        sums.append(own_log + other_log)
        piece = slice(side * rows, (side + 1) * rows)
        out_ref[:, piece, :] = state.reshape(pieces, rows, LANE).astype(BF16)
    decay_ref[...] = stacked(*decays)
    left_high, left_low = split_bf16(sums[0])
    right_high, right_low = split_bf16(sums[1])
    tail = stacked(left_high, right_high, left_low, right_low)
    out_ref[:, 2 * rows :, :] = jnp.broadcast_to(tail[None], (pieces, 8, LANE)).astype(BF16)


def scan_body(in_ref, out_ref):
    pieces, rows = (in_ref.shape[0], out_ref.shape[1] // 2)
    left = right = jnp.zeros((rows, LANE), F32)
    for j in range(pieces):
        out_ref[j, 0:rows, :] = left.astype(BF16)
        out_ref[j, rows : 2 * rows, :] = right.astype(BF16)
        tail = in_ref[j, 2 * rows :, :].astype(F32)
        left = left * jnp.exp(tail[0:1] + tail[2:3]) + in_ref[j, 0:rows, :].astype(F32)
        right = right * jnp.exp(tail[1:2] + tail[3:4]) + in_ref[j, rows : 2 * rows, :].astype(F32)


def part_body(in_ref, first_ref, decay_ref, keep_ref, send_ref):
    pieces, rows = (in_ref.shape[0], in_ref.shape[1] // 2)
    half = pieces * rows
    early = lax.axis_index("core") == 0
    for side in range(2):
        at = slice(side * half, (side + 1) * half)
        piece = slice(side * rows, (side + 1) * rows)
        entering = in_ref[:, piece, :].astype(F32).reshape(half, LANE)
        between = entering * decay_ref[side : side + 1, :] + first_ref[at, :].astype(F32)
        keep_ref[at, :] = jnp.where(early, entering, between).astype(BF16)
        send_ref[at, :] = jnp.where(early, between, entering).astype(BF16)


def local_body(
    q_hbm, k_hbm, v_hbm, g_hbm, outer_hbm, w_hbm, gain_ref,
    att_ref, start_ref, scale_ref, w_ref, q_ref, k_ref, v_ref, g_ref, outer_ref, sems,
):
    far_columns = w_hbm.at[:, head_columns(2, w_ref.shape[1])]
    *copies, far_copy = fetch(
        sems,
        (g_hbm, g_ref),
        (q_hbm, q_ref),
        (k_hbm, k_ref),
        (v_hbm, v_ref),
        (outer_hbm, outer_ref),
        (far_columns, w_ref),
    )
    length = q_ref.shape[0]
    lower = triangle(SPAN, lambda r, c: c <= r)
    row = lax.broadcasted_iota(jnp.int32, (SPAN, SPAN), 0)
    col = lax.broadcasted_iota(jnp.int32, (SPAN, SPAN), 1)
    for copy in copies:
        copy.wait()
    carried = None
    before = jnp.zeros((1, DK), F32)
    for i in range(length // SPAN):
        at = slice(i * SPAN, (i + 1) * SPAN)
        running = dot(lower, g_ref[at, :])
        middle = running[SPAN // 2 : SPAN // 2 + 1]
        ending = running[SPAN - 1 : SPAN]
        query_f = q_ref[at, :].astype(F32)
        key_f = k_ref[at, :].astype(F32)
        value = v_ref[at, :]
        q_inter = query_f * jnp.exp(running)
        q_intra = (query_f * jnp.exp(running - middle)).astype(BF16)
        k_intra = (key_f * jnp.exp(middle - running)).astype(BF16)
        scores = dot(q_intra, k_intra, ((1,), (1,)))
        weights = jnp.where(col <= row, scores, 0.0).astype(BF16)
        attention = dot(weights, value)
        if i:
            attention = attention + dot(q_inter.astype(BF16), carried.astype(BF16))
        att_ref[at, :] = attention
        start_ref[at, :] = (query_f * jnp.exp(running + before)).astype(BF16)
        before = before + ending
        if (i + 1) * SPAN < length:
            k_state = (key_f * jnp.exp(ending - running)).T.astype(BF16)
            block = dot(k_state, value)
            carried = block if i == 0 else carried * jnp.exp(ending).reshape(DK, 1) + block
        outer_f = outer_ref[at, :].astype(F32)
        scale = outer_f / (1.0 + jnp.exp(-outer_f)) * gain_ref[...]
        scale_ref[at, :] = scale.astype(BF16)
    far_copy.wait()


def keep_body(keep_ref, q_ref, att_ref, out_ref, square_ref):
    half = keep_ref.shape[0] // 2
    attention = att_ref[:, columns(lax.axis_index("core"), half)]
    attention = attention + dot(q_ref[:, :LANE], keep_ref[:half, :], ((1,), (1,)))
    attention = attention + dot(q_ref[:, LANE:], keep_ref[half:, :], ((1,), (1,)))
    out_ref[...] = attention
    square_ref[...] = jnp.sum(attention * attention, axis=-1, keepdims=True)


def finish_body(
    other_ref, q_ref, att_ref, kept_ref, square_ref, scale_ref, w_ref, gated_ref, far_ref
):
    half = other_ref.shape[0] // 2
    core = lax.axis_index("core")
    here, there = columns(core, half), columns(1 - core, half)
    attention = att_ref[:, there]
    attention = attention + dot(q_ref[:, :LANE], other_ref[:half, :], ((1,), (1,)))
    attention = attention + dot(q_ref[:, LANE:], other_ref[half:, :], ((1,), (1,)))
    total = square_ref[...] + jnp.sum(attention * attention, axis=-1, keepdims=True)
    inverse = lax.rsqrt(total * (1.0 / DV) + 1e-05)
    gated_ref[:, there] = (attention * inverse * scale_ref[:, there].astype(F32)).astype(BF16)
    gated_ref[:, here] = (kept_ref[...] * inverse * scale_ref[:, here].astype(F32)).astype(BF16)
    far_ref[...] = dot(gated_ref[...], w_ref[...]).astype(BF16)


def onward():
    return jnp.where(lax.axis_index("core") == 0, 1, lax.axis_size("head") - 1)


def direct_body(gated_ref, w_hbm, out_ref, w_ref, sems):
    back = head_columns(lax.axis_size("head") - onward(), w_ref.shape[1])
    (copy,) = fetch(sems, (w_hbm.at[:, back], w_ref))
    copy.wait()
    out_ref[...] = dot(gated_ref[...], w_ref[...]).astype(BF16)


def near_body(gated_ref, w_hbm, onward_ref, own_ref, w_onward_ref, w_own_ref, sems):
    width = w_own_ref.shape[1]
    onward_copy, own_copy = fetch(
        sems,
        (w_hbm.at[:, head_columns(onward(), width)], w_onward_ref),
        (w_hbm.at[:, head_columns(0, width)], w_own_ref),
    )
    onward_copy.wait()
    onward_ref[...] = dot(gated_ref[...], w_onward_ref[...])
    own_copy.wait()
    own_ref[...] = dot(gated_ref[...], w_own_ref[...])


def pass_body(onward_ref, far_ref, out_ref):
    out_ref[...] = (onward_ref[...] + far_ref[...].astype(F32)).astype(BF16)


def sum_body(own_ref, direct_ref, passed_ref, out_ref):
    total = own_ref[...] + direct_ref[...].astype(F32) + passed_ref[...].astype(F32)
    out_ref[...] = total.astype(BF16)


def ring(axis, shift):
    length = lax.axis_size(axis)
    return [(i, (i + shift) % length) for i in range(length)]


def shards(queries, key_vectors, values, log_gate, out_gate, norm_gain, out_weight):
    length = queries.shape[0]
    pieces = lax.axis_size(CHIPS)
    half = DV // 2
    rows = half // pieces
    width = out_weight.shape[1] // lax.axis_size("head")
    shape = jax.ShapeDtypeStruct
    small = shape((8, LANE), F32)
    swap, own_log, k_state = call(
        swap_body,
        (shape((DV + 16, LANE), BF16), small, shape((length, DK), BF16)),
        key_vectors,
        values,
        log_gate,
        fetched=(0, 1, 2),
    )
    swapped = lax.ppermute(swap, "core", ring("core", 1))
    own = call(own_body, shape((DV, LANE), F32), values, k_state, fetched=(0,))
    sent, early, decay = call(
        join_body,
        (shape((pieces, 2 * rows + 8, LANE), BF16), shape((DV, LANE), BF16), small),
        own,
        own_log,
        swapped,
    )
    slices = lax.all_to_all(sent, CHIPS, 0, 0, tiled=True)
    prefixes = call(scan_body, shape((pieces, 2 * rows, LANE), BF16), slices)
    prefixes, queries = lax.optimization_barrier((prefixes, queries))
    inputs = (queries, key_vectors, values, log_gate, out_gate)
    att_local, q_start, scale, w_far = call(
        local_body,
        (
            shape((length, DV), F32),
            shape((length, DK), BF16),
            shape((length, DV), BF16),
            shape((DV, width), BF16),
        ),
        *inputs,
        out_weight,
        norm_gain.reshape(1, DV),
        fetched=(0, 1, 2, 3, 4, 5),
        scratch=[pltpu.VMEM(part.shape, BF16) for part in inputs],
        copies=6,
    )
    entering = lax.all_to_all(prefixes, CHIPS, 0, 0, tiled=True)
    state_half = shape((DV, LANE), BF16)
    entering, att_local, q_start, scale, w_far = lax.optimization_barrier(
        (entering, att_local, q_start, scale, w_far)
    )
    keep, send = call(part_body, (state_half, state_half), entering, early, decay)
    other = lax.ppermute(send, "core", ring("core", 1))
    kept, square = call(
        keep_body, (shape((length, half), F32), shape((length, 1), F32)), keep, q_start, att_local
    )
    block = shape((length, width), BF16)
    block_f = shape((length, width), F32)
    gated, far = call(
        finish_body,
        (shape((length, DV), BF16), block),
        other,
        q_start,
        att_local,
        kept,
        square,
        scale,
        w_far,
    )
    heads = lax.axis_size("head")
    way = [(c * heads + y, c * heads + (y + 1 - 2 * c) % heads) for c in (0, 1) for y in range(heads)]
    against = [(target, source) for source, target in way]
    group = ("core", "head")
    far = lax.ppermute(far, group, way)
    column = pltpu.VMEM((DV, width), BF16)
    direct = call(
        direct_body, block, gated, out_weight, fetched=(1,), scratch=[column], copies=1
    )
    direct = lax.ppermute(direct, group, against)
    passed, own_part = call(
        near_body,
        (block_f, block_f),
        gated,
        out_weight,
        fetched=(1,),
        scratch=[column, column],
        copies=2,
    )
    passed = lax.ppermute(call(pass_body, block, passed, far), group, way)
    return call(sum_body, block, own_part, direct, passed)


def solution(mesh):
    split = Mesh(mesh.devices.reshape(4, 8, 2, mesh.shape["head"]), (*SEQ, "head"))
    in_specs = (
        P(SEQ, "head"),
        P(SEQ, "head"),
        P(SEQ, "head"),
        P(SEQ, "head"),
        P(SEQ, "head"),
        P("head"),
        P("head", None),
    )
    out_specs = P(SEQ, "head")

    return jax.shard_map(
        shards, mesh=split, in_specs=in_specs, out_specs=out_specs, check_vma=False
    )
```

```python
import jax
import jax.numpy as jnp
from jax import lax
from jax.experimental import pallas as pl
from jax.experimental.pallas import tpu as pltpu
from jax.sharding import Mesh
from jax.sharding import PartitionSpec as P


DK = 256
DV = 512
SPAN = 64
LANE = 128
SEQ = ("chip_x", "chip_z", "core")
CHIPS = ("chip_x", "chip_z")
F32 = jnp.float32
BF16 = jnp.bfloat16
VMEM = pl.BlockSpec(memory_space=pltpu.VMEM)
HBM = pl.BlockSpec(memory_space=pltpu.HBM)


def call(body, outs, *args, fetched=(), scratch=(), copies=0, outs_in=VMEM):
    moved = sum(a.size * a.dtype.itemsize for a in args)
    args = [
        pltpu.with_memory_space_constraint(a, pltpu.HBM) if i in fetched else a
        for i, a in enumerate(args)
    ]
    if fetched and not copies:
        scratch = [pltpu.VMEM(args[i].shape, args[i].dtype) for i in fetched]
        copies = len(fetched)
    if copies:
        scratch = [*scratch, pltpu.SemaphoreType.DMA((copies,))]
    return pl.pallas_call(
        body,
        out_shape=outs,
        in_specs=[HBM if i in fetched else VMEM for i in range(len(args))],
        out_specs=jax.tree.map(lambda _: outs_in, outs),
        scratch_shapes=scratch,
        cost_estimate=pl.CostEstimate(flops=10**9, transcendentals=0, bytes_accessed=moved),
        compiler_params=pltpu.CompilerParams(vmem_limit_bytes=16 * 2**20),
    )(*args)


def dot(a, b, dims=((1,), (0,))):
    return lax.dot_general(a, b, (dims, ((), ())), preferred_element_type=F32)


def triangle(length, keep):
    row = lax.broadcasted_iota(jnp.int32, (length, length), 0)
    col = lax.broadcasted_iota(jnp.int32, (length, length), 1)
    return jnp.where(keep(row, col), 1.0, 0.0).astype(BF16)


def stacked(*parts):
    row = lax.broadcasted_iota(jnp.int32, (8, LANE), 0)
    block = jnp.zeros((8, LANE), F32)
    for at, part in enumerate(parts):
        block = jnp.where(row == at, part, block)
    return block


def split_bf16(values):
    high = values.astype(BF16).astype(F32)
    return high, values - high


def fetch(sems, *pairs):
    copies = [pltpu.make_async_copy(src, dst, sems.at[i]) for i, (src, dst) in enumerate(pairs)]
    for copy in copies:
        copy.start()
    return copies


def columns(index, width):
    return pl.ds(pl.multiple_of(index * width, width), width)


def head_columns(shift, width):
    count = lax.axis_size("head")
    return columns(lax.rem(lax.axis_index("head") + shift, count), width)


def swap_body(k_hbm, v_hbm, g_hbm, swap_ref, log_ref, state_ref, k_ref, v_ref, g_ref, sems):
    gate_copy, k_copy, v_copy = fetch(sems, (g_hbm, g_ref), (k_hbm, k_ref), (v_hbm, v_ref))
    length = k_ref.shape[0]
    half = DV // 2
    mask = triangle(length, lambda r, c: c > r)
    gate_copy.wait()
    gate = g_ref[...]
    after = dot(mask, gate)
    total = after[0:1] + gate[0:1].astype(F32)
    k_copy.wait()
    k_state = (k_ref[...].astype(F32) * jnp.exp(after)).astype(BF16)
    state_ref[...] = k_state
    v_copy.wait()
    theirs = columns(1 - lax.axis_index("core"), half)
    state = dot(v_ref[:, theirs], k_state, ((0,), (0,))).astype(BF16)
    swap_ref[0:half, :] = state[:, :LANE]
    swap_ref[half : 2 * half, :] = state[:, LANE:]
    left_high, left_low = split_bf16(total[:, :LANE])
    right_high, right_low = split_bf16(total[:, LANE:])
    tail = stacked(left_high, right_high, left_low, right_low)
    swap_ref[2 * half :, :] = jnp.concatenate([tail, tail], axis=0).astype(BF16)
    log_ref[...] = stacked(total[:, :LANE], total[:, LANE:])


def own_body(v_hbm, state_ref, own_ref, v_ref, sems):
    (copy,) = fetch(sems, (v_hbm, v_ref))
    copy.wait()
    half = DV // 2
    mine = columns(lax.axis_index("core"), half)
    state = dot(v_ref[:, mine], state_ref[...], ((0,), (0,)))
    own_ref[0:half, :] = state[:, :LANE]
    own_ref[half:, :] = state[:, LANE:]


def join_body(own_ref, log_ref, swap_ref, out_ref, first_ref, decay_ref):
    pieces, rows = (out_ref.shape[0], (out_ref.shape[1] - 8) // 2)
    half = pieces * rows
    early = lax.axis_index("core") == 0
    tail = swap_ref[2 * half : 2 * half + 8, :].astype(F32)
    sums = []
    decays = []
    for side in range(2):
        at = slice(side * half, (side + 1) * half)
        own_log = log_ref[side : side + 1, :]
        other_log = tail[side : side + 1] + tail[side + 2 : side + 3]
        own = own_ref[at, :]
        other = swap_ref[at, :].astype(F32)
        first = jnp.where(early, own, other)
        second = jnp.where(early, other, own)
        state = first * jnp.exp(jnp.where(early, other_log, own_log)) + second
        first_ref[at, :] = first.astype(BF16)
        decays.append(jnp.exp(jnp.where(early, own_log, other_log)))
        sums.append(own_log + other_log)
        piece = slice(side * rows, (side + 1) * rows)
        out_ref[:, piece, :] = state.reshape(pieces, rows, LANE).astype(BF16)
    decay_ref[...] = stacked(*decays)
    left_high, left_low = split_bf16(sums[0])
    right_high, right_low = split_bf16(sums[1])
    tail = stacked(left_high, right_high, left_low, right_low)
    out_ref[:, 2 * rows :, :] = jnp.broadcast_to(tail[None], (pieces, 8, LANE)).astype(BF16)


def scan_body(in_ref, out_ref):
    pieces, rows = (in_ref.shape[0], out_ref.shape[1] // 2)
    left = right = jnp.zeros((rows, LANE), F32)
    for j in range(pieces):
        out_ref[j, 0:rows, :] = left.astype(BF16)
        out_ref[j, rows : 2 * rows, :] = right.astype(BF16)
        tail = in_ref[j, 2 * rows :, :].astype(F32)
        left = left * jnp.exp(tail[0:1] + tail[2:3]) + in_ref[j, 0:rows, :].astype(F32)
        right = right * jnp.exp(tail[1:2] + tail[3:4]) + in_ref[j, rows : 2 * rows, :].astype(F32)


def part_body(in_ref, first_ref, decay_ref, keep_ref, send_ref):
    pieces, rows = (in_ref.shape[0], in_ref.shape[1] // 2)
    half = pieces * rows
    early = lax.axis_index("core") == 0
    for side in range(2):
        at = slice(side * half, (side + 1) * half)
        piece = slice(side * rows, (side + 1) * rows)
        entering = in_ref[:, piece, :].astype(F32).reshape(half, LANE)
        between = entering * decay_ref[side : side + 1, :] + first_ref[at, :].astype(F32)
        keep_ref[at, :] = jnp.where(early, entering, between).astype(BF16)
        send_ref[at, :] = jnp.where(early, between, entering).astype(BF16)


def local_body(
    q_hbm, k_hbm, v_hbm, g_hbm, outer_hbm, w_hbm, gain_ref,
    att_ref, start_ref, scale_ref, w_ref, q_ref, k_ref, v_ref, g_ref, outer_ref, sems,
):
    far_columns = w_hbm.at[:, head_columns(2, w_ref.shape[1])]
    *copies, far_copy = fetch(
        sems,
        (g_hbm, g_ref),
        (q_hbm, q_ref),
        (k_hbm, k_ref),
        (v_hbm, v_ref),
        (outer_hbm, outer_ref),
        (far_columns, w_ref),
    )
    length = q_ref.shape[0]
    lower = triangle(SPAN, lambda r, c: c <= r)
    row = lax.broadcasted_iota(jnp.int32, (SPAN, SPAN), 0)
    col = lax.broadcasted_iota(jnp.int32, (SPAN, SPAN), 1)
    for copy in copies:
        copy.wait()
    carried = None
    before = jnp.zeros((1, DK), F32)
    for i in range(length // SPAN):
        at = slice(i * SPAN, (i + 1) * SPAN)
        running = dot(lower, g_ref[at, :])
        middle = running[SPAN // 2 : SPAN // 2 + 1]
        ending = running[SPAN - 1 : SPAN]
        query_f = q_ref[at, :].astype(F32)
        key_f = k_ref[at, :].astype(F32)
        value = v_ref[at, :]
        q_inter = query_f * jnp.exp(running)
        q_intra = (query_f * jnp.exp(running - middle)).astype(BF16)
        k_intra = (key_f * jnp.exp(middle - running)).astype(BF16)
        scores = dot(q_intra, k_intra, ((1,), (1,)))
        weights = jnp.where(col <= row, scores, 0.0).astype(BF16)
        attention = dot(weights, value)
        if i:
            attention = attention + dot(q_inter.astype(BF16), carried.astype(BF16))
        att_ref[at, :] = attention
        start_ref[at, :] = (query_f * jnp.exp(running + before)).astype(BF16)
        before = before + ending
        if (i + 1) * SPAN < length:
            k_state = (key_f * jnp.exp(ending - running)).T.astype(BF16)
            block = dot(k_state, value)
            carried = block if i == 0 else carried * jnp.exp(ending).reshape(DK, 1) + block
        outer_f = outer_ref[at, :].astype(F32)
        scale = outer_f / (1.0 + jnp.exp(-outer_f)) * gain_ref[...]
        scale_ref[at, :] = scale.astype(BF16)
    far_copy.wait()


def keep_body(keep_ref, q_ref, att_ref, out_ref, square_ref):
    half = keep_ref.shape[0] // 2
    attention = att_ref[:, columns(lax.axis_index("core"), half)]
    attention = attention + dot(q_ref[:, :LANE], keep_ref[:half, :], ((1,), (1,)))
    attention = attention + dot(q_ref[:, LANE:], keep_ref[half:, :], ((1,), (1,)))
    out_ref[...] = attention
    square_ref[...] = jnp.sum(attention * attention, axis=-1, keepdims=True)


def finish_body(
    other_ref, q_ref, att_ref, kept_ref, square_ref, scale_ref, w_ref, gated_ref, far_ref
):
    half = other_ref.shape[0] // 2
    core = lax.axis_index("core")
    here, there = columns(core, half), columns(1 - core, half)
    attention = att_ref[:, there]
    attention = attention + dot(q_ref[:, :LANE], other_ref[:half, :], ((1,), (1,)))
    attention = attention + dot(q_ref[:, LANE:], other_ref[half:, :], ((1,), (1,)))
    total = square_ref[...] + jnp.sum(attention * attention, axis=-1, keepdims=True)
    inverse = lax.rsqrt(total * (1.0 / DV) + 1e-05)
    gated_ref[:, there] = (attention * inverse * scale_ref[:, there].astype(F32)).astype(BF16)
    gated_ref[:, here] = (kept_ref[...] * inverse * scale_ref[:, here].astype(F32)).astype(BF16)
    far_ref[...] = dot(gated_ref[...], w_ref[...]).astype(BF16)


def onward():
    return jnp.where(lax.axis_index("core") == 0, 1, lax.axis_size("head") - 1)


def direct_body(gated_ref, w_hbm, out_ref, w_ref, sems):
    back = head_columns(lax.axis_size("head") - onward(), w_ref.shape[1])
    (copy,) = fetch(sems, (w_hbm.at[:, back], w_ref))
    copy.wait()
    out_ref[...] = dot(gated_ref[...], w_ref[...]).astype(BF16)


def near_body(gated_ref, w_hbm, onward_ref, own_ref, w_onward_ref, w_own_ref, sems):
    width = w_own_ref.shape[1]
    onward_copy, own_copy = fetch(
        sems,
        (w_hbm.at[:, head_columns(onward(), width)], w_onward_ref),
        (w_hbm.at[:, head_columns(0, width)], w_own_ref),
    )
    onward_copy.wait()
    onward_ref[...] = dot(gated_ref[...], w_onward_ref[...])
    own_copy.wait()
    own_ref[...] = dot(gated_ref[...], w_own_ref[...])


def pass_body(onward_ref, far_ref, out_ref):
    out_ref[...] = (onward_ref[...] + far_ref[...].astype(F32)).astype(BF16)


def sum_body(own_ref, direct_ref, passed_ref, out_ref):
    total = own_ref[...] + direct_ref[...].astype(F32) + passed_ref[...].astype(F32)
    out_ref[...] = total.astype(BF16)


def ring(axis, shift):
    length = lax.axis_size(axis)
    return [(i, (i + shift) % length) for i in range(length)]


def shards(queries, key_vectors, values, log_gate, out_gate, norm_gain, out_weight):
    length = queries.shape[0]
    pieces = lax.axis_size(CHIPS)
    half = DV // 2
    rows = half // pieces
    width = out_weight.shape[1] // lax.axis_size("head")
    shape = jax.ShapeDtypeStruct
    small = shape((8, LANE), F32)
    swap, own_log, k_state = call(
        swap_body,
        (shape((DV + 16, LANE), BF16), small, shape((length, DK), BF16)),
        key_vectors,
        values,
        log_gate,
        fetched=(0, 1, 2),
    )
    swapped = lax.ppermute(swap, "core", ring("core", 1))
    own = call(own_body, shape((DV, LANE), F32), values, k_state, fetched=(0,))
    sent, early, decay = call(
        join_body,
        (shape((pieces, 2 * rows + 8, LANE), BF16), shape((DV, LANE), BF16), small),
        own,
        own_log,
        swapped,
    )
    slices = lax.all_to_all(sent, CHIPS, 0, 0, tiled=True)
    prefixes = call(scan_body, shape((pieces, 2 * rows, LANE), BF16), slices)
    prefixes, queries = lax.optimization_barrier((prefixes, queries))
    inputs = (queries, key_vectors, values, log_gate, out_gate)
    att_local, q_start, scale, w_far = call(
        local_body,
        (
            shape((length, DV), F32),
            shape((length, DK), BF16),
            shape((length, DV), BF16),
            shape((DV, width), BF16),
        ),
        *inputs,
        out_weight,
        norm_gain.reshape(1, DV),
        fetched=(0, 1, 2, 3, 4, 5),
        scratch=[pltpu.VMEM(part.shape, BF16) for part in inputs],
        copies=6,
    )
    entering = lax.all_to_all(prefixes, CHIPS, 0, 0, tiled=True)
    state_half = shape((DV, LANE), BF16)
    entering, att_local, q_start, scale, w_far = lax.optimization_barrier(
        (entering, att_local, q_start, scale, w_far)
    )
    keep, send = call(part_body, (state_half, state_half), entering, early, decay)
    other = lax.ppermute(send, "core", ring("core", 1))
    kept, square = call(
        keep_body, (shape((length, half), F32), shape((length, 1), F32)), keep, q_start, att_local
    )
    block = shape((length, width), BF16)
    block_f = shape((length, width), F32)
    gated, far = call(
        finish_body,
        (shape((length, DV), BF16), block),
        other,
        q_start,
        att_local,
        kept,
        square,
        scale,
        w_far,
    )
    heads = lax.axis_size("head")
    way = [(c * heads + y, c * heads + (y + 1 - 2 * c) % heads) for c in (0, 1) for y in range(heads)]
    against = [(target, source) for source, target in way]
    group = ("core", "head")
    far = lax.ppermute(far, group, way)
    column = pltpu.VMEM((DV, width), BF16)
    direct = call(direct_body, block, gated, out_weight, fetched=(1,), scratch=[column], copies=1)
    direct = lax.ppermute(direct, group, against)
    passed, own_part = call(
        near_body,
        (block_f, block_f),
        gated,
        out_weight,
        fetched=(1,),
        scratch=[column, column],
        copies=2,
    )
    passed = call(pass_body, block, passed, far)
    passed = lax.ppermute(passed, group, way)
    return call(sum_body, block, own_part, direct, passed)


def solution(mesh):
    split = Mesh(mesh.devices.reshape(4, 8, 2, mesh.shape["head"]), (*SEQ, "head"))
    in_specs = (
        P(SEQ, "head"),
        P(SEQ, "head"),
        P(SEQ, "head"),
        P(SEQ, "head"),
        P(SEQ, "head"),
        P("head"),
        P("head", None),
    )
    out_specs = P(SEQ, "head")

    return jax.shard_map(
        shards, mesh=split, in_specs=in_specs, out_specs=out_specs, check_vma=False
    )
```

```python
import jax
import jax.numpy as jnp
from jax import lax
from jax.experimental import pallas as pl
from jax.experimental.pallas import tpu as pltpu
from jax.sharding import Mesh
from jax.sharding import PartitionSpec as P


DK = 256
DV = 512
SPAN = 64
LANE = 128
SEQ = ("chip_x", "chip_z", "core")
CHIPS = ("chip_x", "chip_z")
F32 = jnp.float32
BF16 = jnp.bfloat16
VMEM = pl.BlockSpec(memory_space=pltpu.VMEM)
HBM = pl.BlockSpec(memory_space=pltpu.HBM)


def call(body, outs, *args, fetched=(), scratch=(), copies=0, outs_in=VMEM):
    moved = sum(a.size * a.dtype.itemsize for a in args)
    args = [
        pltpu.with_memory_space_constraint(a, pltpu.HBM) if i in fetched else a
        for i, a in enumerate(args)
    ]
    if fetched and not copies:
        scratch = [pltpu.VMEM(args[i].shape, args[i].dtype) for i in fetched]
        copies = len(fetched)
    if copies:
        scratch = [*scratch, pltpu.SemaphoreType.DMA((copies,))]
    return pl.pallas_call(
        body,
        out_shape=outs,
        in_specs=[HBM if i in fetched else VMEM for i in range(len(args))],
        out_specs=jax.tree.map(lambda _: outs_in, outs),
        scratch_shapes=scratch,
        cost_estimate=pl.CostEstimate(flops=10**9, transcendentals=0, bytes_accessed=moved),
        compiler_params=pltpu.CompilerParams(vmem_limit_bytes=16 * 2**20),
    )(*args)


def dot(a, b, dims=((1,), (0,))):
    return lax.dot_general(a, b, (dims, ((), ())), preferred_element_type=F32)


def triangle(length, keep):
    row = lax.broadcasted_iota(jnp.int32, (length, length), 0)
    col = lax.broadcasted_iota(jnp.int32, (length, length), 1)
    return jnp.where(keep(row, col), 1.0, 0.0).astype(BF16)


def stacked(*parts):
    row = lax.broadcasted_iota(jnp.int32, (8, LANE), 0)
    block = jnp.zeros((8, LANE), F32)
    for at, part in enumerate(parts):
        block = jnp.where(row == at, part, block)
    return block


def split_bf16(values):
    high = values.astype(BF16).astype(F32)
    return high, values - high


def fetch(sems, *pairs):
    copies = [pltpu.make_async_copy(src, dst, sems.at[i]) for i, (src, dst) in enumerate(pairs)]
    for copy in copies:
        copy.start()
    return copies


def columns(index, width):
    return pl.ds(pl.multiple_of(index * width, width), width)


def head_columns(shift, width):
    count = lax.axis_size("head")
    return columns(lax.rem(lax.axis_index("head") + shift, count), width)


def swap_body(k_hbm, v_hbm, g_hbm, swap_ref, log_ref, state_ref, k_ref, v_ref, g_ref, sems):
    gate_copy, k_copy, v_copy = fetch(sems, (g_hbm, g_ref), (k_hbm, k_ref), (v_hbm, v_ref))
    length = k_ref.shape[0]
    half = DV // 2
    mask = triangle(length, lambda r, c: c > r)
    gate_copy.wait()
    gate = g_ref[...]
    after = dot(mask, gate)
    total = after[0:1] + gate[0:1].astype(F32)
    k_copy.wait()
    v_copy.wait()
    k_state = (k_ref[...].astype(F32) * jnp.exp(after)).astype(BF16)
    state_ref[...] = k_state
    theirs = columns(1 - lax.axis_index("core"), half)
    state = dot(v_ref[:, theirs], k_state, ((0,), (0,))).astype(BF16)
    swap_ref[0:half, :] = state[:, :LANE]
    swap_ref[half : 2 * half, :] = state[:, LANE:]
    left_high, left_low = split_bf16(total[:, :LANE])
    right_high, right_low = split_bf16(total[:, LANE:])
    tail = stacked(left_high, right_high, left_low, right_low)
    swap_ref[2 * half :, :] = jnp.concatenate([tail, tail], axis=0).astype(BF16)
    log_ref[...] = stacked(total[:, :LANE], total[:, LANE:])


def own_body(v_hbm, state_ref, own_ref, v_ref, sems):
    (copy,) = fetch(sems, (v_hbm, v_ref))
    copy.wait()
    half = DV // 2
    mine = columns(lax.axis_index("core"), half)
    state = dot(v_ref[:, mine], state_ref[...], ((0,), (0,)))
    own_ref[0:half, :] = state[:, :LANE]
    own_ref[half:, :] = state[:, LANE:]


def join_body(own_ref, log_ref, swap_ref, out_ref, first_ref, decay_ref):
    pieces, rows = (out_ref.shape[0], (out_ref.shape[1] - 8) // 2)
    half = pieces * rows
    early = lax.axis_index("core") == 0
    tail = swap_ref[2 * half : 2 * half + 8, :].astype(F32)
    sums = []
    decays = []
    for side in range(2):
        at = slice(side * half, (side + 1) * half)
        own_log = log_ref[side : side + 1, :]
        other_log = tail[side : side + 1] + tail[side + 2 : side + 3]
        own = own_ref[at, :]
        other = swap_ref[at, :].astype(F32)
        first = jnp.where(early, own, other)
        second = jnp.where(early, other, own)
        state = first * jnp.exp(jnp.where(early, other_log, own_log)) + second
        first_ref[at, :] = first.astype(BF16)
        decays.append(jnp.exp(jnp.where(early, own_log, other_log)))
        sums.append(own_log + other_log)
        piece = slice(side * rows, (side + 1) * rows)
        out_ref[:, piece, :] = state.reshape(pieces, rows, LANE).astype(BF16)
    decay_ref[...] = stacked(*decays)
    left_high, left_low = split_bf16(sums[0])
    right_high, right_low = split_bf16(sums[1])
    tail = stacked(left_high, right_high, left_low, right_low)
    out_ref[:, 2 * rows :, :] = jnp.broadcast_to(tail[None], (pieces, 8, LANE)).astype(BF16)


CHUNKS = 4


def flush(copies, sems, src, dst, index):
    size = src.shape[0] // CHUNKS
    at = pl.ds(index * size, size)
    copies.append(pltpu.make_async_copy(src.at[at], dst.at[at], sems.at[index]))
    copies[-1].start()


def scan_body(in_ref, out_hbm, out_ref, sems):
    pieces, rows = (in_ref.shape[0], out_ref.shape[1] // 2)
    left = right = jnp.zeros((rows, LANE), F32)
    copies = []
    for j in range(pieces):
        out_ref[j, 0:rows, :] = left.astype(BF16)
        out_ref[j, rows : 2 * rows, :] = right.astype(BF16)
        tail = in_ref[j, 2 * rows :, :].astype(F32)
        left = left * jnp.exp(tail[0:1] + tail[2:3]) + in_ref[j, 0:rows, :].astype(F32)
        right = right * jnp.exp(tail[1:2] + tail[3:4]) + in_ref[j, rows : 2 * rows, :].astype(F32)
        if (j + 1) % (pieces // CHUNKS) == 0:
            flush(copies, sems, out_ref, out_hbm, j * CHUNKS // pieces)
    for copy in copies:
        copy.wait()


def part_body(in_ref, first_ref, decay_ref, keep_ref, send_ref):
    pieces, rows = (in_ref.shape[0], in_ref.shape[1] // 2)
    half = pieces * rows
    early = lax.axis_index("core") == 0
    for side in range(2):
        at = slice(side * half, (side + 1) * half)
        piece = slice(side * rows, (side + 1) * rows)
        entering = in_ref[:, piece, :].astype(F32).reshape(half, LANE)
        between = entering * decay_ref[side : side + 1, :] + first_ref[at, :].astype(F32)
        keep_ref[at, :] = jnp.where(early, entering, between).astype(BF16)
        send_ref[at, :] = jnp.where(early, between, entering).astype(BF16)


def local_body(
    q_hbm, k_hbm, v_hbm, g_hbm, outer_hbm, w_hbm, gain_ref,
    att_ref, start_ref, scale_ref, w_ref, q_ref, k_ref, v_ref, g_ref, outer_ref, sems,
):
    far_columns = w_hbm.at[:, head_columns(2, w_ref.shape[1])]
    *copies, far_copy = fetch(
        sems,
        (g_hbm, g_ref),
        (q_hbm, q_ref),
        (k_hbm, k_ref),
        (v_hbm, v_ref),
        (outer_hbm, outer_ref),
        (far_columns, w_ref),
    )
    length = q_ref.shape[0]
    lower = triangle(SPAN, lambda r, c: c <= r)
    row = lax.broadcasted_iota(jnp.int32, (SPAN, SPAN), 0)
    col = lax.broadcasted_iota(jnp.int32, (SPAN, SPAN), 1)
    for copy in copies:
        copy.wait()
    carried = None
    before = jnp.zeros((1, DK), F32)
    for i in range(length // SPAN):
        at = slice(i * SPAN, (i + 1) * SPAN)
        running = dot(lower, g_ref[at, :])
        middle = running[SPAN // 2 : SPAN // 2 + 1]
        ending = running[SPAN - 1 : SPAN]
        query_f = q_ref[at, :].astype(F32)
        key_f = k_ref[at, :].astype(F32)
        value = v_ref[at, :]
        q_inter = query_f * jnp.exp(running)
        q_intra = (query_f * jnp.exp(running - middle)).astype(BF16)
        k_intra = (key_f * jnp.exp(middle - running)).astype(BF16)
        scores = dot(q_intra, k_intra, ((1,), (1,)))
        weights = jnp.where(col <= row, scores, 0.0).astype(BF16)
        attention = dot(weights, value)
        if i:
            attention = attention + dot(q_inter.astype(BF16), carried.astype(BF16))
        att_ref[at, :] = attention
        start_ref[at, :] = (query_f * jnp.exp(running + before)).astype(BF16)
        before = before + ending
        if (i + 1) * SPAN < length:
            k_state = (key_f * jnp.exp(ending - running)).T.astype(BF16)
            block = dot(k_state, value)
            carried = block if i == 0 else carried * jnp.exp(ending).reshape(DK, 1) + block
        outer_f = outer_ref[at, :].astype(F32)
        scale = outer_f / (1.0 + jnp.exp(-outer_f)) * gain_ref[...]
        scale_ref[at, :] = scale.astype(BF16)
    far_copy.wait()


def keep_body(keep_ref, q_ref, att_ref, out_ref, square_ref):
    half = keep_ref.shape[0] // 2
    attention = att_ref[:, columns(lax.axis_index("core"), half)]
    attention = attention + dot(q_ref[:, :LANE], keep_ref[:half, :], ((1,), (1,)))
    attention = attention + dot(q_ref[:, LANE:], keep_ref[half:, :], ((1,), (1,)))
    out_ref[...] = attention
    square_ref[...] = jnp.sum(attention * attention, axis=-1, keepdims=True)


def finish_body(
    other_ref, q_ref, att_ref, kept_ref, square_ref, scale_ref, w_ref,
    gated_ref, far_on_ref, far_back_ref,
):
    half = other_ref.shape[0] // 2
    core = lax.axis_index("core")
    here, there = columns(core, half), columns(1 - core, half)
    attention = att_ref[:, there]
    attention = attention + dot(q_ref[:, :LANE], other_ref[:half, :], ((1,), (1,)))
    attention = attention + dot(q_ref[:, LANE:], other_ref[half:, :], ((1,), (1,)))
    total = square_ref[...] + jnp.sum(attention * attention, axis=-1, keepdims=True)
    inverse = lax.rsqrt(total * (1.0 / DV) + 1e-05)
    gated_ref[:, there] = (attention * inverse * scale_ref[:, there].astype(F32)).astype(BF16)
    gated_ref[:, here] = (kept_ref[...] * inverse * scale_ref[:, here].astype(F32)).astype(BF16)
    rows = far_on_ref.shape[0]
    far_on_ref[...] = dot(gated_ref[:rows, :], w_ref[...]).astype(BF16)
    far_back_ref[...] = dot(gated_ref[rows:, :], w_ref[...]).astype(BF16)


def fetch_columns(w_hbm, w_ref, sems, *shifts):
    width = w_ref.shape[-1]
    pairs = [(w_hbm.at[:, head_columns(s, width)], w_ref.at[i]) for i, s in enumerate(shifts)]
    return fetch(sems, *pairs)


def onward():
    return jnp.where(lax.axis_index("core") == 0, 1, lax.axis_size("head") - 1)


def direct_body(gated_ref, w_hbm, on_ref, back_ref, w_ref, sems):
    copies = fetch_columns(w_hbm, w_ref, sems, onward(), lax.axis_size("head") - onward())
    half = on_ref.shape[0]
    copies[0].wait()
    on_ref[...] = dot(gated_ref[half:, :], w_ref[0]).astype(BF16)
    copies[1].wait()
    back_ref[...] = dot(gated_ref[:half, :], w_ref[1]).astype(BF16)


def near_body(gated_ref, w_hbm, on_ref, back_ref, own_ref, w_ref, sems):
    copies = fetch_columns(w_hbm, w_ref, sems, onward(), lax.axis_size("head") - onward(), 0)
    half = on_ref.shape[0]
    copies[0].wait()
    on_ref[...] = dot(gated_ref[:half, :], w_ref[0])
    copies[1].wait()
    back_ref[...] = dot(gated_ref[half:, :], w_ref[1])
    copies[2].wait()
    own_ref[...] = dot(gated_ref[...], w_ref[2])


def pass_body(on_ref, back_ref, far_on_ref, far_back_ref, on_out_ref, back_out_ref):
    on_out_ref[...] = (on_ref[...] + far_on_ref[...].astype(F32)).astype(BF16)
    back_out_ref[...] = (back_ref[...] + far_back_ref[...].astype(F32)).astype(BF16)


def sum_body(own_ref, on_a_ref, on_b_ref, back_a_ref, back_b_ref, out_hbm, out_ref, sems):
    length, half = (own_ref.shape[0], on_a_ref.shape[0])
    size = length // CHUNKS
    copies = []
    for i in range(CHUNKS):
        at, start = slice(i * size, (i + 1) * size), i * size % half
        part = slice(start, start + size)
        on, back = (on_a_ref, back_a_ref) if i * size < half else (on_b_ref, back_b_ref)
        total = own_ref[at, :] + on[part, :].astype(F32) + back[part, :].astype(F32)
        out_ref[at, :] = total.astype(BF16)
        flush(copies, sems, out_ref, out_hbm, i)
    for copy in copies:
        copy.wait()


def ring(axis, shift):
    length = lax.axis_size(axis)
    return [(i, (i + shift) % length) for i in range(length)]


def shards(queries, key_vectors, values, log_gate, out_gate, norm_gain, out_weight):
    length = queries.shape[0]
    pieces = lax.axis_size(CHIPS)
    half = DV // 2
    rows = half // pieces
    width = out_weight.shape[1] // lax.axis_size("head")
    shape = jax.ShapeDtypeStruct
    small = shape((8, LANE), F32)
    swap, own_log, k_state = call(
        swap_body,
        (shape((DV + 16, LANE), BF16), small, shape((length, DK), BF16)),
        key_vectors,
        values,
        log_gate,
        fetched=(0, 1, 2),
    )
    swapped = lax.ppermute(swap, "core", ring("core", 1))
    own = call(own_body, shape((DV, LANE), F32), values, k_state, fetched=(0,))
    sent, early, decay = call(
        join_body,
        (shape((pieces, 2 * rows + 8, LANE), BF16), shape((DV, LANE), BF16), small),
        own,
        own_log,
        swapped,
    )
    slices = lax.all_to_all(sent, CHIPS, 0, 0, tiled=True)
    carried = shape((pieces, 2 * rows, LANE), BF16)
    prefixes = call(
        scan_body,
        carried,
        slices,
        scratch=[pltpu.VMEM(carried.shape, BF16)],
        copies=CHUNKS,
        outs_in=HBM,
    )
    prefixes, queries = lax.optimization_barrier((prefixes, queries))
    inputs = (queries, key_vectors, values, log_gate, out_gate)
    att_local, q_start, scale, w_far = call(
        local_body,
        (
            shape((length, DV), F32),
            shape((length, DK), BF16),
            shape((length, DV), BF16),
            shape((DV, width), BF16),
        ),
        *inputs,
        out_weight,
        norm_gain.reshape(1, DV),
        fetched=(0, 1, 2, 3, 4, 5),
        scratch=[pltpu.VMEM(part.shape, BF16) for part in inputs],
        copies=6,
    )
    entering = lax.all_to_all(prefixes, CHIPS, 0, 0, tiled=True)
    state_half = shape((DV, LANE), BF16)
    entering, att_local, q_start, scale, w_far = lax.optimization_barrier(
        (entering, att_local, q_start, scale, w_far)
    )
    keep, send = call(part_body, (state_half, state_half), entering, early, decay)
    other = lax.ppermute(send, "core", ring("core", 1))
    kept, square = call(
        keep_body, (shape((length, half), F32), shape((length, 1), F32)), keep, q_start, att_local
    )
    near = shape((length // 2, width), BF16)
    near_f = shape((length // 2, width), F32)
    gated, far_on, far_back = call(
        finish_body,
        (shape((length, DV), BF16), near, near),
        other,
        q_start,
        att_local,
        kept,
        square,
        scale,
        w_far,
    )
    heads = lax.axis_size("head")
    on = [(c * heads + y, c * heads + (y + 1 - 2 * c) % heads) for c in (0, 1) for y in range(heads)]
    back = [(target, source) for source, target in on]
    group = ("core", "head")
    far_on = lax.ppermute(far_on, group, on)
    far_back = lax.ppermute(far_back, group, back)
    on_b, back_a = call(
        direct_body,
        (near, near),
        gated,
        out_weight,
        fetched=(1,),
        scratch=[pltpu.VMEM((2, DV, width), BF16)],
        copies=2,
    )
    on_b = lax.ppermute(on_b, group, on)
    back_a = lax.ppermute(back_a, group, back)
    on_a, back_b, own_part = call(
        near_body,
        (near_f, near_f, shape((length, width), F32)),
        gated,
        out_weight,
        fetched=(1,),
        scratch=[pltpu.VMEM((3, DV, width), BF16)],
        copies=3,
    )
    on_a, back_b = call(pass_body, (near, near), on_a, back_b, far_on, far_back)
    on_a = lax.ppermute(on_a, group, on)
    back_b = lax.ppermute(back_b, group, back)
    return call(
        sum_body,
        shape((length, width), BF16),
        own_part,
        on_a,
        on_b,
        back_a,
        back_b,
        scratch=[pltpu.VMEM((length, width), BF16)],
        copies=CHUNKS,
        outs_in=HBM,
    )


def solution(mesh):
    split = Mesh(mesh.devices.reshape(4, 8, 2, mesh.shape["head"]), (*SEQ, "head"))
    in_specs = (
        P(SEQ, "head"),
        P(SEQ, "head"),
        P(SEQ, "head"),
        P(SEQ, "head"),
        P(SEQ, "head"),
        P("head"),
        P("head", None),
    )
    out_specs = P(SEQ, "head")

    return jax.shard_map(
        shards, mesh=split, in_specs=in_specs, out_specs=out_specs, check_vma=False
    )
```

```python
import jax
import jax.numpy as jnp
from jax import lax
from jax.experimental import pallas as pl
from jax.experimental.pallas import tpu as pltpu
from jax.sharding import Mesh
from jax.sharding import PartitionSpec as P


DK = 256
DV = 512
SPAN = 64
LANE = 128
SEQ = ("chip_x", "chip_z", "core")
CHIPS = ("chip_x", "chip_z")
F32 = jnp.float32
BF16 = jnp.bfloat16
VMEM = pl.BlockSpec(memory_space=pltpu.VMEM)
HBM = pl.BlockSpec(memory_space=pltpu.HBM)


def call(body, outs, *args, fetched=(), scratch=(), copies=0, outs_in=VMEM):
    moved = sum(a.size * a.dtype.itemsize for a in args)
    args = [
        pltpu.with_memory_space_constraint(a, pltpu.HBM) if i in fetched else a
        for i, a in enumerate(args)
    ]
    if fetched and not copies:
        scratch = [pltpu.VMEM(args[i].shape, args[i].dtype) for i in fetched]
        copies = len(fetched)
    if copies:
        scratch = [*scratch, pltpu.SemaphoreType.DMA((copies,))]
    return pl.pallas_call(
        body,
        out_shape=outs,
        in_specs=[HBM if i in fetched else VMEM for i in range(len(args))],
        out_specs=jax.tree.map(lambda _: outs_in, outs),
        scratch_shapes=scratch,
        cost_estimate=pl.CostEstimate(flops=10**9, transcendentals=0, bytes_accessed=moved),
        compiler_params=pltpu.CompilerParams(vmem_limit_bytes=16 * 2**20),
    )(*args)


def dot(a, b, dims=((1,), (0,))):
    return lax.dot_general(a, b, (dims, ((), ())), preferred_element_type=F32)


def triangle(length, keep):
    row = lax.broadcasted_iota(jnp.int32, (length, length), 0)
    col = lax.broadcasted_iota(jnp.int32, (length, length), 1)
    return jnp.where(keep(row, col), 1.0, 0.0).astype(BF16)


def stacked(*parts):
    row = lax.broadcasted_iota(jnp.int32, (8, LANE), 0)
    block = jnp.zeros((8, LANE), F32)
    for at, part in enumerate(parts):
        block = jnp.where(row == at, part, block)
    return block


def split_bf16(values):
    high = values.astype(BF16).astype(F32)
    return high, values - high


def fetch(sems, *pairs):
    copies = [pltpu.make_async_copy(src, dst, sems.at[i]) for i, (src, dst) in enumerate(pairs)]
    for copy in copies:
        copy.start()
    return copies


def columns(index, width):
    return pl.ds(pl.multiple_of(index * width, width), width)


def head_columns(shift, width):
    count = lax.axis_size("head")
    return columns(lax.rem(lax.axis_index("head") + shift, count), width)


def swap_body(k_hbm, v_hbm, g_hbm, swap_ref, log_ref, state_ref, k_ref, v_ref, g_ref, sems):
    gate_copy, k_copy, v_copy = fetch(sems, (g_hbm, g_ref), (k_hbm, k_ref), (v_hbm, v_ref))
    length = k_ref.shape[0]
    half = DV // 2
    mask = triangle(length, lambda r, c: c > r)
    gate_copy.wait()
    gate = g_ref[...]
    after = dot(mask, gate)
    total = after[0:1] + gate[0:1].astype(F32)
    k_copy.wait()
    v_copy.wait()
    k_state = (k_ref[...].astype(F32) * jnp.exp(after)).astype(BF16)
    state_ref[...] = k_state
    theirs = columns(1 - lax.axis_index("core"), half)
    state = dot(v_ref[:, theirs], k_state, ((0,), (0,))).astype(BF16)
    swap_ref[0:half, :] = state[:, :LANE]
    swap_ref[half : 2 * half, :] = state[:, LANE:]
    left_high, left_low = split_bf16(total[:, :LANE])
    right_high, right_low = split_bf16(total[:, LANE:])
    tail = stacked(left_high, right_high, left_low, right_low)
    swap_ref[2 * half :, :] = jnp.concatenate([tail, tail], axis=0).astype(BF16)
    log_ref[...] = stacked(total[:, :LANE], total[:, LANE:])


def own_body(v_hbm, state_ref, own_ref, v_ref, sems):
    (copy,) = fetch(sems, (v_hbm, v_ref))
    copy.wait()
    half = DV // 2
    mine = columns(lax.axis_index("core"), half)
    state = dot(v_ref[:, mine], state_ref[...], ((0,), (0,)))
    own_ref[0:half, :] = state[:, :LANE]
    own_ref[half:, :] = state[:, LANE:]


def join_body(own_ref, log_ref, swap_ref, out_ref, first_ref, decay_ref):
    pieces, rows = (out_ref.shape[0], (out_ref.shape[1] - 8) // 2)
    half = pieces * rows
    early = lax.axis_index("core") == 0
    tail = swap_ref[2 * half : 2 * half + 8, :].astype(F32)
    sums = []
    decays = []
    for side in range(2):
        at = slice(side * half, (side + 1) * half)
        own_log = log_ref[side : side + 1, :]
        other_log = tail[side : side + 1] + tail[side + 2 : side + 3]
        own = own_ref[at, :]
        other = swap_ref[at, :].astype(F32)
        first = jnp.where(early, own, other)
        second = jnp.where(early, other, own)
        state = first * jnp.exp(jnp.where(early, other_log, own_log)) + second
        first_ref[at, :] = first.astype(BF16)
        decays.append(jnp.exp(jnp.where(early, own_log, other_log)))
        sums.append(own_log + other_log)
        piece = slice(side * rows, (side + 1) * rows)
        out_ref[:, piece, :] = state.reshape(pieces, rows, LANE).astype(BF16)
    decay_ref[...] = stacked(*decays)
    left_high, left_low = split_bf16(sums[0])
    right_high, right_low = split_bf16(sums[1])
    tail = stacked(left_high, right_high, left_low, right_low)
    out_ref[:, 2 * rows :, :] = jnp.broadcast_to(tail[None], (pieces, 8, LANE)).astype(BF16)


def scan_body(in_ref, out_ref):
    pieces, rows = (in_ref.shape[0], out_ref.shape[1] // 2)
    left = right = jnp.zeros((rows, LANE), F32)
    for j in range(pieces):
        out_ref[j, 0:rows, :] = left.astype(BF16)
        out_ref[j, rows : 2 * rows, :] = right.astype(BF16)
        tail = in_ref[j, 2 * rows :, :].astype(F32)
        left = left * jnp.exp(tail[0:1] + tail[2:3]) + in_ref[j, 0:rows, :].astype(F32)
        right = right * jnp.exp(tail[1:2] + tail[3:4]) + in_ref[j, rows : 2 * rows, :].astype(F32)


def part_body(in_ref, first_ref, decay_ref, keep_ref, send_ref):
    pieces, rows = (in_ref.shape[0], in_ref.shape[1] // 2)
    half = pieces * rows
    early = lax.axis_index("core") == 0
    for side in range(2):
        at = slice(side * half, (side + 1) * half)
        piece = slice(side * rows, (side + 1) * rows)
        entering = in_ref[:, piece, :].astype(F32).reshape(half, LANE)
        between = entering * decay_ref[side : side + 1, :] + first_ref[at, :].astype(F32)
        keep_ref[at, :] = jnp.where(early, entering, between).astype(BF16)
        send_ref[at, :] = jnp.where(early, between, entering).astype(BF16)


def local_body(
    q_hbm, k_hbm, v_hbm, g_hbm, outer_hbm, w_hbm, gain_ref,
    att_ref, start_ref, scale_ref, w_ref, q_ref, k_ref, v_ref, g_ref, outer_ref, sems,
):
    far_columns = w_hbm.at[:, head_columns(2, w_ref.shape[1])]
    *copies, far_copy = fetch(
        sems,
        (g_hbm, g_ref),
        (q_hbm, q_ref),
        (k_hbm, k_ref),
        (v_hbm, v_ref),
        (outer_hbm, outer_ref),
        (far_columns, w_ref),
    )
    length = q_ref.shape[0]
    lower = triangle(SPAN, lambda r, c: c <= r)
    row = lax.broadcasted_iota(jnp.int32, (SPAN, SPAN), 0)
    col = lax.broadcasted_iota(jnp.int32, (SPAN, SPAN), 1)
    for copy in copies:
        copy.wait()
    carried = None
    before = jnp.zeros((1, DK), F32)
    for i in range(length // SPAN):
        at = slice(i * SPAN, (i + 1) * SPAN)
        running = dot(lower, g_ref[at, :])
        middle = running[SPAN // 2 : SPAN // 2 + 1]
        ending = running[SPAN - 1 : SPAN]
        query_f = q_ref[at, :].astype(F32)
        key_f = k_ref[at, :].astype(F32)
        value = v_ref[at, :]
        q_inter = query_f * jnp.exp(running)
        q_intra = (query_f * jnp.exp(running - middle)).astype(BF16)
        k_intra = (key_f * jnp.exp(middle - running)).astype(BF16)
        scores = dot(q_intra, k_intra, ((1,), (1,)))
        weights = jnp.where(col <= row, scores, 0.0).astype(BF16)
        attention = dot(weights, value)
        if i:
            attention = attention + dot(q_inter.astype(BF16), carried.astype(BF16))
        att_ref[at, :] = attention
        start_ref[at, :] = (query_f * jnp.exp(running + before)).astype(BF16)
        before = before + ending
        if (i + 1) * SPAN < length:
            k_state = (key_f * jnp.exp(ending - running)).T.astype(BF16)
            block = dot(k_state, value)
            carried = block if i == 0 else carried * jnp.exp(ending).reshape(DK, 1) + block
        outer_f = outer_ref[at, :].astype(F32)
        scale = outer_f / (1.0 + jnp.exp(-outer_f)) * gain_ref[...]
        scale_ref[at, :] = scale.astype(BF16)
    far_copy.wait()


def keep_body(
    keep_ref, q_ref, att_ref, scale_ref, w_ref, gated_ref, square_ref, far_ref
):
    half = keep_ref.shape[0] // 2
    here = columns(lax.axis_index("core"), half)
    attention = att_ref[:, here]
    attention = attention + dot(q_ref[:, :LANE], keep_ref[:half, :], ((1,), (1,)))
    attention = attention + dot(q_ref[:, LANE:], keep_ref[half:, :], ((1,), (1,)))
    gated = (attention * scale_ref[:, here].astype(F32)).astype(BF16)
    gated_ref[...] = gated
    far_ref[...] = dot(gated, w_ref[here, :])
    square_ref[...] = jnp.sum(attention * attention, axis=-1, keepdims=True)


def finish_body(
    other_ref, q_ref, att_ref, kept_ref, square_ref, kept_far_ref, scale_ref, w_ref,
    gated_ref, norm_ref, far_up_ref, far_down_ref,
):
    half = other_ref.shape[0] // 2
    core = lax.axis_index("core")
    here, there = columns(core, half), columns(1 - core, half)
    attention = att_ref[:, there]
    attention = attention + dot(q_ref[:, :LANE], other_ref[:half, :], ((1,), (1,)))
    attention = attention + dot(q_ref[:, LANE:], other_ref[half:, :], ((1,), (1,)))
    gated = (attention * scale_ref[:, there].astype(F32)).astype(BF16)
    far = kept_far_ref[...] + dot(gated, w_ref[there, :])
    total = square_ref[...] + jnp.sum(attention * attention, axis=-1, keepdims=True)
    norm = lax.rsqrt(total * (1.0 / DV) + 1e-05)
    norm_ref[...] = norm
    far = (far * norm).astype(BF16)
    split = far_up_ref.shape[0]
    far_up_ref[...] = far[:split]
    far_down_ref[...] = far[split:]
    gated_ref[:, there] = gated
    gated_ref[:, here] = kept_ref[...]


def fetch_columns(w_hbm, w_ref, sems, *shifts):
    width = w_ref.shape[-1]
    pairs = [(w_hbm.at[:, head_columns(s, width)], w_ref.at[i]) for i, s in enumerate(shifts)]
    return fetch(sems, *pairs)


def direct_body(gated_ref, norm_ref, w_hbm, up_ref, down_ref, w_ref, sems):
    copies = fetch_columns(w_hbm, w_ref, sems, 1, 3)
    half = up_ref.shape[0]
    top, low = slice(0, half), slice(half, 2 * half)
    copies[0].wait()
    up_ref[...] = (dot(gated_ref[low, :], w_ref[0]) * norm_ref[low, :]).astype(BF16)
    copies[1].wait()
    down_ref[...] = (dot(gated_ref[top, :], w_ref[1]) * norm_ref[top, :]).astype(BF16)


def near_body(gated_ref, norm_ref, w_hbm, up_ref, down_ref, own_ref, w_ref, sems):
    copies = fetch_columns(w_hbm, w_ref, sems, 1, 3, 0)
    half = up_ref.shape[0]
    top, low = slice(0, half), slice(half, 2 * half)
    copies[0].wait()
    up_ref[...] = dot(gated_ref[top, :], w_ref[0]) * norm_ref[top, :]
    copies[1].wait()
    down_ref[...] = dot(gated_ref[low, :], w_ref[1]) * norm_ref[low, :]
    copies[2].wait()
    own_ref[...] = dot(gated_ref[...], w_ref[2]) * norm_ref[...]


def pass_body(up_ref, down_ref, far_up_ref, far_down_ref, up_out_ref, down_out_ref):
    up_out_ref[...] = (up_ref[...] + far_up_ref[...].astype(F32)).astype(BF16)
    down_out_ref[...] = (down_ref[...] + far_down_ref[...].astype(F32)).astype(BF16)


CHUNKS = 4


def sum_body(own_ref, below_a_ref, below_b_ref, above_a_ref, above_b_ref, out_hbm, out_ref, sems):
    length, half = (own_ref.shape[0], below_a_ref.shape[0])
    size = length // CHUNKS
    copies = []
    for i in range(CHUNKS):
        at, start = slice(i * size, (i + 1) * size), i * size % half
        part = slice(start, start + size)
        below, above = (below_a_ref, above_a_ref) if i * size < half else (below_b_ref, above_b_ref)
        total = own_ref[at, :] + below[part, :].astype(F32) + above[part, :].astype(F32)
        out_ref[at, :] = total.astype(BF16)
        copies.append(pltpu.make_async_copy(out_ref.at[at], out_hbm.at[at], sems.at[i]))
        copies[-1].start()
    for copy in copies:
        copy.wait()


def ring(axis, shift):
    length = lax.axis_size(axis)
    return [(i, (i + shift) % length) for i in range(length)]


def shards(queries, key_vectors, values, log_gate, out_gate, norm_gain, out_weight):
    length = queries.shape[0]
    pieces = lax.axis_size(CHIPS)
    half = DV // 2
    rows = half // pieces
    width = out_weight.shape[1] // lax.axis_size("head")
    shape = jax.ShapeDtypeStruct
    small = shape((8, LANE), F32)
    swap, own_log, k_state = call(
        swap_body,
        (shape((DV + 16, LANE), BF16), small, shape((length, DK), BF16)),
        key_vectors,
        values,
        log_gate,
        fetched=(0, 1, 2),
    )
    swapped = lax.ppermute(swap, "core", ring("core", 1))
    own = call(own_body, shape((DV, LANE), F32), values, k_state, fetched=(0,))
    sent, early, decay = call(
        join_body,
        (shape((pieces, 2 * rows + 8, LANE), BF16), shape((DV, LANE), BF16), small),
        own,
        own_log,
        swapped,
    )
    slices = lax.all_to_all(sent, CHIPS, 0, 0, tiled=True)
    prefixes = call(scan_body, shape((pieces, 2 * rows, LANE), BF16), slices)
    prefixes, queries = lax.optimization_barrier((prefixes, queries))
    inputs = (queries, key_vectors, values, log_gate, out_gate)
    att_local, q_start, scale, w_far = call(
        local_body,
        (
            shape((length, DV), F32),
            shape((length, DK), BF16),
            shape((length, DV), BF16),
            shape((DV, width), BF16),
        ),
        *inputs,
        out_weight,
        norm_gain.reshape(1, DV),
        fetched=(0, 1, 2, 3, 4, 5),
        scratch=[pltpu.VMEM(part.shape, BF16) for part in inputs],
        copies=6,
    )
    entering = lax.all_to_all(prefixes, CHIPS, 0, 0, tiled=True)
    state_half = shape((DV, LANE), BF16)
    entering, att_local, q_start, scale, w_far = lax.optimization_barrier(
        (entering, att_local, q_start, scale, w_far)
    )
    keep, send = call(part_body, (state_half, state_half), entering, early, decay)
    other = lax.ppermute(send, "core", ring("core", 1))
    column = shape((length, 1), F32)
    near = shape((length // 2, width), BF16)
    near_f = shape((length // 2, width), F32)
    kept, square, kept_far = call(
        keep_body,
        (shape((length, half), BF16), column, shape((length, width), F32)),
        keep,
        q_start,
        att_local,
        scale,
        w_far,
    )
    gated, norm, far_up, far_down = call(
        finish_body,
        (shape((length, DV), BF16), column, near, near),
        other,
        q_start,
        att_local,
        kept,
        square,
        kept_far,
        scale,
        w_far,
    )
    up, down = ring("head", 1), ring("head", -1)
    far_up = lax.ppermute(far_up, "head", up)
    far_down = lax.ppermute(far_down, "head", down)
    up_b, down_a = call(
        direct_body,
        (near, near),
        gated,
        norm,
        out_weight,
        fetched=(2,),
        scratch=[pltpu.VMEM((2, DV, width), BF16)],
        copies=2,
    )
    below_b = lax.ppermute(up_b, "head", up)
    above_a = lax.ppermute(down_a, "head", down)
    up_a, down_b, own_part = call(
        near_body,
        (near_f, near_f, shape((length, width), F32)),
        gated,
        norm,
        out_weight,
        fetched=(2,),
        scratch=[pltpu.VMEM((3, DV, width), BF16)],
        copies=3,
    )
    up_a, down_b = call(pass_body, (near, near), up_a, down_b, far_up, far_down)
    below_a = lax.ppermute(up_a, "head", up)
    above_b = lax.ppermute(down_b, "head", down)
    return call(
        sum_body,
        shape((length, width), BF16),
        own_part,
        below_a,
        below_b,
        above_a,
        above_b,
        scratch=[pltpu.VMEM((length, width), BF16)],
        copies=CHUNKS,
        outs_in=HBM,
    )


def solution(mesh):
    split = Mesh(mesh.devices.reshape(4, 8, 2, mesh.shape["head"]), (*SEQ, "head"))
    in_specs = (
        P(SEQ, "head"),
        P(SEQ, "head"),
        P(SEQ, "head"),
        P(SEQ, "head"),
        P(SEQ, "head"),
        P("head"),
        P("head", None),
    )
    out_specs = P(SEQ, "head")

    return jax.shard_map(
        shards, mesh=split, in_specs=in_specs, out_specs=out_specs, check_vma=False
    )
```

```python
import functools

import jax
import jax.numpy as jnp
from jax import lax
from jax.experimental import pallas as pl
from jax.experimental.pallas import tpu as pltpu
from jax.sharding import Mesh
from jax.sharding import PartitionSpec as P


DK = 256
DV = 512
SPAN = 64
LANE = 128
SEQ = ("chip_x", "chip_z", "core")
CHIPS = ("chip_x", "chip_z")
F32 = jnp.float32
BF16 = jnp.bfloat16
VMEM = pl.BlockSpec(memory_space=pltpu.VMEM)
HBM = pl.BlockSpec(memory_space=pltpu.HBM)


def call(body, outs, *args, fetched=(), scratch=(), copies=0, outs_in=VMEM):
    moved = sum(a.size * a.dtype.itemsize for a in args)
    args = [
        pltpu.with_memory_space_constraint(a, pltpu.HBM) if i in fetched else a
        for i, a in enumerate(args)
    ]
    if fetched and not copies:
        scratch = [pltpu.VMEM(args[i].shape, args[i].dtype) for i in fetched]
        copies = len(fetched)
    if copies:
        scratch = [*scratch, pltpu.SemaphoreType.DMA((copies,))]
    return pl.pallas_call(
        body,
        out_shape=outs,
        in_specs=[HBM if i in fetched else VMEM for i in range(len(args))],
        out_specs=jax.tree.map(lambda _: outs_in, outs),
        scratch_shapes=scratch,
        cost_estimate=pl.CostEstimate(flops=10**9, transcendentals=0, bytes_accessed=moved),
        compiler_params=pltpu.CompilerParams(vmem_limit_bytes=16 * 2**20),
    )(*args)


def dot(a, b, dims=((1,), (0,))):
    return lax.dot_general(a, b, (dims, ((), ())), preferred_element_type=F32)


def triangle(length, keep):
    row = lax.broadcasted_iota(jnp.int32, (length, length), 0)
    col = lax.broadcasted_iota(jnp.int32, (length, length), 1)
    return jnp.where(keep(row, col), 1.0, 0.0).astype(BF16)


def stacked(*parts):
    row = lax.broadcasted_iota(jnp.int32, (8, LANE), 0)
    block = jnp.zeros((8, LANE), F32)
    for at, part in enumerate(parts):
        block = jnp.where(row == at, part, block)
    return block


def split_bf16(values):
    high = values.astype(BF16).astype(F32)
    return high, values - high


def fetch(sems, *pairs):
    copies = [pltpu.make_async_copy(src, dst, sems.at[i]) for i, (src, dst) in enumerate(pairs)]
    for copy in copies:
        copy.start()
    return copies


def columns(index, width):
    return pl.ds(pl.multiple_of(index * width, width), width)


def head_columns(shift, width):
    count = lax.axis_size("head")
    return columns(lax.rem(lax.axis_index("head") + shift, count), width)


def swap_body(k_hbm, v_hbm, g_hbm, swap_ref, log_ref, state_ref, k_ref, v_ref, g_ref, sems):
    half = DV // 2
    theirs = v_hbm.at[:, columns(1 - lax.axis_index("core"), half)]
    gate_copy, k_copy, v_copy = fetch(sems, (g_hbm, g_ref), (k_hbm, k_ref), (theirs, v_ref))
    length = k_ref.shape[0]
    mask = triangle(length, lambda r, c: c > r)
    gate_copy.wait()
    gate = g_ref[...]
    after = dot(mask, gate)
    total = after[0:1] + gate[0:1].astype(F32)
    k_copy.wait()
    v_copy.wait()
    k_state = (k_ref[...].astype(F32) * jnp.exp(after)).astype(BF16)
    state_ref[...] = k_state
    state = dot(v_ref[...], k_state, ((0,), (0,))).astype(BF16)
    swap_ref[0:half, :] = state[:, :LANE]
    swap_ref[half : 2 * half, :] = state[:, LANE:]
    left_high, left_low = split_bf16(total[:, :LANE])
    right_high, right_low = split_bf16(total[:, LANE:])
    tail = stacked(left_high, right_high, left_low, right_low)
    swap_ref[2 * half :, :] = jnp.concatenate([tail, tail], axis=0).astype(BF16)
    log_ref[...] = stacked(total[:, :LANE], total[:, LANE:])


def own_body(v_hbm, state_ref, own_ref, v_ref, sems):
    half = DV // 2
    mine = v_hbm.at[:, columns(lax.axis_index("core"), half)]
    (copy,) = fetch(sems, (mine, v_ref))
    copy.wait()
    state = dot(v_ref[...], state_ref[...], ((0,), (0,)))
    own_ref[0:half, :] = state[:, :LANE]
    own_ref[half:, :] = state[:, LANE:]


def join_body(own_ref, log_ref, swap_ref, out_ref, first_ref, decay_ref):
    pieces, rows = (out_ref.shape[0], (out_ref.shape[1] - 8) // 2)
    half = pieces * rows
    early = lax.axis_index("core") == 0
    tail = swap_ref[2 * half : 2 * half + 8, :].astype(F32)
    sums = []
    decays = []
    for side in range(2):
        at = slice(side * half, (side + 1) * half)
        own_log = log_ref[side : side + 1, :]
        other_log = tail[side : side + 1] + tail[side + 2 : side + 3]
        own = own_ref[at, :]
        other = swap_ref[at, :].astype(F32)
        first = jnp.where(early, own, other)
        second = jnp.where(early, other, own)
        state = first * jnp.exp(jnp.where(early, other_log, own_log)) + second
        first_ref[at, :] = first.astype(BF16)
        decays.append(jnp.exp(jnp.where(early, own_log, other_log)))
        sums.append(own_log + other_log)
        piece = slice(side * rows, (side + 1) * rows)
        out_ref[:, piece, :] = state.reshape(pieces, rows, LANE).astype(BF16)
    decay_ref[...] = stacked(*decays)
    left_high, left_low = split_bf16(sums[0])
    right_high, right_low = split_bf16(sums[1])
    tail = stacked(left_high, right_high, left_low, right_low)
    out_ref[:, 2 * rows :, :] = jnp.broadcast_to(tail[None], (pieces, 8, LANE)).astype(BF16)


def scan_body(in_ref, out_ref):
    pieces, rows = (in_ref.shape[0], out_ref.shape[1] // 2)
    left = right = jnp.zeros((rows, LANE), F32)
    for j in range(pieces):
        out_ref[j, 0:rows, :] = left.astype(BF16)
        out_ref[j, rows : 2 * rows, :] = right.astype(BF16)
        tail = in_ref[j, 2 * rows :, :].astype(F32)
        left = left * jnp.exp(tail[0:1] + tail[2:3]) + in_ref[j, 0:rows, :].astype(F32)
        right = right * jnp.exp(tail[1:2] + tail[3:4]) + in_ref[j, rows : 2 * rows, :].astype(F32)


def part_body(in_ref, first_ref, decay_ref, keep_ref, send_ref):
    pieces, rows = (in_ref.shape[0], in_ref.shape[1] // 2)
    half = pieces * rows
    early = lax.axis_index("core") == 0
    for side in range(2):
        at = slice(side * half, (side + 1) * half)
        piece = slice(side * rows, (side + 1) * rows)
        entering = in_ref[:, piece, :].astype(F32).reshape(half, LANE)
        between = entering * decay_ref[side : side + 1, :] + first_ref[at, :].astype(F32)
        keep_ref[at, :] = jnp.where(early, entering, between).astype(BF16)
        send_ref[at, :] = jnp.where(early, between, entering).astype(BF16)


def local_body(
    q_hbm, k_hbm, v_hbm, g_hbm, outer_hbm, w_hbm, gain_ref,
    att_ref, start_ref, scale_ref, w_ref, q_ref, k_ref, v_ref, g_ref, outer_ref, sems,
):
    far_columns = w_hbm.at[:, head_columns(2, w_ref.shape[1])]
    *copies, far_copy = fetch(
        sems,
        (g_hbm, g_ref),
        (q_hbm, q_ref),
        (k_hbm, k_ref),
        (v_hbm, v_ref),
        (outer_hbm, outer_ref),
        (far_columns, w_ref),
    )
    length = q_ref.shape[0]
    lower = triangle(SPAN, lambda r, c: c <= r)
    row = lax.broadcasted_iota(jnp.int32, (SPAN, SPAN), 0)
    col = lax.broadcasted_iota(jnp.int32, (SPAN, SPAN), 1)
    for copy in copies:
        copy.wait()
    carried = None
    before = jnp.zeros((1, DK), F32)
    for i in range(length // SPAN):
        at = slice(i * SPAN, (i + 1) * SPAN)
        running = dot(lower, g_ref[at, :])
        middle = running[SPAN // 2 : SPAN // 2 + 1]
        ending = running[SPAN - 1 : SPAN]
        query_f = q_ref[at, :].astype(F32)
        key_f = k_ref[at, :].astype(F32)
        value = v_ref[at, :]
        q_inter = query_f * jnp.exp(running)
        q_intra = (query_f * jnp.exp(running - middle)).astype(BF16)
        k_intra = (key_f * jnp.exp(middle - running)).astype(BF16)
        scores = dot(q_intra, k_intra, ((1,), (1,)))
        weights = jnp.where(col <= row, scores, 0.0).astype(BF16)
        attention = dot(weights, value)
        if i:
            attention = attention + dot(q_inter.astype(BF16), carried.astype(BF16))
        att_ref[at, :] = attention
        start_ref[at, :] = (query_f * jnp.exp(running + before)).astype(BF16)
        before = before + ending
        if (i + 1) * SPAN < length:
            k_state = (key_f * jnp.exp(ending - running)).T.astype(BF16)
            block = dot(k_state, value)
            carried = block if i == 0 else carried * jnp.exp(ending).reshape(DK, 1) + block
        outer_f = outer_ref[at, :].astype(F32)
        scale = outer_f / (1.0 + jnp.exp(-outer_f)) * gain_ref[...]
        scale_ref[at, :] = scale.astype(BF16)
    far_copy.wait()


def keep_body(
    keep_ref, q_ref, att_ref, scale_ref, w_ref, gated_ref, square_ref, far_ref
):
    half = keep_ref.shape[0] // 2
    here = columns(lax.axis_index("core"), half)
    attention = att_ref[:, here]
    attention = attention + dot(q_ref[:, :LANE], keep_ref[:half, :], ((1,), (1,)))
    attention = attention + dot(q_ref[:, LANE:], keep_ref[half:, :], ((1,), (1,)))
    gated = (attention * scale_ref[:, here].astype(F32)).astype(BF16)
    gated_ref[...] = gated
    far_ref[...] = dot(gated, w_ref[here, :])
    square_ref[...] = jnp.sum(attention * attention, axis=-1, keepdims=True)


def finish_body(
    row, other_ref, q_ref, att_ref, kept_ref, square_ref, kept_far_ref, scale_ref, w_ref,
    gated_ref, norm_ref, far_ref,
):
    half = other_ref.shape[0] // 2
    core = lax.axis_index("core")
    here, there = columns(core, half), columns(1 - core, half)
    at = slice(row, row + far_ref.shape[0])
    attention = att_ref[at, there]
    attention = attention + dot(q_ref[at, :LANE], other_ref[:half, :], ((1,), (1,)))
    attention = attention + dot(q_ref[at, LANE:], other_ref[half:, :], ((1,), (1,)))
    gated = (attention * scale_ref[at, there].astype(F32)).astype(BF16)
    far = kept_far_ref[at, :] + dot(gated, w_ref[there, :])
    total = square_ref[at, :] + jnp.sum(attention * attention, axis=-1, keepdims=True)
    norm = lax.rsqrt(total * (1.0 / DV) + 1e-05)
    norm_ref[...] = norm
    far_ref[...] = (far * norm).astype(BF16)
    gated_ref[:, there] = gated
    gated_ref[:, here] = kept_ref[at, :]


def fetch_columns(w_hbm, w_ref, sems, *shifts):
    width = w_ref.shape[-1]
    pairs = [(w_hbm.at[:, head_columns(s, width)], w_ref.at[i]) for i, s in enumerate(shifts)]
    return fetch(sems, *pairs)


def direct_body(top_ref, low_ref, norm_top_ref, norm_low_ref, w_hbm, up_ref, down_ref, w_ref, sems):
    copies = fetch_columns(w_hbm, w_ref, sems, 1, 3)
    copies[0].wait()
    up_ref[...] = (dot(low_ref[...], w_ref[0]) * norm_low_ref[...]).astype(BF16)
    copies[1].wait()
    down_ref[...] = (dot(top_ref[...], w_ref[1]) * norm_top_ref[...]).astype(BF16)


def near_body(
    top_ref, low_ref, norm_top_ref, norm_low_ref, w_hbm, up_ref, down_ref, own_ref, w_ref, sems
):
    copies = fetch_columns(w_hbm, w_ref, sems, 1, 3, 0)
    half = up_ref.shape[0]
    copies[0].wait()
    up_ref[...] = dot(top_ref[...], w_ref[0]) * norm_top_ref[...]
    copies[1].wait()
    down_ref[...] = dot(low_ref[...], w_ref[1]) * norm_low_ref[...]
    copies[2].wait()
    own_ref[:half, :] = dot(top_ref[...], w_ref[2]) * norm_top_ref[...]
    own_ref[half:, :] = dot(low_ref[...], w_ref[2]) * norm_low_ref[...]


def pass_body(up_ref, down_ref, far_up_ref, far_down_ref, up_out_ref, down_out_ref):
    up_out_ref[...] = (up_ref[...] + far_up_ref[...].astype(F32)).astype(BF16)
    down_out_ref[...] = (down_ref[...] + far_down_ref[...].astype(F32)).astype(BF16)


CHUNKS = 4


def sum_body(own_ref, below_a_ref, below_b_ref, above_a_ref, above_b_ref, out_hbm, out_ref, sems):
    length, half = (own_ref.shape[0], below_a_ref.shape[0])
    size = length // CHUNKS
    copies = []
    for i in range(CHUNKS):
        at, start = slice(i * size, (i + 1) * size), i * size % half
        part = slice(start, start + size)
        below, above = (below_a_ref, above_a_ref) if i * size < half else (below_b_ref, above_b_ref)
        total = own_ref[at, :] + below[part, :].astype(F32) + above[part, :].astype(F32)
        out_ref[at, :] = total.astype(BF16)
        copies.append(pltpu.make_async_copy(out_ref.at[at], out_hbm.at[at], sems.at[i]))
        copies[-1].start()
    for copy in copies:
        copy.wait()


def ring(axis, shift):
    length = lax.axis_size(axis)
    return [(i, (i + shift) % length) for i in range(length)]


def shards(queries, key_vectors, values, log_gate, out_gate, norm_gain, out_weight):
    length = queries.shape[0]
    pieces = lax.axis_size(CHIPS)
    half = DV // 2
    rows = half // pieces
    width = out_weight.shape[1] // lax.axis_size("head")
    shape = jax.ShapeDtypeStruct
    small = shape((8, LANE), F32)
    swap, own_log, k_state = call(
        swap_body,
        (shape((DV + 16, LANE), BF16), small, shape((length, DK), BF16)),
        key_vectors,
        values,
        log_gate,
        fetched=(0, 1, 2),
        scratch=[pltpu.VMEM((length, n), BF16) for n in (DK, half, DK)],
        copies=3,
    )
    swapped = lax.ppermute(swap, "core", ring("core", 1))
    own = call(
        own_body,
        shape((DV, LANE), F32),
        values,
        k_state,
        fetched=(0,),
        scratch=[pltpu.VMEM((length, half), BF16)],
        copies=1,
    )
    sent, early, decay = call(
        join_body,
        (shape((pieces, 2 * rows + 8, LANE), BF16), shape((DV, LANE), BF16), small),
        own,
        own_log,
        swapped,
    )
    slices = lax.all_to_all(sent, CHIPS, 0, 0, tiled=True)
    prefixes = call(scan_body, shape((pieces, 2 * rows, LANE), BF16), slices)
    prefixes, queries = lax.optimization_barrier((prefixes, queries))
    inputs = (queries, key_vectors, values, log_gate, out_gate)
    att_local, q_start, scale, w_far = call(
        local_body,
        (
            shape((length, DV), F32),
            shape((length, DK), BF16),
            shape((length, DV), BF16),
            shape((DV, width), BF16),
        ),
        *inputs,
        out_weight,
        norm_gain.reshape(1, DV),
        fetched=(0, 1, 2, 3, 4, 5),
        scratch=[pltpu.VMEM(part.shape, BF16) for part in inputs],
        copies=6,
    )
    entering = lax.all_to_all(prefixes, CHIPS, 0, 0, tiled=True)
    state_half = shape((DV, LANE), BF16)
    entering, att_local, q_start, scale, w_far = lax.optimization_barrier(
        (entering, att_local, q_start, scale, w_far)
    )
    keep, send = call(part_body, (state_half, state_half), entering, early, decay)
    other = lax.ppermute(send, "core", ring("core", 1))
    column = shape((length, 1), F32)
    near = shape((length // 2, width), BF16)
    near_f = shape((length // 2, width), F32)
    kept, square, kept_far = call(
        keep_body,
        (shape((length, half), BF16), column, shape((length, width), F32)),
        keep,
        q_start,
        att_local,
        scale,
        w_far,
    )
    up, down = ring("head", 1), ring("head", -1)
    rows_out = (shape((length // 2, DV), BF16), shape((length // 2, 1), F32), near)
    finish_in = (other, q_start, att_local, kept, square, kept_far, scale, w_far)
    top, norm_top, far_up = call(functools.partial(finish_body, 0), rows_out, *finish_in)
    far_up = lax.ppermute(far_up, "head", up)
    low, norm_low, far_down = call(
        functools.partial(finish_body, length // 2), rows_out, *finish_in
    )
    far_down = lax.ppermute(far_down, "head", down)
    gated = (top, low, norm_top, norm_low)
    up_b, down_a = call(
        direct_body,
        (near, near),
        *gated,
        out_weight,
        fetched=(4,),
        scratch=[pltpu.VMEM((2, DV, width), BF16)],
        copies=2,
    )
    below_b = lax.ppermute(up_b, "head", up)
    above_a = lax.ppermute(down_a, "head", down)
    up_a, down_b, own_part = call(
        near_body,
        (near_f, near_f, shape((length, width), F32)),
        *gated,
        out_weight,
        fetched=(4,),
        scratch=[pltpu.VMEM((3, DV, width), BF16)],
        copies=3,
    )
    up_a, down_b = call(pass_body, (near, near), up_a, down_b, far_up, far_down)
    below_a = lax.ppermute(up_a, "head", up)
    above_b = lax.ppermute(down_b, "head", down)
    return call(
        sum_body,
        shape((length, width), BF16),
        own_part,
        below_a,
        below_b,
        above_a,
        above_b,
        scratch=[pltpu.VMEM((length, width), BF16)],
        copies=CHUNKS,
        outs_in=HBM,
    )


def solution(mesh):
    split = Mesh(mesh.devices.reshape(4, 8, 2, mesh.shape["head"]), (*SEQ, "head"))
    in_specs = (
        P(SEQ, "head"),
        P(SEQ, "head"),
        P(SEQ, "head"),
        P(SEQ, "head"),
        P(SEQ, "head"),
        P("head"),
        P("head", None),
    )
    out_specs = P(SEQ, "head")

    return jax.shard_map(
        shards, mesh=split, in_specs=in_specs, out_specs=out_specs, check_vma=False
    )
```

```python
import functools

import jax
import jax.numpy as jnp
from jax import lax
from jax.experimental import pallas as pl
from jax.experimental.pallas import tpu as pltpu
from jax.sharding import Mesh
from jax.sharding import PartitionSpec as P


DK = 256
DV = 512
SPAN = 64
LANE = 128
SEQ = ("chip_x", "chip_z", "core")
CHIPS = ("chip_x", "chip_z")
F32 = jnp.float32
BF16 = jnp.bfloat16
VMEM = pl.BlockSpec(memory_space=pltpu.VMEM)
HBM = pl.BlockSpec(memory_space=pltpu.HBM)


def call(body, outs, *args, fetched=(), scratch=(), copies=0, outs_in=VMEM):
    moved = sum(a.size * a.dtype.itemsize for a in args)
    args = [
        pltpu.with_memory_space_constraint(a, pltpu.HBM) if i in fetched else a
        for i, a in enumerate(args)
    ]
    if fetched and not copies:
        scratch = [pltpu.VMEM(args[i].shape, args[i].dtype) for i in fetched]
        copies = len(fetched)
    if copies:
        scratch = [*scratch, pltpu.SemaphoreType.DMA((copies,))]
    return pl.pallas_call(
        body,
        out_shape=outs,
        in_specs=[HBM if i in fetched else VMEM for i in range(len(args))],
        out_specs=jax.tree.map(lambda _: outs_in, outs),
        scratch_shapes=scratch,
        cost_estimate=pl.CostEstimate(flops=10**9, transcendentals=0, bytes_accessed=moved),
        compiler_params=pltpu.CompilerParams(vmem_limit_bytes=16 * 2**20),
    )(*args)


def dot(a, b, dims=((1,), (0,))):
    return lax.dot_general(a, b, (dims, ((), ())), preferred_element_type=F32)


def triangle(length, keep):
    row = lax.broadcasted_iota(jnp.int32, (length, length), 0)
    col = lax.broadcasted_iota(jnp.int32, (length, length), 1)
    return jnp.where(keep(row, col), 1.0, 0.0).astype(BF16)


def stacked(*parts):
    row = lax.broadcasted_iota(jnp.int32, (8, LANE), 0)
    block = jnp.zeros((8, LANE), F32)
    for at, part in enumerate(parts):
        block = jnp.where(row == at, part, block)
    return block


def split_bf16(values):
    high = values.astype(BF16).astype(F32)
    return high, values - high


def fetch(sems, *pairs):
    copies = [pltpu.make_async_copy(src, dst, sems.at[i]) for i, (src, dst) in enumerate(pairs)]
    for copy in copies:
        copy.start()
    return copies


def columns(index, width):
    return pl.ds(pl.multiple_of(index * width, width), width)


def head_columns(shift, width):
    count = lax.axis_size("head")
    return columns(lax.rem(lax.axis_index("head") + shift, count), width)


def state_body(
    which, k_hbm, v_hbm, g_hbm, swap_ref, own_ref, log_ref, k_ref, v_ref, g_ref, sems
):
    @pl.when(lax.axis_index("core") == which)
    def _():
        gate_copy, k_copy, v_copy = fetch(sems, (g_hbm, g_ref), (k_hbm, k_ref), (v_hbm, v_ref))
        length = k_ref.shape[0]
        half = DV // 2
        mask = triangle(length, lambda r, c: c > r)
        gate_copy.wait()
        gate = g_ref[...]
        after = dot(mask, gate)
        total = after[0:1] + gate[0:1].astype(F32)
        k_copy.wait()
        v_copy.wait()
        k_state = (k_ref[...].astype(F32) * jnp.exp(after)).astype(BF16)
        theirs, mine = (slice(at * half, (at + 1) * half) for at in (1 - which, which))
        state = dot(v_ref[:, theirs], k_state, ((0,), (0,))).astype(BF16)
        swap_ref[0:half, :] = state[:, :LANE]
        swap_ref[half : 2 * half, :] = state[:, LANE:]
        left_high, left_low = split_bf16(total[:, :LANE])
        right_high, right_low = split_bf16(total[:, LANE:])
        tail = stacked(left_high, right_high, left_low, right_low)
        swap_ref[2 * half :, :] = jnp.concatenate([tail, tail], axis=0).astype(BF16)
        state = dot(v_ref[:, mine], k_state, ((0,), (0,)))
        own_ref[0:half, :] = state[:, :LANE]
        own_ref[half:, :] = state[:, LANE:]
        log_ref[...] = stacked(total[:, :LANE], total[:, LANE:])


def join_body(
    own_0_ref, log_0_ref, swap_0_ref, own_1_ref, log_1_ref, swap_1_ref,
    out_ref, first_ref, decay_ref,
):
    pieces, rows = (out_ref.shape[0], (out_ref.shape[1] - 8) // 2)
    half = pieces * rows
    early = lax.axis_index("core") == 0
    swapped = jnp.where(early, swap_1_ref[...], swap_0_ref[...])
    own_state = jnp.where(early, own_0_ref[...], own_1_ref[...])
    logs = jnp.where(early, log_0_ref[...], log_1_ref[...])
    tail = swapped[2 * half : 2 * half + 8].astype(F32)
    sums = []
    decays = []
    for side in range(2):
        at = slice(side * half, (side + 1) * half)
        own_log = logs[side : side + 1]
        other_log = tail[side : side + 1] + tail[side + 2 : side + 3]
        own = own_state[at]
        other = swapped[at].astype(F32)
        first = jnp.where(early, own, other)
        second = jnp.where(early, other, own)
        state = first * jnp.exp(jnp.where(early, other_log, own_log)) + second
        first_ref[at, :] = first.astype(BF16)
        decays.append(jnp.exp(jnp.where(early, own_log, other_log)))
        sums.append(own_log + other_log)
        piece = slice(side * rows, (side + 1) * rows)
        out_ref[:, piece, :] = state.reshape(pieces, rows, LANE).astype(BF16)
    decay_ref[...] = stacked(*decays)
    left_high, left_low = split_bf16(sums[0])
    right_high, right_low = split_bf16(sums[1])
    tail = stacked(left_high, right_high, left_low, right_low)
    out_ref[:, 2 * rows :, :] = jnp.broadcast_to(tail[None], (pieces, 8, LANE)).astype(BF16)


def scan_body(in_ref, out_ref):
    pieces, rows = (in_ref.shape[0], out_ref.shape[1] // 2)
    left = right = jnp.zeros((rows, LANE), F32)
    for j in range(pieces):
        out_ref[j, 0:rows, :] = left.astype(BF16)
        out_ref[j, rows : 2 * rows, :] = right.astype(BF16)
        tail = in_ref[j, 2 * rows :, :].astype(F32)
        left = left * jnp.exp(tail[0:1] + tail[2:3]) + in_ref[j, 0:rows, :].astype(F32)
        right = right * jnp.exp(tail[1:2] + tail[3:4]) + in_ref[j, rows : 2 * rows, :].astype(F32)


def part_body(in_ref, first_ref, decay_ref, keep_ref, send_ref):
    pieces, rows = (in_ref.shape[0], in_ref.shape[1] // 2)
    half = pieces * rows
    early = lax.axis_index("core") == 0
    for side in range(2):
        at = slice(side * half, (side + 1) * half)
        piece = slice(side * rows, (side + 1) * rows)
        entering = in_ref[:, piece, :].astype(F32).reshape(half, LANE)
        between = entering * decay_ref[side : side + 1, :] + first_ref[at, :].astype(F32)
        keep_ref[at, :] = jnp.where(early, entering, between).astype(BF16)
        send_ref[at, :] = jnp.where(early, between, entering).astype(BF16)


def local_body(
    q_hbm, k_hbm, v_hbm, g_hbm, outer_hbm, w_hbm, gain_ref,
    att_ref, start_ref, scale_ref, w_ref, q_ref, k_ref, v_ref, g_ref, outer_ref, sems,
):
    far_columns = w_hbm.at[:, head_columns(2, w_ref.shape[1])]
    *copies, far_copy = fetch(
        sems,
        (g_hbm, g_ref),
        (q_hbm, q_ref),
        (k_hbm, k_ref),
        (v_hbm, v_ref),
        (outer_hbm, outer_ref),
        (far_columns, w_ref),
    )
    length = q_ref.shape[0]
    lower = triangle(SPAN, lambda r, c: c <= r)
    row = lax.broadcasted_iota(jnp.int32, (SPAN, SPAN), 0)
    col = lax.broadcasted_iota(jnp.int32, (SPAN, SPAN), 1)
    for copy in copies:
        copy.wait()
    carried = None
    before = jnp.zeros((1, DK), F32)
    for i in range(length // SPAN):
        at = slice(i * SPAN, (i + 1) * SPAN)
        running = dot(lower, g_ref[at, :])
        middle = running[SPAN // 2 : SPAN // 2 + 1]
        ending = running[SPAN - 1 : SPAN]
        query_f = q_ref[at, :].astype(F32)
        key_f = k_ref[at, :].astype(F32)
        value = v_ref[at, :]
        q_inter = query_f * jnp.exp(running)
        q_intra = (query_f * jnp.exp(running - middle)).astype(BF16)
        k_intra = (key_f * jnp.exp(middle - running)).astype(BF16)
        scores = dot(q_intra, k_intra, ((1,), (1,)))
        weights = jnp.where(col <= row, scores, 0.0).astype(BF16)
        attention = dot(weights, value)
        if i:
            attention = attention + dot(q_inter.astype(BF16), carried.astype(BF16))
        att_ref[at, :] = attention
        start_ref[at, :] = (query_f * jnp.exp(running + before)).astype(BF16)
        before = before + ending
        if (i + 1) * SPAN < length:
            k_state = (key_f * jnp.exp(ending - running)).T.astype(BF16)
            block = dot(k_state, value)
            carried = block if i == 0 else carried * jnp.exp(ending).reshape(DK, 1) + block
        outer_f = outer_ref[at, :].astype(F32)
        scale = outer_f / (1.0 + jnp.exp(-outer_f)) * gain_ref[...]
        scale_ref[at, :] = scale.astype(BF16)
    far_copy.wait()


def keep_body(
    keep_ref, q_ref, att_ref, scale_ref, w_ref, gated_ref, square_ref, far_ref
):
    half = keep_ref.shape[0] // 2
    here = columns(lax.axis_index("core"), half)
    attention = att_ref[:, here]
    attention = attention + dot(q_ref[:, :LANE], keep_ref[:half, :], ((1,), (1,)))
    attention = attention + dot(q_ref[:, LANE:], keep_ref[half:, :], ((1,), (1,)))
    gated = (attention * scale_ref[:, here].astype(F32)).astype(BF16)
    gated_ref[...] = gated
    far_ref[...] = dot(gated, w_ref[here, :])
    square_ref[...] = jnp.sum(attention * attention, axis=-1, keepdims=True)


def finish_body(
    row, other_ref, q_ref, att_ref, kept_ref, square_ref, kept_far_ref, scale_ref, w_ref,
    gated_ref, norm_ref, far_ref,
):
    half = other_ref.shape[0] // 2
    core = lax.axis_index("core")
    here, there = columns(core, half), columns(1 - core, half)
    at = slice(row, row + far_ref.shape[0])
    attention = att_ref[at, there]
    attention = attention + dot(q_ref[at, :LANE], other_ref[:half, :], ((1,), (1,)))
    attention = attention + dot(q_ref[at, LANE:], other_ref[half:, :], ((1,), (1,)))
    gated = (attention * scale_ref[at, there].astype(F32)).astype(BF16)
    far = kept_far_ref[at, :] + dot(gated, w_ref[there, :])
    total = square_ref[at, :] + jnp.sum(attention * attention, axis=-1, keepdims=True)
    norm = lax.rsqrt(total * (1.0 / DV) + 1e-05)
    norm_ref[...] = norm
    far_ref[...] = (far * norm).astype(BF16)
    gated_ref[:, there] = gated
    gated_ref[:, here] = kept_ref[at, :]


def fetch_columns(w_hbm, w_ref, sems, *shifts):
    width = w_ref.shape[-1]
    pairs = [(w_hbm.at[:, head_columns(s, width)], w_ref.at[i]) for i, s in enumerate(shifts)]
    return fetch(sems, *pairs)


def direct_body(top_ref, low_ref, norm_top_ref, norm_low_ref, w_hbm, up_ref, down_ref, w_ref, sems):
    copies = fetch_columns(w_hbm, w_ref, sems, 1, 3)
    copies[0].wait()
    up_ref[...] = (dot(low_ref[...], w_ref[0]) * norm_low_ref[...]).astype(BF16)
    copies[1].wait()
    down_ref[...] = (dot(top_ref[...], w_ref[1]) * norm_top_ref[...]).astype(BF16)


def near_body(
    top_ref, low_ref, norm_top_ref, norm_low_ref, w_hbm, up_ref, down_ref, own_ref, w_ref, sems
):
    copies = fetch_columns(w_hbm, w_ref, sems, 1, 3, 0)
    half = up_ref.shape[0]
    copies[0].wait()
    up_ref[...] = dot(top_ref[...], w_ref[0]) * norm_top_ref[...]
    copies[1].wait()
    down_ref[...] = dot(low_ref[...], w_ref[1]) * norm_low_ref[...]
    copies[2].wait()
    own_ref[:half, :] = dot(top_ref[...], w_ref[2]) * norm_top_ref[...]
    own_ref[half:, :] = dot(low_ref[...], w_ref[2]) * norm_low_ref[...]


def pass_body(up_ref, down_ref, far_up_ref, far_down_ref, up_out_ref, down_out_ref):
    up_out_ref[...] = (up_ref[...] + far_up_ref[...].astype(F32)).astype(BF16)
    down_out_ref[...] = (down_ref[...] + far_down_ref[...].astype(F32)).astype(BF16)


def sum_body(own_ref, below_a_ref, below_b_ref, above_a_ref, above_b_ref, out_hbm, out_ref, sems):
    split = below_a_ref.shape[0]
    copies = []
    for i, (at, below, above) in enumerate(
        (
            (slice(0, split), below_a_ref, above_a_ref),
            (slice(split, own_ref.shape[0]), below_b_ref, above_b_ref),
        )
    ):
        total = own_ref[at, :] + below[...].astype(F32) + above[...].astype(F32)
        out_ref[at, :] = total.astype(BF16)
        copies += fetch(sems.at[pl.ds(i, 1)], (out_ref.at[at], out_hbm.at[at]))
    for copy in copies:
        copy.wait()


def ring(axis, shift):
    length = lax.axis_size(axis)
    return [(i, (i + shift) % length) for i in range(length)]


def shards(queries, key_vectors, values, log_gate, out_gate, norm_gain, out_weight):
    length = queries.shape[0]
    pieces = lax.axis_size(CHIPS)
    half = DV // 2
    rows = half // pieces
    width = out_weight.shape[1] // lax.axis_size("head")
    shape = jax.ShapeDtypeStruct
    small = shape((8, LANE), F32)
    state_out = (shape((DV + 16, LANE), BF16), shape((DV, LANE), F32), small)
    states = []
    for core in (1, 0):
        swap, own, own_log = call(
            functools.partial(state_body, core),
            state_out,
            key_vectors,
            values,
            log_gate,
            fetched=(0, 1, 2),
        )
        swap = lax.ppermute(swap, "core", [(core, 1 - core)])
        states.append((own, own_log, swap))
    sent, early, decay = call(
        join_body,
        (shape((pieces, 2 * rows + 8, LANE), BF16), shape((DV, LANE), BF16), small),
        *states[1],
        *states[0],
    )
    slices = lax.all_to_all(sent, CHIPS, 0, 0, tiled=True)
    prefixes = call(scan_body, shape((pieces, 2 * rows, LANE), BF16), slices)
    prefixes, queries = lax.optimization_barrier((prefixes, queries))
    inputs = (queries, key_vectors, values, log_gate, out_gate)
    att_local, q_start, scale, w_far = call(
        local_body,
        (
            shape((length, DV), F32),
            shape((length, DK), BF16),
            shape((length, DV), BF16),
            shape((DV, width), BF16),
        ),
        *inputs,
        out_weight,
        norm_gain.reshape(1, DV),
        fetched=(0, 1, 2, 3, 4, 5),
        scratch=[pltpu.VMEM(part.shape, BF16) for part in inputs],
        copies=6,
    )
    entering = lax.all_to_all(prefixes, CHIPS, 0, 0, tiled=True)
    state_half = shape((DV, LANE), BF16)
    entering, att_local, q_start, scale, w_far = lax.optimization_barrier(
        (entering, att_local, q_start, scale, w_far)
    )
    keep, send = call(part_body, (state_half, state_half), entering, early, decay)
    other = lax.ppermute(send, "core", ring("core", 1))
    column = shape((length, 1), F32)
    split = length // 2 + length // 32
    tops, lows = shape((split, width), BF16), shape((length - split, width), BF16)
    kept, square, kept_far = call(
        keep_body,
        (shape((length, half), BF16), column, shape((length, width), F32)),
        keep,
        q_start,
        att_local,
        scale,
        w_far,
    )
    up, down = ring("head", 1), ring("head", -1)
    rows_out = [(shape((n, DV), BF16), shape((n, 1), F32), shape((n, width), BF16))
                for n in (split, length - split)]
    finish_in = (other, q_start, att_local, kept, square, kept_far, scale, w_far)
    top, norm_top, far_up = call(functools.partial(finish_body, 0), rows_out[0], *finish_in)
    far_up = lax.ppermute(far_up, "head", up)
    low, norm_low, far_down = call(functools.partial(finish_body, split), rows_out[1], *finish_in)
    far_down = lax.ppermute(far_down, "head", down)
    gated = (top, low, norm_top, norm_low)
    up_b, down_a = call(
        direct_body,
        (lows, tops),
        *gated,
        out_weight,
        fetched=(4,),
        scratch=[pltpu.VMEM((2, DV, width), BF16)],
        copies=2,
    )
    below_b = lax.ppermute(up_b, "head", up)
    above_a = lax.ppermute(down_a, "head", down)
    up_a, down_b, own_part = call(
        near_body,
        (shape(tops.shape, F32), shape(lows.shape, F32), shape((length, width), F32)),
        *gated,
        out_weight,
        fetched=(4,),
        scratch=[pltpu.VMEM((3, DV, width), BF16)],
        copies=3,
    )
    up_a, down_b = call(pass_body, (tops, lows), up_a, down_b, far_up, far_down)
    below_a = lax.ppermute(up_a, "head", up)
    above_b = lax.ppermute(down_b, "head", down)
    return call(
        sum_body,
        shape((length, width), BF16),
        own_part,
        below_a,
        below_b,
        above_a,
        above_b,
        scratch=[pltpu.VMEM((length, width), BF16)],
        copies=2,
        outs_in=HBM,
    )


def solution(mesh):
    split = Mesh(mesh.devices.reshape(4, 8, 2, mesh.shape["head"]), (*SEQ, "head"))
    in_specs = (
        P(SEQ, "head"),
        P(SEQ, "head"),
        P(SEQ, "head"),
        P(SEQ, "head"),
        P(SEQ, "head"),
        P("head"),
        P("head", None),
    )
    out_specs = P(SEQ, "head")

    return jax.shard_map(
        shards, mesh=split, in_specs=in_specs, out_specs=out_specs, check_vma=False
    )
```

```python
import functools

import jax
import jax.numpy as jnp
from jax import lax
from jax.experimental import pallas as pl
from jax.experimental.pallas import tpu as pltpu
from jax.sharding import Mesh
from jax.sharding import PartitionSpec as P


DK = 256
DV = 512
SPAN = 64
LANE = 128
SEQ = ("chip_x", "chip_z", "core")
CHIPS = ("chip_x", "chip_z")
F32 = jnp.float32
BF16 = jnp.bfloat16
VMEM = pl.BlockSpec(memory_space=pltpu.VMEM)
HBM = pl.BlockSpec(memory_space=pltpu.HBM)


def call(body, outs, *args, fetched=(), scratch=(), copies=0, outs_in=VMEM):
    moved = sum(a.size * a.dtype.itemsize for a in args)
    args = [
        pltpu.with_memory_space_constraint(a, pltpu.HBM) if i in fetched else a
        for i, a in enumerate(args)
    ]
    if fetched and not copies:
        scratch = [pltpu.VMEM(args[i].shape, args[i].dtype) for i in fetched]
        copies = len(fetched)
    if copies:
        scratch = [*scratch, pltpu.SemaphoreType.DMA((copies,))]
    return pl.pallas_call(
        body,
        out_shape=outs,
        in_specs=[HBM if i in fetched else VMEM for i in range(len(args))],
        out_specs=jax.tree.map(lambda _: outs_in, outs),
        scratch_shapes=scratch,
        cost_estimate=pl.CostEstimate(flops=10**9, transcendentals=0, bytes_accessed=moved),
        compiler_params=pltpu.CompilerParams(vmem_limit_bytes=16 * 2**20),
    )(*args)


def dot(a, b, dims=((1,), (0,))):
    return lax.dot_general(a, b, (dims, ((), ())), preferred_element_type=F32)


def triangle(length, keep):
    row = lax.broadcasted_iota(jnp.int32, (length, length), 0)
    col = lax.broadcasted_iota(jnp.int32, (length, length), 1)
    return jnp.where(keep(row, col), 1.0, 0.0).astype(BF16)


def stacked(*parts):
    row = lax.broadcasted_iota(jnp.int32, (8, LANE), 0)
    block = jnp.zeros((8, LANE), F32)
    for at, part in enumerate(parts):
        block = jnp.where(row == at, part, block)
    return block


def split_bf16(values):
    high = values.astype(BF16).astype(F32)
    return high, values - high


def fetch(sems, *pairs):
    copies = [pltpu.make_async_copy(src, dst, sems.at[i]) for i, (src, dst) in enumerate(pairs)]
    for copy in copies:
        copy.start()
    return copies


def columns(index, width):
    return pl.ds(pl.multiple_of(index * width, width), width)


def head_columns(shift, width):
    count = lax.axis_size("head")
    return columns(lax.rem(lax.axis_index("head") + shift, count), width)


def swap_body(k_hbm, v_hbm, g_hbm, swap_ref, log_ref, state_ref, k_ref, v_ref, g_ref, sems):
    half = DV // 2
    theirs = v_hbm.at[:, columns(1 - lax.axis_index("core"), half)]
    gate_copy, k_copy, v_copy = fetch(sems, (g_hbm, g_ref), (k_hbm, k_ref), (theirs, v_ref))
    length = k_ref.shape[0]
    mask = triangle(length, lambda r, c: c > r)
    gate_copy.wait()
    gate = g_ref[...]
    after = dot(mask, gate)
    total = after[0:1] + gate[0:1].astype(F32)
    k_copy.wait()
    v_copy.wait()
    k_state = (k_ref[...].astype(F32) * jnp.exp(after)).astype(BF16)
    state_ref[...] = k_state
    state = dot(v_ref[...], k_state, ((0,), (0,))).astype(BF16)
    swap_ref[0:half, :] = state[:, :LANE]
    swap_ref[half : 2 * half, :] = state[:, LANE:]
    left_high, left_low = split_bf16(total[:, :LANE])
    right_high, right_low = split_bf16(total[:, LANE:])
    tail = stacked(left_high, right_high, left_low, right_low)
    swap_ref[2 * half :, :] = jnp.concatenate([tail, tail], axis=0).astype(BF16)
    log_ref[...] = stacked(total[:, :LANE], total[:, LANE:])


def own_body(v_hbm, state_ref, own_ref, v_ref, sems):
    half = DV // 2
    mine = v_hbm.at[:, columns(lax.axis_index("core"), half)]
    (copy,) = fetch(sems, (mine, v_ref))
    copy.wait()
    state = dot(v_ref[...], state_ref[...], ((0,), (0,)))
    own_ref[0:half, :] = state[:, :LANE]
    own_ref[half:, :] = state[:, LANE:]


def join_body(own_ref, log_ref, swap_ref, out_ref, first_ref, decay_ref):
    pieces, rows = (out_ref.shape[0], (out_ref.shape[1] - 8) // 2)
    half = pieces * rows
    early = lax.axis_index("core") == 0
    tail = swap_ref[2 * half : 2 * half + 8, :].astype(F32)
    sums = []
    decays = []
    for side in range(2):
        at = slice(side * half, (side + 1) * half)
        own_log = log_ref[side : side + 1, :]
        other_log = tail[side : side + 1] + tail[side + 2 : side + 3]
        own = own_ref[at, :]
        other = swap_ref[at, :].astype(F32)
        first = jnp.where(early, own, other)
        second = jnp.where(early, other, own)
        state = first * jnp.exp(jnp.where(early, other_log, own_log)) + second
        first_ref[at, :] = first.astype(BF16)
        decays.append(jnp.exp(jnp.where(early, own_log, other_log)))
        sums.append(own_log + other_log)
        piece = slice(side * rows, (side + 1) * rows)
        out_ref[:, piece, :] = state.reshape(pieces, rows, LANE).astype(BF16)
    decay_ref[...] = stacked(*decays)
    left_high, left_low = split_bf16(sums[0])
    right_high, right_low = split_bf16(sums[1])
    tail = stacked(left_high, right_high, left_low, right_low)
    out_ref[:, 2 * rows :, :] = jnp.broadcast_to(tail[None], (pieces, 8, LANE)).astype(BF16)


def scan_body(in_ref, out_ref):
    pieces, rows = (in_ref.shape[0], out_ref.shape[1] // 2)
    left = right = jnp.zeros((rows, LANE), F32)
    for j in range(pieces):
        out_ref[j, 0:rows, :] = left.astype(BF16)
        out_ref[j, rows : 2 * rows, :] = right.astype(BF16)
        tail = in_ref[j, 2 * rows :, :].astype(F32)
        left = left * jnp.exp(tail[0:1] + tail[2:3]) + in_ref[j, 0:rows, :].astype(F32)
        right = right * jnp.exp(tail[1:2] + tail[3:4]) + in_ref[j, rows : 2 * rows, :].astype(F32)


def part_body(in_ref, first_ref, decay_ref, keep_ref, send_ref):
    pieces, rows = (in_ref.shape[0], in_ref.shape[1] // 2)
    half = pieces * rows
    early = lax.axis_index("core") == 0
    for side in range(2):
        at = slice(side * half, (side + 1) * half)
        piece = slice(side * rows, (side + 1) * rows)
        entering = in_ref[:, piece, :].astype(F32).reshape(half, LANE)
        between = entering * decay_ref[side : side + 1, :] + first_ref[at, :].astype(F32)
        keep_ref[at, :] = jnp.where(early, entering, between).astype(BF16)
        send_ref[at, :] = jnp.where(early, between, entering).astype(BF16)


def local_body(
    q_hbm, k_hbm, v_hbm, g_hbm, outer_hbm, w_hbm, gain_ref,
    att_ref, start_ref, scale_ref, w_ref, q_ref, k_ref, v_ref, g_ref, outer_ref, sems,
):
    far_columns = w_hbm.at[:, head_columns(2, w_ref.shape[1])]
    *copies, far_copy = fetch(
        sems,
        (g_hbm, g_ref),
        (q_hbm, q_ref),
        (k_hbm, k_ref),
        (v_hbm, v_ref),
        (outer_hbm, outer_ref),
        (far_columns, w_ref),
    )
    length = q_ref.shape[0]
    lower = triangle(SPAN, lambda r, c: c <= r)
    row = lax.broadcasted_iota(jnp.int32, (SPAN, SPAN), 0)
    col = lax.broadcasted_iota(jnp.int32, (SPAN, SPAN), 1)
    for copy in copies:
        copy.wait()
    carried = None
    before = jnp.zeros((1, DK), F32)
    for i in range(length // SPAN):
        at = slice(i * SPAN, (i + 1) * SPAN)
        running = dot(lower, g_ref[at, :])
        middle = running[SPAN // 2 : SPAN // 2 + 1]
        ending = running[SPAN - 1 : SPAN]
        query_f = q_ref[at, :].astype(F32)
        key_f = k_ref[at, :].astype(F32)
        value = v_ref[at, :]
        q_inter = query_f * jnp.exp(running)
        q_intra = (query_f * jnp.exp(running - middle)).astype(BF16)
        k_intra = (key_f * jnp.exp(middle - running)).astype(BF16)
        scores = dot(q_intra, k_intra, ((1,), (1,)))
        weights = jnp.where(col <= row, scores, 0.0).astype(BF16)
        attention = dot(weights, value)
        if i:
            attention = attention + dot(q_inter.astype(BF16), carried.astype(BF16))
        att_ref[at, :] = attention
        start_ref[at, :] = (query_f * jnp.exp(running + before)).astype(BF16)
        before = before + ending
        if (i + 1) * SPAN < length:
            k_state = (key_f * jnp.exp(ending - running)).T.astype(BF16)
            block = dot(k_state, value)
            carried = block if i == 0 else carried * jnp.exp(ending).reshape(DK, 1) + block
        outer_f = outer_ref[at, :].astype(F32)
        scale = outer_f / (1.0 + jnp.exp(-outer_f)) * gain_ref[...]
        scale_ref[at, :] = scale.astype(BF16)
    far_copy.wait()


def keep_body(
    keep_ref, q_ref, att_ref, scale_ref, w_ref, gated_ref, square_ref, far_ref
):
    half = keep_ref.shape[0] // 2
    here = columns(lax.axis_index("core"), half)
    attention = att_ref[:, here]
    attention = attention + dot(q_ref[:, :LANE], keep_ref[:half, :], ((1,), (1,)))
    attention = attention + dot(q_ref[:, LANE:], keep_ref[half:, :], ((1,), (1,)))
    gated = (attention * scale_ref[:, here].astype(F32)).astype(BF16)
    gated_ref[...] = gated
    far_ref[...] = dot(gated, w_ref[here, :])
    square_ref[...] = jnp.sum(attention * attention, axis=-1, keepdims=True)


def finish_body(
    row, other_ref, q_ref, att_ref, kept_ref, square_ref, kept_far_ref, scale_ref, w_ref,
    gated_ref, norm_ref, far_ref,
):
    half = other_ref.shape[0] // 2
    core = lax.axis_index("core")
    here, there = columns(core, half), columns(1 - core, half)
    at = slice(row, row + far_ref.shape[0])
    attention = att_ref[at, there]
    attention = attention + dot(q_ref[at, :LANE], other_ref[:half, :], ((1,), (1,)))
    attention = attention + dot(q_ref[at, LANE:], other_ref[half:, :], ((1,), (1,)))
    gated = (attention * scale_ref[at, there].astype(F32)).astype(BF16)
    far = kept_far_ref[at, :] + dot(gated, w_ref[there, :])
    total = square_ref[at, :] + jnp.sum(attention * attention, axis=-1, keepdims=True)
    norm = lax.rsqrt(total * (1.0 / DV) + 1e-05)
    norm_ref[...] = norm
    far_ref[...] = (far * norm).astype(BF16)
    gated_ref[:, there] = gated
    gated_ref[:, here] = kept_ref[at, :]


def direct_body(
    top_ref, low_ref, norm_top_ref, norm_low_ref, w_hbm, up_ref, down_ref, w_up_ref, w_down_ref, sems
):
    width = w_up_ref.shape[1]
    up_copy, down_copy = fetch(
        sems,
        (w_hbm.at[:, head_columns(1, width)], w_up_ref),
        (w_hbm.at[:, head_columns(3, width)], w_down_ref),
    )
    up_copy.wait()
    up_ref[...] = (dot(low_ref[...], w_up_ref[...]) * norm_low_ref[...]).astype(BF16)
    down_copy.wait()
    down_ref[...] = (dot(top_ref[...], w_down_ref[...]) * norm_top_ref[...]).astype(BF16)


def near_body(
    top_ref, low_ref, norm_top_ref, norm_low_ref, w_up_ref, w_down_ref, up_ref, down_ref
):
    up_ref[...] = dot(top_ref[...], w_up_ref[...]) * norm_top_ref[...]
    down_ref[...] = dot(low_ref[...], w_down_ref[...]) * norm_low_ref[...]


def own_part_body(top_ref, low_ref, norm_top_ref, norm_low_ref, w_hbm, own_ref, w_ref, sems):
    (copy,) = fetch(sems, (w_hbm.at[:, head_columns(0, w_ref.shape[1])], w_ref))
    split = top_ref.shape[0]
    copy.wait()
    own_ref[:split, :] = dot(top_ref[...], w_ref[...]) * norm_top_ref[...]
    own_ref[split:, :] = dot(low_ref[...], w_ref[...]) * norm_low_ref[...]


def pass_body(up_ref, down_ref, far_up_ref, far_down_ref, up_out_ref, down_out_ref):
    up_out_ref[...] = (up_ref[...] + far_up_ref[...].astype(F32)).astype(BF16)
    down_out_ref[...] = (down_ref[...] + far_down_ref[...].astype(F32)).astype(BF16)


def sum_body(own_ref, below_a_ref, below_b_ref, above_a_ref, above_b_ref, out_hbm, out_ref, sems):
    split = below_a_ref.shape[0]
    copies = []
    for i, (at, below, above) in enumerate(
        (
            (slice(0, split), below_a_ref, above_a_ref),
            (slice(split, own_ref.shape[0]), below_b_ref, above_b_ref),
        )
    ):
        total = own_ref[at, :] + below[...].astype(F32) + above[...].astype(F32)
        out_ref[at, :] = total.astype(BF16)
        copies += fetch(sems.at[pl.ds(i, 1)], (out_ref.at[at], out_hbm.at[at]))
    for copy in copies:
        copy.wait()


def ring(axis, shift):
    length = lax.axis_size(axis)
    return [(i, (i + shift) % length) for i in range(length)]


def shards(queries, key_vectors, values, log_gate, out_gate, norm_gain, out_weight):
    length = queries.shape[0]
    pieces = lax.axis_size(CHIPS)
    half = DV // 2
    rows = half // pieces
    width = out_weight.shape[1] // lax.axis_size("head")
    shape = jax.ShapeDtypeStruct
    small = shape((8, LANE), F32)
    swap, own_log, k_state = call(
        swap_body,
        (shape((DV + 16, LANE), BF16), small, shape((length, DK), BF16)),
        key_vectors,
        values,
        log_gate,
        fetched=(0, 1, 2),
        scratch=[pltpu.VMEM((length, n), BF16) for n in (DK, half, DK)],
        copies=3,
    )
    swapped = lax.ppermute(swap, "core", ring("core", 1))
    own = call(
        own_body,
        shape((DV, LANE), F32),
        values,
        k_state,
        fetched=(0,),
        scratch=[pltpu.VMEM((length, half), BF16)],
        copies=1,
    )
    sent, early, decay = call(
        join_body,
        (shape((pieces, 2 * rows + 8, LANE), BF16), shape((DV, LANE), BF16), small),
        own,
        own_log,
        swapped,
    )
    sent, queries = lax.optimization_barrier((sent, queries))
    slices = lax.all_to_all(sent, CHIPS, 0, 0, tiled=True)
    inputs = (queries, key_vectors, values, log_gate, out_gate)
    att_local, q_start, scale, w_far = call(
        local_body,
        (
            shape((length, DV), F32),
            shape((length, DK), BF16),
            shape((length, DV), BF16),
            shape((DV, width), BF16),
        ),
        *inputs,
        out_weight,
        norm_gain.reshape(1, DV),
        fetched=(0, 1, 2, 3, 4, 5),
        scratch=[pltpu.VMEM(part.shape, BF16) for part in inputs],
        copies=6,
    )
    slices, att_local, q_start, scale, w_far = lax.optimization_barrier(
        (slices, att_local, q_start, scale, w_far)
    )
    prefixes = call(scan_body, shape((pieces, 2 * rows, LANE), BF16), slices)
    entering = lax.all_to_all(prefixes, CHIPS, 0, 0, tiled=True)
    state_half = shape((DV, LANE), BF16)
    keep, send = call(part_body, (state_half, state_half), entering, early, decay)
    other = lax.ppermute(send, "core", ring("core", 1))
    column = shape((length, 1), F32)
    split = length // 2 + length // 32
    tops, lows = shape((split, width), BF16), shape((length - split, width), BF16)
    kept, square, kept_far = call(
        keep_body,
        (shape((length, half), BF16), column, shape((length, width), F32)),
        keep,
        q_start,
        att_local,
        scale,
        w_far,
    )
    up, down = ring("head", 1), ring("head", -1)
    rows_out = [
        (shape((n, DV), BF16), shape((n, 1), F32), shape((n, width), BF16))
        for n in (split, length - split)
    ]
    finish_in = (other, q_start, att_local, kept, square, kept_far, scale, w_far)
    top, norm_top, far_up = call(functools.partial(finish_body, 0), rows_out[0], *finish_in)
    far_up = lax.ppermute(far_up, "head", up)
    low, norm_low, far_down = call(functools.partial(finish_body, split), rows_out[1], *finish_in)
    far_down = lax.ppermute(far_down, "head", down)
    gated = (top, low, norm_top, norm_low)
    weight = shape((DV, width), BF16)
    up_b, down_a, w_up, w_down = call(
        direct_body,
        (lows, tops, weight, weight),
        *gated,
        out_weight,
        fetched=(4,),
        copies=2,
    )
    below_b = lax.ppermute(up_b, "head", up)
    above_a = lax.ppermute(down_a, "head", down)
    up_a, down_b = call(
        near_body, (shape(tops.shape, F32), shape(lows.shape, F32)), *gated, w_up, w_down
    )
    up_a, down_b = call(pass_body, (tops, lows), up_a, down_b, far_up, far_down)
    below_a = lax.ppermute(up_a, "head", up)
    above_b = lax.ppermute(down_b, "head", down)
    own_part = call(
        own_part_body,
        shape((length, width), F32),
        *gated,
        out_weight,
        fetched=(4,),
        scratch=[pltpu.VMEM((DV, width), BF16)],
        copies=1,
    )
    return call(
        sum_body,
        shape((length, width), BF16),
        own_part,
        below_a,
        below_b,
        above_a,
        above_b,
        scratch=[pltpu.VMEM((length, width), BF16)],
        copies=2,
        outs_in=HBM,
    )


def solution(mesh):
    split = Mesh(mesh.devices.reshape(4, 8, 2, mesh.shape["head"]), (*SEQ, "head"))
    in_specs = (
        P(SEQ, "head"),
        P(SEQ, "head"),
        P(SEQ, "head"),
        P(SEQ, "head"),
        P(SEQ, "head"),
        P("head"),
        P("head", None),
    )
    out_specs = P(SEQ, "head")

    return jax.shard_map(
        shards, mesh=split, in_specs=in_specs, out_specs=out_specs, check_vma=False
    )
```
